128 devices in a mesh: row: 16 (over z, y_hi, core), col: 8 (over y_lo, x).
Axes of the slice: x: 4, y: 4 (y_hi: 2, y_lo: 2; y = y_hi * 2 + y_lo), z: 4, core: 2. Of those that a mesh axis runs over, the one named last changes fastest.
Arguments:
- fine_residual: float32 [16, 3, 6291456], P(None, None, ('row', 'col')), may hold values from -6 to 6
- restriction: float32 [3, 3, 6291456], P(None, None, ('row', 'col')), may hold values from -1.25 to 1.25
- restriction_pattern: int32 [6291456], P(('row', 'col')), may hold values 0 or 1
- cell_aggregate: int32 [768, 1024], P('row', 'col'), may hold values from 0 to 786431, as said below
- block_inverse: float32 [3, 3, 768, 1024], P(None, None, 'row', 'col'), may hold values from -4 to 4, as said below
- off_blocks: float32 [4, 3, 3, 768, 1024], P(None, None, None, 'row', 'col'), may hold values from -0.5 to 0.5
- operator_pattern: int32 [4, 768, 1024], P(None, 'row', 'col'), may hold values 0 or 1
Outputs:
- coarse_solution: float32 [16, 3, 768, 1024], P(None, None, 'row', 'col')
- fine_correction: float32 [16, 3, 6291456], P(None, None, ('row', 'col'))
The draws below stay inside these ranges and needn't reach their ends.
Inputs may be any that keep to these rules, and one draw needn't show every extreme that they name: `cell_aggregate`: every aggregate number 0 to 786431 stands in exactly one coarse cell. Aggregate g = f * 6144 + a lies in the tile numbered a mod 128, where the tile of rows i * 48 to (i + 1) * 48 - 1 and columns j * 128 to (j + 1) * 128 - 1 is numbered i * 8 + j. `block_inverse`: each 3x3 block is the inverse of a cell's diagonal block.
All inputs are finite; a program needn't handle non-finite values. No bound on the sum of `restriction_pattern` or of `operator_pattern` on one device may be relied on, other than what follows from the above.
Results may differ from the reference program's by a relative error of at most 0.00002.
Values sent between devices are 32-bit elements; how exact they have to be, the bound alone decides.
A program may use at most 128 MiB of HBM per device.

```python
import jax
import jax.numpy as jnp

NRHS = 16
CR = 48
CC = 128
FPA = 8
ITERS = 4
AGG_DEV = 6144
FINE = 6291456
NCR = 768
NCC = 1024
N_ROW = 16
N_COL = 8


def draw_cell_aggregate(key, part):
    devices = N_ROW * N_COL

    def tile_cells(tile):
        order = jax.random.permutation(jax.random.fold_in(key, tile), AGG_DEV)
        owner = order % devices
        local = order // devices * devices + tile
        return (owner * AGG_DEV + local).astype(jnp.int32)
    tiles = jax.vmap(tile_cells)(jnp.arange(devices, dtype=jnp.int32))
    grid = tiles.reshape(N_ROW, N_COL, CR, CC).transpose(0, 2, 1, 3)
    return grid.reshape(N_ROW * CR, N_COL * CC)


def draw_block_inverse(key, part):
    scale_key = jax.random.fold_in(key, 11)
    noise_key = jax.random.fold_in(key, 12)
    scale = jnp.exp(jax.random.uniform(scale_key, (NCR, NCC), jnp.float32, jnp.log(0.5), jnp.log(2.0)))
    noise = 0.3 * jnp.clip(jax.random.normal(noise_key, (3, 3, NCR, NCC), jnp.float32), -2.5, 2.5)
    identity = jnp.eye(3, dtype=jnp.float32)[:, :, None, None]
    return (scale[None, None] * (identity + noise)).astype(jnp.float32)


def touch_ends(result, rng, low, high):
    shape = result.shape
    place = [jax.random.randint(jax.random.fold_in(rng, axis), (), 0, shape[axis]) for axis in range(len(shape))]
    result = result.at[tuple(place)].set(low)
    longest = shape.index(max(shape))
    place[longest] = (place[longest] + 1) % shape[longest]
    return result.at[tuple(place)].set(high)


def block_scale(rng, dims, split, smallest, high):
    def one(dim, parts):
        heights = jax.random.uniform(jax.random.fold_in(jax.random.fold_in(rng, 6), dim), (parts,), jnp.float32, smallest / len(split), high / len(split))
        return jnp.repeat(jnp.exp(heights), dims[dim] // parts).reshape((-1,) + (1,) * (len(dims) - dim - 1))

    level = one(*split[0])
    for cut in split[1:]:
        level = level * one(*cut)
    return level


def centred(stream_key, extent, width, bound, pieces=(), kind=jnp.bfloat16):
    drawn = width * jax.random.normal(stream_key, extent, jnp.float32)
    if pieces:
        drawn = drawn * block_scale(stream_key, extent, pieces, -0.22, 0.18)
    return jnp.clip(drawn, -bound, bound).astype(kind)


def setup_inputs(seed: int = 0) -> dict:
    key_list = jax.random.split(jax.random.key(seed), 8)
    return {
        "fine_residual": centred(key_list[0], (NRHS, 3, FINE), 1.0, 6.0, ((2, 128),), jnp.float32),
        "restriction": centred(key_list[1], (3, 3, FINE), (3 * FPA) ** -0.5, 1.25, ((2, 128),), jnp.float32),
        "restriction_pattern": touch_ends((jax.random.randint(key_list[2], (FINE,), 0, 4) < 3).astype(jnp.int32), jax.random.fold_in(key_list[2], 1), 0, 1),
        "cell_aggregate": draw_cell_aggregate(jax.random.fold_in(key_list[7], 71), 0),
        "block_inverse": draw_block_inverse(jax.random.fold_in(key_list[7], 71), 0),
        "off_blocks": centred(key_list[5], (4, 3, 3, NCR, NCC), 0.1, 0.5, ((3, 16), (4, 8)), jnp.float32),
        "operator_pattern": touch_ends((jax.random.randint(key_list[6], (4, NCR, NCC), 0, 4) < 3).astype(jnp.int32), jax.random.fold_in(key_list[6], 1), 0, 1),
    }


def apply_inverse(inverse, vector):
    total = inverse[:, 0][None] * vector[:, 0][:, None]
    for source in range(1, 3):
        total = total + inverse[:, source][None] * vector[:, source][:, None]
    return total


def neighbours(padded):
    height = padded.shape[-2] - 2
    breadth = padded.shape[-1] - 2
    return (padded[..., 0:height, 1:breadth + 1], padded[..., 2:height + 2, 1:breadth + 1],
            padded[..., 1:height + 1, 0:breadth], padded[..., 1:height + 1, 2:breadth + 2])


def sweep_once(padded, target_side, inverse, coupling):
    total = target_side
    for direction, shifted in enumerate(neighbours(padded)):
        for source in range(3):
            total = total - coupling[direction, :, source][None] * shifted[:, source][:, None]
    return apply_inverse(inverse, total)


def restrict_terms(residual, restriction, pattern):
    masked = residual * pattern.astype(jnp.float32)[None, None]
    total = restriction[:, 0][None] * masked[:, 0][:, None]
    for source in range(1, 3):
        total = total + restriction[:, source][None] * masked[:, source][:, None]
    loads = total.shape[0]
    return total.reshape(loads, 3, -1, FPA, AGG_DEV).sum(axis=3).reshape(loads, 3, -1)


def prolong_terms(values, restriction, pattern):
    loads = values.shape[0]
    slabs = values.shape[2] // AGG_DEV
    expanded = jnp.broadcast_to(values.reshape(loads, 3, slabs, 1, AGG_DEV), (loads, 3, slabs, FPA, AGG_DEV)).reshape(loads, 3, -1)
    total = restriction[0][None] * expanded[:, 0][:, None]
    for source in range(1, 3):
        total = total + restriction[source][None] * expanded[:, source][:, None]
    return total * pattern.astype(jnp.float32)[None, None]


def reference(fine_residual, restriction, restriction_pattern, cell_aggregate, block_inverse, off_blocks, operator_pattern):
    loads = fine_residual.shape[0]
    aggregate_rhs = restrict_terms(fine_residual, restriction, restriction_pattern)
    flat_cells = cell_aggregate.reshape(-1)
    coarse_rhs = jnp.take(aggregate_rhs, flat_cells, axis=2).reshape(loads, 3, NCR, NCC)
    coupling = off_blocks * operator_pattern.astype(jnp.float32)[:, None, None]
    iterate = apply_inverse(block_inverse, coarse_rhs)
    for sweep_index in range(ITERS - 1):
        padded = jnp.pad(iterate, ((0, 0), (0, 0), (1, 1), (1, 1)))
        iterate = sweep_once(padded, coarse_rhs, block_inverse, coupling)
    aggregate_solution = jnp.zeros_like(aggregate_rhs).at[:, :, flat_cells].set(iterate.reshape(loads, 3, -1))
    fine_correction = prolong_terms(aggregate_solution, restriction, restriction_pattern)
    return iterate, fine_correction
```

```python
import functools

import jax
import jax.numpy as jnp
from jax import lax
from jax.experimental import pallas as pl
from jax.experimental.pallas import tpu as pltpu
from jax.sharding import PartitionSpec as P

MESH = pl.DeviceIdType.MESH
ND = 128
NQ = 16
NI = 48
NK = 48
W = 48
AGG = 6144
FPA = 8
CHUNKS = 3
LANES = 128
F32 = jnp.float32


def me_index():
    return lax.axis_index("row") * 8 + lax.axis_index("col")


def coords(p):
    return (p // 8, p % 8)


def lane_ids():
    return lax.broadcasted_iota(jnp.int32, (8, LANES), 1)


def bcast_row(ref, *idx):
    return jnp.broadcast_to(ref[idx], (8, LANES))


def start_barrier():
    bar = pltpu.get_barrier_semaphore()
    me = me_index()

    def sig(o, c):
        p = lax.rem(me + o, ND)
        pl.semaphore_signal(bar, inc=1, device_id=coords(p), device_id_type=MESH)
        return c

    lax.fori_loop(1, ND, sig, 0)


def end_barrier():
    pl.semaphore_wait(pltpu.get_barrier_semaphore(), ND - 1)


def send_chunk(S, R, b, ssem, rsem):
    me = me_index()

    def send(o, c):
        p = lax.rem(me + o, ND)
        pltpu.make_async_remote_copy(
            S.at[b, p, pl.ds(0, 6)],
            R.at[b, me, pl.ds(0, 6)],
            ssem.at[b],
            rsem.at[b],
            device_id=coords(p),
            device_id_type=MESH,
        ).start()
        return c

    lax.fori_loop(1, ND, send, 0)


def wait_chunk(R, b, sem):
    block = R.at[b, pl.ds(0, ND - 1), pl.ds(0, 6)]
    pltpu.make_async_copy(block, block, sem.at[b]).wait()


def keep_own(S, R, b):
    me = me_index()
    R[b, me] = S[b, me]


def restrict_chunk(b, r, w, pat, A):
    def one(kk, c):
        k = b * 16 + kk
        acc = [[None] * 2 for _ in range(3)]
        for p in range(FPA):
            n = pl.multiple_of(p * AGG + k * LANES, LANES)
            there = bcast_row(pat, pl.ds(p * 48 + k, 1), slice(None)).astype(F32)
            here = [
                [r[j, qg * 8 : qg * 8 + 8, pl.ds(n, LANES)] * there for qg in range(2)]
                for j in range(3)
            ]
            for i in range(3):
                for j in range(3):
                    wij = jnp.broadcast_to(w[i, j : j + 1, pl.ds(n, LANES)], (8, LANES))
                    for qg in range(2):
                        term = wij * here[j][qg]
                        acc[i][qg] = term if acc[i][qg] is None else acc[i][qg] + term
        for i in range(3):
            for qg in range(2):
                at = pl.multiple_of(k * W + i * 16 + qg * 8, 8)
                A[pl.ds(at, 8), :] = acc[i][qg]
        return c

    lax.fori_loop(0, 16, one, 0)


def pack_chunk(b, A, S2d):
    for h in range(2):
        k8 = b * 16 + 8 * h
        six, seven = (k8 + 6) * W, (k8 + 7) * W
        for m in range(3):
            at = (k8 + 2 * m) * W
            head = A[at : at + 96, :]
            if m == 0:
                tail = [A[six : six + 32, :]]
            elif m == 1:
                tail = [A[seven : seven + 32, :]]
            else:
                tail = [A[six + 32 : six + 48, :], A[seven + 32 : seven + 48, :]]
            turned = jnp.concatenate([head] + tail, axis=0).T
            for t0 in range(16):
                rows = pl.ds(b * 1024 + t0 * 64 + 2 * m + h, 8, stride=8)
                S2d[rows, :] = turned[t0 * 8 : t0 * 8 + 8, :]


def unfold_chunk(b, R2d):
    lane = lane_ids()

    def one(fb, c):
        base = b * 1024 + fb * 64
        for h in range(2):
            x0 = R2d[pl.ds(base + h, 8, stride=8), :]
            x1 = R2d[pl.ds(base + 2 + h, 8, stride=8), :]
            x2 = R2d[pl.ds(base + 4 + h, 8, stride=8), :]
            six = jnp.where(lane < 32, pltpu.roll(x0, 32, 1), pltpu.roll(x2, 64, 1))
            seven = jnp.where(lane < 80, pltpu.roll(x1, 80, 1), pltpu.roll(x2, 96, 1))
            R2d[pl.ds(base + 6 + h, 8, stride=8), :] = jnp.where(lane < 48, six, seven)
        return c

    lax.fori_loop(0, 16, one, 0)


def fold_chunk(b, S2d):
    lane = lane_ids()

    def one(fb, c):
        base = b * 1024 + fb * 64
        for h in range(2):
            d = S2d[pl.ds(base + 6 + h, 8, stride=8), :]
            late = lane >= 96
            for m, moved in enumerate(
                (
                    pltpu.roll(d, 96, 1),
                    pltpu.roll(d, 48, 1),
                    jnp.where(lane < 112, pltpu.roll(d, 64, 1), pltpu.roll(d, 32, 1)),
                )
            ):
                rows = pl.ds(base + 2 * m + h, 8, stride=8)
                S2d[rows, :] = jnp.where(late, moved, S2d[rows, :])
        return c

    lax.fori_loop(0, 16, one, 0)


def gather_rows(slot, R2d, G):
    def some(blk, c):
        for u in range(64):
            c0 = blk * 64 + u
            G[pl.ds(c0, 1), :] = R2d[pl.ds(slot[c0], 1), :]
        return c

    lax.fori_loop(0, AGG // 64, some, 0)


def cells_to_planes(G, odd, rhs):
    def one(two, c):
        for u in range(4):
            row = two * 4 + u
            at = pl.multiple_of(row * LANES, LANES)
            turned = G[pl.ds(at, LANES), :].T
            is_odd = bcast_row(odd, pl.ds(row, 1), slice(None)) == 1
            for v in range(6):
                here = jnp.where(
                    is_odd, turned[W + v * 8 : W + v * 8 + 8, :], turned[v * 8 : v * 8 + 8, :]
                )
                rhs[pl.ds(pl.multiple_of(row * W + v * 8, 8), 8), :] = here
        return c

    lax.fori_loop(0, NI // 4, one, 0)


def solve_block(binv, row, total):
    out = []
    for i in range(3):
        acc = None
        for j in range(3):
            coef = bcast_row(binv, i * 3 + j, pl.ds(row, 1), slice(None))
            terms = [coef * total[j][qg] for qg in range(2)]
            acc = terms if acc is None else [x + y for x, y in zip(acc, terms)]
        out.append(acc)
    return out


def first_sweep(rhs, binv, X):
    def one(row, c):
        base = pl.multiple_of(row * W, 8)
        total = [
            [rhs[pl.ds(base + j * 16 + qg * 8, 8), :] for qg in range(2)] for j in range(3)
        ]
        new = solve_block(binv, row, total)
        for i in range(3):
            for qg in range(2):
                X[0, pl.ds(base + W + i * 16 + qg * 8, 8), :] = new[i][qg]
        return c

    lax.fori_loop(0, NI, one, 0)


def shift_columns(s, X, XL, XR, PL, PR):
    lane = lane_ids()

    def one(blk, carry):
        left, right = carry
        left, right = list(left), list(right)
        for u in range(4):
            row = blk * 4 + u
            base = pl.multiple_of(row * W, 8)
            for v in range(6):
                x = X[s, pl.ds(base + W + v * 8, 8), :]
                XL[pl.ds(base + v * 8, 8), :] = pltpu.roll(x, 1, 1)
                XR[pl.ds(base + v * 8, 8), :] = pltpu.roll(x, LANES - 1, 1)
                first = jnp.broadcast_to(x[:, 0:1], (8, LANES))
                last = jnp.broadcast_to(x[:, LANES - 1 : LANES], (8, LANES))
                left[v] = jnp.where(lane == row, first, left[v])
                right[v] = jnp.where(lane == row, last, right[v])
        return tuple(left), tuple(right)

    zero = tuple(jnp.zeros((8, LANES), F32) for _ in range(6))
    left, right = lax.fori_loop(0, NI // 4, one, (zero, zero))
    for v in range(6):
        PL[s, v * 8 : v * 8 + 8, :] = left[v]
        PR[s, v * 8 : v * 8 + 8, :] = right[v]


def halo_copies(s, X, PL, PR, HL, HR, hs, hr):
    row, col = lax.axis_index("row"), lax.axis_index("col")
    own_first = X.at[s, pl.ds(W, W)]
    own_last = X.at[s, pl.ds(NI * W, W)]
    above = X.at[s, pl.ds(0, W)]
    below = X.at[s, pl.ds((NI + 1) * W, W)]
    table = [
        (row > 0, row < 15, own_first, below, (row - 1, col), 0),
        (row < 15, row > 0, own_last, above, (row + 1, col), 1),
        (col > 0, col < 7, PL.at[s], HR.at[s], (row, col - 1), 2),
        (col < 7, col > 0, PR.at[s], HL.at[s], (row, col + 1), 3),
    ]
    return [
        (
            sends,
            receives,
            pltpu.make_async_remote_copy(
                src, dst, hs.at[s, n], hr.at[s, n], device_id=dev, device_id_type=MESH
            ),
            dst,
        )
        for sends, receives, src, dst, dev, n in table
    ]


def exchange_halo(s, X, PL, PR, HL, HR, hs, hr):
    copies = halo_copies(s, X, PL, PR, HL, HR, hs, hr)
    for sends, _, copy, _ in copies:
        pl.when(sends)(copy.start)
    for _, receives, copy, dst in copies:
        pl.when(receives)(copy.wait_recv)

        def clear(dst=dst):
            dst[...] = jnp.zeros((W, LANES), F32)

        pl.when(jnp.logical_not(receives))(clear)


def fill_columns(s, XL, XR, HL, HR):
    lane = lane_ids()

    def one(blk, c):
        for u in range(4):
            row = blk * 4 + u
            base = pl.multiple_of(row * W, 8)
            for v in range(6):
                at = pl.ds(base + v * 8, 8)
                edge = pltpu.roll(HL[s, v * 8 : v * 8 + 8, :], LANES - row, 1)
                XL[at, :] = jnp.where(lane == 0, edge, XL[at, :])
                edge = pltpu.roll(HR[s, v * 8 : v * 8 + 8, :], LANES - 1 - row, 1)
                XR[at, :] = jnp.where(lane == LANES - 1, edge, XR[at, :])
        return c

    lax.fori_loop(0, NI // 4, one, 0)


def sweep(s, rhs, binv, coup, X, XL, XR, out):
    def one(row, c):
        base = pl.multiple_of(row * W, 8)

        def at(v):
            return pl.ds(base + v * 8, 8)

        total = [[rhs[at(j * 2 + qg), :] for qg in range(2)] for j in range(3)]
        for d in range(4):
            for k in range(3):
                near = []
                for qg in range(2):
                    v = k * 2 + qg
                    if d == 0:
                        near.append(X[s, at(v), :])
                    elif d == 1:
                        near.append(X[s, at(v + 12), :])
                    elif d == 2:
                        near.append(XL[at(v), :])
                    else:
                        near.append(XR[at(v), :])
                for j in range(3):
                    coef = bcast_row(coup, d * 9 + j * 3 + k, pl.ds(row, 1), slice(None))
                    for qg in range(2):
                        total[j][qg] = total[j][qg] - coef * near[qg]
        new = solve_block(binv, row, total)
        for i in range(3):
            for qg in range(2):
                v = i * 2 + qg
                if out is None:
                    X[s + 1, at(v + 6), :] = new[i][qg]
                else:
                    planes, last = out
                    last[at(v), :] = new[i][qg]
                    planes[pl.ds((qg * 8 * 3 + i) * NI + row, 8, stride=3 * NI), :] = new[i][qg]
        return c

    lax.fori_loop(0, NI, one, 0)


def planes_to_cells(last, G):
    def one(blk, c):
        for u in range(4):
            row = blk * 4 + u
            x = last[pl.ds(pl.multiple_of(row * W, 8), W), :]
            turned = jnp.concatenate([x, x, x[0:32]], axis=0).T
            G[pl.ds(pl.multiple_of(row * LANES, LANES), LANES), :] = turned
        return c

    lax.fori_loop(0, NI // 4, one, 0)


def collect_chunk(b, inv, G, S2d):
    lane = lax.broadcasted_iota(jnp.int32, (1, LANES), 1)

    def one(fb, c):
        for u in range(4):
            f = fb * 4 + u
            for rr in range(8):
                even = G[pl.ds(inv[(b * ND + f) * 16 + rr * 2], 1), :]
                odd = G[pl.ds(inv[(b * ND + f) * 16 + rr * 2 + 1], 1), :]
                S2d[pl.ds(b * 1024 + f * 8 + rr, 1), :] = jnp.where(lane < W, even, odd)
        return c

    lax.fori_loop(0, ND // 4, one, 0)


def spread_chunk(b, R2d, Y):
    for h in range(2):
        k8 = b * 16 + 8 * h
        six, seven = (k8 + 6) * W, (k8 + 7) * W
        for m in range(3):
            parts = [
                R2d[pl.ds(b * 1024 + t0 * 64 + 2 * m + h, 8, stride=8), :] for t0 in range(16)
            ]
            turned = jnp.concatenate(parts, axis=0).T
            at = (k8 + 2 * m) * W
            Y[at : at + 96, :] = turned[0:96]
            if m == 0:
                Y[six : six + 32, :] = turned[96:128]
            elif m == 1:
                Y[seven : seven + 32, :] = turned[96:128]
            else:
                Y[six + 32 : six + 48, :] = turned[96:112]
                Y[seven + 32 : seven + 48, :] = turned[112:128]


def coarse_kernel(
    slot,
    inv,
    r_hbm,
    w_hbm,
    pat,
    odd,
    binv,
    off,
    opat,
    planes,
    Y,
    r,
    w,
    A,
    S,
    R,
    S2,
    R2,
    G,
    rhs,
    X,
    XL,
    XR,
    PL,
    PR,
    HL,
    HR,
    coup,
    load_sem,
    s1,
    r1,
    s2,
    r2,
    hs,
    hr,
):
    loads = []
    for b in range(CHUNKS):
        for p in range(FPA):
            n = pl.ds(p * AGG + b * 2048, 2048)
            loads.append((b, r_hbm.at[:, :, n], r.at[:, :, n], load_sem.at[0, b, p]))
            loads.append((b, w_hbm.at[:, :, n], w.at[:, :, n], load_sem.at[1, b, p]))
    loads = [(b, pltpu.make_async_copy(x, y, z)) for b, x, y, z in loads]
    for _, copy in loads:
        copy.start()
    start_barrier()

    S_rows, R_rows = S.reshape(CHUNKS * 1024, LANES), R.reshape(CHUNKS * 1024, LANES)
    S2_rows, R2_rows = S2.reshape(CHUNKS * 1024, LANES), R2.reshape(CHUNKS * 1024, LANES)
    for b in range(CHUNKS):
        for at, copy in loads:
            if at == b:
                copy.wait()
        restrict_chunk(b, r, w, pat, A)
        pack_chunk(b, A, S_rows)
        if b == 0:
            end_barrier()
        send_chunk(S, R, b, s1, r1)
        keep_own(S, R, b)

    def couple(row, c):
        at = pl.ds(pl.multiple_of(row * 8, 8), 8)
        for d in range(4):
            there = opat[d, at, :].astype(F32)
            for e in range(9):
                coup[d * 9 + e, at, :] = off[d * 9 + e, at, :] * there
        return c

    lax.fori_loop(0, NI // 8, couple, 0)

    for b in range(CHUNKS):
        wait_chunk(R, b, r1)
        unfold_chunk(b, R_rows)
    gather_rows(slot, R_rows, G)
    cells_to_planes(G, odd, rhs)
    first_sweep(rhs, binv, X)
    for s in range(3):
        shift_columns(s, X, XL, XR, PL, PR)
        exchange_halo(s, X, PL, PR, HL, HR, hs, hr)
        fill_columns(s, XL, XR, HL, HR)
        sweep(s, rhs, binv, coup, X, XL, XR, (planes, rhs) if s == 2 else None)

    planes_to_cells(rhs, G)
    for b in range(CHUNKS):
        collect_chunk(b, inv, G, S2_rows)
        fold_chunk(b, S2_rows)
        send_chunk(S2, R2, b, s2, r2)
        keep_own(S2, R2, b)
    for b in range(CHUNKS):
        wait_chunk(R2, b, r2)
        spread_chunk(b, R2_rows, Y)

    for b in range(CHUNKS):
        wait_chunk(R, b, s1)
        wait_chunk(R, b, s2)
    for s in range(3):
        for sends, _, copy, _ in halo_copies(s, X, PL, PR, HL, HR, hs, hr):
            pl.when(sends)(copy.wait_send)


def prolong_kernel(y, w, pat, out):
    block = pl.program_id(0)
    del block

    def one(k, c):
        n = pl.multiple_of(k * LANES, LANES)
        base = pl.multiple_of(k * W, 8)
        there = bcast_row(pat, pl.ds(k, 1), slice(None)).astype(F32)
        src = [
            [y[pl.ds(base + i * 16 + qg * 8, 8), :] * there for qg in range(2)] for i in range(3)
        ]
        for j in range(3):
            acc = None
            for i in range(3):
                wij = jnp.broadcast_to(w[i, j : j + 1, pl.ds(n, LANES)], (8, LANES))
                terms = [wij * src[i][qg] for qg in range(2)]
                acc = terms if acc is None else [x + z for x, z in zip(acc, terms)]
            for qg in range(2):
                out[j, qg * 8 : qg * 8 + 8, pl.ds(n, LANES)] = acc[qg]
        return c

    lax.fori_loop(0, NK, one, 0)


def inverse_slots(owner, local):
    cell = jnp.arange(AGG, dtype=jnp.int32)
    by_owner = (owner[:, None] == jnp.arange(ND)[None]).astype(jnp.bfloat16)
    by_local = local[:, None] == jnp.arange(NK)[None]
    low = jnp.where(by_local, (cell % LANES)[:, None], 0).astype(jnp.bfloat16)
    high = jnp.where(by_local, (cell // LANES)[:, None], 0).astype(jnp.bfloat16)
    both = lax.dot_general(
        by_owner,
        jnp.concatenate([low, high], axis=1),
        (((0,), (0,)), ((), ())),
        preferred_element_type=F32,
    )
    found = (both[:, NK:] * LANES + both[:, :NK]).astype(jnp.int32)
    return found.reshape(ND, 3, 2, 4, 2).transpose(1, 0, 3, 2, 4).reshape(-1)


def body(residual, restriction, pattern, cell_aggregate, block_inverse, off_blocks, op_pattern):
    owner = (cell_aggregate // AGG).reshape(-1)
    local = (cell_aggregate % AGG // ND).reshape(-1)
    slot = (
        local // 16 * 1024 + owner * 8 + local % 8 // 2 * 2 + local // 8 % 2
    )
    odd = (local % 2).reshape(NI, LANES)
    inv = inverse_slots(owner, local)
    turned = residual.transpose(1, 0, 2)
    pat = pattern.reshape(384, LANES)

    vmem = pl.BlockSpec(memory_space=pltpu.VMEM)
    smem = pl.BlockSpec(memory_space=pltpu.SMEM)
    hbm = pl.BlockSpec(memory_space=pl.ANY)
    msg = pltpu.VMEM((CHUNKS, ND, 8, LANES), F32)
    plane = pltpu.VMEM((NI * W, LANES), F32)
    edge = pltpu.VMEM((3, W, LANES), F32)
    planes, y = pl.pallas_call(
        coarse_kernel,
        out_shape=(
            jax.ShapeDtypeStruct((NQ * 3 * NI, LANES), F32),
            jax.ShapeDtypeStruct((NK * W, LANES), F32),
        ),
        in_specs=[smem, smem, hbm, hbm, vmem, vmem, vmem, vmem, vmem],
        out_specs=(vmem, vmem),
        scratch_shapes=[
            pltpu.VMEM((3, NQ, FPA * AGG), F32),
            pltpu.VMEM((3, 3, FPA * AGG), F32),
            plane,
            msg,
            msg,
            msg,
            msg,
            pltpu.VMEM((AGG, LANES), F32),
            plane,
            pltpu.VMEM((3, (NI + 2) * W, LANES), F32),
            plane,
            plane,
            edge,
            edge,
            edge,
            edge,
            pltpu.VMEM((36, NI, LANES), F32),
            pltpu.SemaphoreType.DMA((2, CHUNKS, FPA)),
            pltpu.SemaphoreType.DMA((CHUNKS,)),
            pltpu.SemaphoreType.DMA((CHUNKS,)),
            pltpu.SemaphoreType.DMA((CHUNKS,)),
            pltpu.SemaphoreType.DMA((CHUNKS,)),
            pltpu.SemaphoreType.DMA((3, 4)),
            pltpu.SemaphoreType.DMA((3, 4)),
        ],
        compiler_params=pltpu.CompilerParams(
            collective_id=0, has_side_effects=True, vmem_limit_bytes=48 * 1024 * 1024
        ),
    )(
        slot,
        inv,
        turned,
        restriction,
        pat,
        odd,
        block_inverse.reshape(9, NI, LANES),
        off_blocks.reshape(36, NI, LANES),
        op_pattern,
    )
    fine = pl.pallas_call(
        prolong_kernel,
        grid=(FPA,),
        out_shape=jax.ShapeDtypeStruct((3, NQ, FPA * AGG), F32),
        in_specs=[
            pl.BlockSpec((NK * W, LANES), lambda p: (0, 0)),
            pl.BlockSpec((3, 3, AGG), lambda p: (0, 0, p)),
            pl.BlockSpec((NK, LANES), lambda p: (p, 0)),
        ],
        out_specs=pl.BlockSpec((3, NQ, AGG), lambda p: (0, 0, p)),
        compiler_params=pltpu.CompilerParams(vmem_limit_bytes=16 * 1024 * 1024),
    )(y, restriction, pat)
    return planes.reshape(NQ, 3, NI, LANES), fine.transpose(1, 0, 2)


def solution(mesh):
    in_specs = (
        P(None, None, ("row", "col")),
        P(None, None, ("row", "col")),
        P(("row", "col")),
        P("row", "col"),
        P(None, None, "row", "col"),
        P(None, None, None, "row", "col"),
        P(None, "row", "col"),
    )
    out_specs = (P(None, None, "row", "col"), P(None, None, ("row", "col")))
    return jax.shard_map(body, mesh=mesh, in_specs=in_specs, out_specs=out_specs, check_vma=False)
```

```python
import functools

import jax
import jax.numpy as jnp
from jax import lax
from jax.experimental import pallas as pl
from jax.experimental.pallas import tpu as pltpu
from jax.sharding import PartitionSpec as P

MESH = pl.DeviceIdType.MESH
ND = 128
NQ = 16
NI = 48
NK = 48
W = 48
AGG = 6144
FPA = 8
CHUNKS = 3
LANES = 128
F32 = jnp.float32


def me_index():
    return lax.axis_index("row") * 8 + lax.axis_index("col")


def lane_ids():
    return lax.broadcasted_iota(jnp.int32, (8, LANES), 1)


def bcast_row(ref, *idx):
    return jnp.broadcast_to(ref[idx], (8, LANES))


def each_peer(visit):
    row, col = lax.axis_index("row"), lax.axis_index("col")
    cols = [lax.rem(col + d, 8) for d in range(8)]
    for other in cols[1:]:
        visit(row, other)

    def one(d, c):
        there = lax.rem(row + d, 16)
        for other in cols:
            visit(there, other)
        return c

    lax.fori_loop(1, 16, one, 0)


def start_barrier():
    bar = pltpu.get_barrier_semaphore()
    each_peer(
        lambda row, col: pl.semaphore_signal(
            bar, inc=1, device_id=(row, col), device_id_type=MESH
        )
    )


def end_barrier():
    pl.semaphore_wait(pltpu.get_barrier_semaphore(), ND - 1)


def send_chunk(S, R, b, ssem, rsem):
    dst = R.at[b, me_index(), pl.ds(0, 6)]

    def visit(row, col):
        pltpu.make_async_remote_copy(
            S.at[b, row * 8 + col, pl.ds(0, 6)],
            dst,
            ssem.at[b],
            rsem.at[b],
            device_id=(row, col),
            device_id_type=MESH,
        ).start()

    each_peer(visit)


def wait_chunk(R, b, sem):
    block = R.at[b, pl.ds(0, ND - 1), pl.ds(0, 6)]
    pltpu.make_async_copy(block, block, sem.at[b]).wait()


def keep_own(S, R, b):
    me = me_index()
    R[b, me] = S[b, me]


def restrict_chunk(b, r, w, pat, A):
    def one(kk, c):
        k = b * 16 + kk
        acc = [[None] * 2 for _ in range(3)]
        for p in range(FPA):
            n = pl.multiple_of(p * AGG + k * LANES, LANES)
            there = bcast_row(pat, pl.ds(p * 48 + k, 1), slice(None)).astype(F32)
            here = [
                [r[j, qg * 8 : qg * 8 + 8, pl.ds(n, LANES)] * there for qg in range(2)]
                for j in range(3)
            ]
            for i in range(3):
                for j in range(3):
                    wij = jnp.broadcast_to(w[i, j : j + 1, pl.ds(n, LANES)], (8, LANES))
                    for qg in range(2):
                        term = wij * here[j][qg]
                        acc[i][qg] = term if acc[i][qg] is None else acc[i][qg] + term
        for i in range(3):
            for qg in range(2):
                at = pl.multiple_of(k * W + i * 16 + qg * 8, 8)
                A[pl.ds(at, 8), :] = acc[i][qg]
        return c

    lax.fori_loop(0, 16, one, 0)


def pack_chunk(b, A, S2d):
    for h in range(2):
        k8 = b * 16 + 8 * h
        six, seven = (k8 + 6) * W, (k8 + 7) * W
        for m in range(3):
            at = (k8 + 2 * m) * W
            head = A[at : at + 96, :]
            if m == 0:
                tail = [A[six : six + 32, :]]
            elif m == 1:
                tail = [A[seven : seven + 32, :]]
            else:
                tail = [A[six + 32 : six + 48, :], A[seven + 32 : seven + 48, :]]
            turned = jnp.concatenate([head] + tail, axis=0).T
            for t0 in range(16):
                rows = pl.ds(b * 1024 + t0 * 64 + 2 * m + h, 8, stride=8)
                S2d[rows, :] = turned[t0 * 8 : t0 * 8 + 8, :]


def unfold_chunk(b, R2d):
    lane = lane_ids()

    def one(fb, c):
        for base, h in [(b * 1024 + (fb * 4 + u) * 64, h) for u in range(4) for h in range(2)]:
            x0 = R2d[pl.ds(base + h, 8, stride=8), :]
            x1 = R2d[pl.ds(base + 2 + h, 8, stride=8), :]
            x2 = R2d[pl.ds(base + 4 + h, 8, stride=8), :]
            six = jnp.where(lane < 32, pltpu.roll(x0, 32, 1), pltpu.roll(x2, 64, 1))
            seven = jnp.where(lane < 80, pltpu.roll(x1, 80, 1), pltpu.roll(x2, 96, 1))
            R2d[pl.ds(base + 6 + h, 8, stride=8), :] = jnp.where(lane < 48, six, seven)
        return c

    lax.fori_loop(0, 4, one, 0)


def fold_chunk(b, S2d):
    lane = lane_ids()

    def one(fb, c):
        for base, h in [(b * 1024 + (fb * 4 + u) * 64, h) for u in range(4) for h in range(2)]:
            d = S2d[pl.ds(base + 6 + h, 8, stride=8), :]
            late = lane >= 96
            for m, moved in enumerate(
                (
                    pltpu.roll(d, 96, 1),
                    pltpu.roll(d, 48, 1),
                    jnp.where(lane < 112, pltpu.roll(d, 64, 1), pltpu.roll(d, 32, 1)),
                )
            ):
                rows = pl.ds(base + 2 * m + h, 8, stride=8)
                S2d[rows, :] = jnp.where(late, moved, S2d[rows, :])
        return c

    lax.fori_loop(0, 4, one, 0)


def index_tables(ca, slot_v, odd, inv_v):
    def one(blk, acc):
        rows = pl.ds(pl.multiple_of(blk * 8, 8), 8)
        pair = lax.shift_right_logical(ca[rows, :], 7)
        owner = lax.shift_right_logical(lax.shift_right_logical(pair, 4) * 171, 9)
        local = pair - owner * NK
        bit = [lax.shift_right_logical(local, n) & 1 for n in range(4)]
        chunk = lax.shift_right_logical(local, 4)
        at = chunk * 1024 + owner * 8 + (bit[2] * 2 + bit[1]) * 2 + bit[3]
        slot_v[rows, :] = jnp.clip(at, 0, CHUNKS * 1024 - 1)
        odd[rows, :] = bit[0]
        for u in range(8):
            who = jnp.broadcast_to(owner[u : u + 1], (ND, LANES))
            by_owner = (who == lax.broadcasted_iota(jnp.int32, (ND, LANES), 0)).astype(F32)
            which = jnp.broadcast_to(local[u : u + 1], (NK, LANES))
            here = which == lax.broadcasted_iota(jnp.int32, (NK, LANES), 0)
            column = lax.broadcasted_iota(jnp.int32, (NK, LANES), 1).astype(F32)
            line = (blk * 8 + u).astype(F32)
            cells = jnp.concatenate(
                [jnp.where(here, column, 0.0), jnp.where(here, line, 0.0)], axis=0
            )
            acc = acc + lax.dot_general(
                by_owner.astype(jnp.bfloat16),
                cells.astype(jnp.bfloat16),
                (((1,), (1,)), ((), ())),
                preferred_element_type=F32,
            )
        return acc

    acc = lax.fori_loop(0, NI // 8, one, jnp.zeros((ND, 2 * NK), F32))
    cell = (acc[:, NK:] * LANES + acc[:, :NK]).astype(jnp.int32)
    inv_v[:, 0:NK] = jnp.clip(cell, 0, AGG - 1)


def gather_rows(slot, R2d, G):
    def some(row, c):
        base = pl.multiple_of(row * LANES, LANES)
        for u in range(LANES):
            G[pl.ds(base + u, 1), :] = R2d[pl.ds(slot[row, u], 1), :]
        return c

    lax.fori_loop(0, NI, some, 0)


def solve_block(binv, row, total):
    out = []
    for i in range(3):
        acc = None
        for j in range(3):
            coef = bcast_row(binv, i * 3 + j, pl.ds(row, 1), slice(None))
            terms = [coef * total[j][qg] for qg in range(2)]
            acc = terms if acc is None else [x + y for x, y in zip(acc, terms)]
        out.append(acc)
    return out


def cells_to_planes(G, odd, rhs, binv, X):
    def one(two, c):
        for u in range(4):
            row = two * 4 + u
            base = pl.multiple_of(row * W, 8)
            turned = G[pl.ds(pl.multiple_of(row * LANES, LANES), LANES), :].T
            is_odd = bcast_row(odd, pl.ds(row, 1), slice(None)) == 1
            total = [[None] * 2 for _ in range(3)]
            for v in range(6):
                here = jnp.where(
                    is_odd, turned[W + v * 8 : W + v * 8 + 8, :], turned[v * 8 : v * 8 + 8, :]
                )
                rhs[pl.ds(base + v * 8, 8), :] = here
                total[v // 2][v % 2] = here
            new = solve_block(binv, row, total)
            for v in range(6):
                X[0, pl.ds(base + W + v * 8, 8), :] = new[v // 2][v % 2]
        return c

    lax.fori_loop(0, NI // 4, one, 0)


def couplings(off, opat, binv, coup, pc, pb):
    def couple(blk, c):
        at = pl.ds(pl.multiple_of(blk * 8, 8), 8)
        for d in range(4):
            there = opat[d, at, :].astype(F32)
            for e in range(9):
                coup[d * 9 + e, at, :] = off[d * 9 + e, at, :] * there
        return c

    lax.fori_loop(0, NI // 8, couple, 0)

    def pack(e, c):
        for blk in range(3):
            for src, plane, keep in (
                (coup, 18 + e, (0,)),
                (coup, 27 + e, (1,)),
                (binv, e, (0, 1)),
            ):
                parts = [
                    bcast_row(src, plane, slice(blk * 16 + n, blk * 16 + n + 1), slice(None))
                    for n in range(16)
                ]
                turned = jnp.concatenate(parts, axis=0).T
                for side in keep:
                    line = turned[0:1] if side == 0 else turned[LANES - 1 : LANES]
                    dst = pb if src is binv else pc
                    for qg in range(2):
                        dst[side, e, qg * 3 + blk : qg * 3 + blk + 1, :] = line
        return c

    lax.fori_loop(0, 9, pack, 0)

    def mask(e, c):
        lane = lax.broadcasted_iota(jnp.int32, (NI, LANES), 1)
        coup[18 + e] = jnp.where(lane == 0, 0.0, coup[18 + e])
        coup[27 + e] = jnp.where(lane == LANES - 1, 0.0, coup[27 + e])
        return c

    lax.fori_loop(0, 9, mask, 0)


def pack_edges(s, X, E):
    for blk in range(3):
        for v in range(6):
            parts = [
                X[s, (blk * 16 + n + 1) * W + v * 8 : (blk * 16 + n + 1) * W + v * 8 + 8, :]
                for n in range(16)
            ]
            turned = jnp.concatenate(parts, axis=0).T
            at = v % 2 * 3 + blk
            E[0, s, v // 2, at : at + 1, :] = turned[0:1]
            E[1, s, v // 2, at : at + 1, :] = turned[LANES - 1 : LANES]


def halo_copies(s, X, E, H, hs, hr):
    row, col = lax.axis_index("row"), lax.axis_index("col")
    own_first = X.at[s, pl.ds(W, W)]
    own_last = X.at[s, pl.ds(NI * W, W)]
    above = X.at[s, pl.ds(0, W)]
    below = X.at[s, pl.ds((NI + 1) * W, W)]
    table = [
        (row > 0, row < 15, own_first, below, (row - 1, col)),
        (row < 15, row > 0, own_last, above, (row + 1, col)),
        (col > 0, col < 7, E.at[0, s], H.at[1, s], (row, col - 1)),
        (col < 7, col > 0, E.at[1, s], H.at[0, s], (row, col + 1)),
    ]
    return [
        (
            sends,
            receives,
            pltpu.make_async_remote_copy(
                src, dst, hs.at[s, n], hr.at[s, n], device_id=dev, device_id_type=MESH
            ),
            dst,
        )
        for n, (sends, receives, src, dst, dev) in enumerate(table)
    ]


def start_copies(copies):
    for sends, _, copy, _ in copies:
        pl.when(sends)(copy.start)


def finish_copies(copies):
    for _, receives, copy, dst in copies:
        pl.when(receives)(copy.wait_recv)

        def clear(dst=dst):
            dst[...] = jnp.zeros(dst.shape, F32)

        pl.when(jnp.logical_not(receives))(clear)


def sweep_row(s, row, rhs, binv, coup, X, new_at):
    base = pl.multiple_of(row * W, 8)

    def at(v):
        return pl.ds(base + v * 8, 8)

    own = [X[s, at(v + 6), :] for v in range(6)]
    left = [pltpu.roll(x, 1, 1) for x in own]
    right = [pltpu.roll(x, LANES - 1, 1) for x in own]
    total = [[rhs[at(j * 2 + qg), :] for qg in range(2)] for j in range(3)]
    for d in range(4):
        for k in range(3):
            near = []
            for qg in range(2):
                v = k * 2 + qg
                if d == 0:
                    near.append(X[s, at(v), :])
                elif d == 1:
                    near.append(X[s, at(v + 12), :])
                else:
                    near.append((left if d == 2 else right)[v])
            for j in range(3):
                coef = bcast_row(coup, d * 9 + j * 3 + k, pl.ds(row, 1), slice(None))
                for qg in range(2):
                    total[j][qg] = total[j][qg] - coef * near[qg]
    new = solve_block(binv, row, total)
    for v in range(6):
        new_at(row, v)[...] = new[v // 2][v % 2]


def correct_edges(s, H, pc, pb, D):
    for side in range(2):
        push = []
        for j in range(3):
            acc = None
            for k in range(3):
                term = pc[side, j * 3 + k] * H[side, s, k]
                acc = term if acc is None else acc + term
            push.append(acc)
        for i in range(3):
            acc = None
            for j in range(3):
                term = pb[side, i * 3 + j] * push[j]
                acc = term if acc is None else acc + term
            D[side, i] = -acc


def add_edges(blk, D, new_at):
    sub = lax.broadcasted_iota(jnp.int32, (8, LANES), 0)
    zero = jnp.zeros((LANES - 16, LANES), F32)
    for v in range(6):
        at = v % 2 * 3 + blk
        first = jnp.where(sub == 0, bcast_row(D, 0, v // 2, slice(at, at + 1), slice(None)), 0.0)
        last = jnp.where(sub == 7, bcast_row(D, 1, v // 2, slice(at, at + 1), slice(None)), 0.0)
        turned = jnp.concatenate([first, zero, last], axis=0).T
        for n in range(16):
            ref = new_at(blk * 16 + n, v)
            ref[...] = ref[...] + turned[n * 8 : n * 8 + 8]


def planes_to_cells(last, G):
    def one(blk, c):
        for u in range(4):
            row = blk * 4 + u
            x = last[pl.ds(pl.multiple_of(row * W, 8), W), :]
            turned = jnp.concatenate([x, x, x[0:32]], axis=0).T
            G[pl.ds(pl.multiple_of(row * LANES, LANES), LANES), :] = turned
        return c

    lax.fori_loop(0, NI // 4, one, 0)


def collect_chunk(b, inv, G, S2d):
    lane = lax.broadcasted_iota(jnp.int32, (1, LANES), 1)

    def one(fb, c):
        for u in range(4):
            f = fb * 4 + u
            for rr in range(8):
                k = b * 16 + rr % 2 * 8 + rr // 2 * 2
                even = G[pl.ds(inv[f, k], 1), :]
                odd = G[pl.ds(inv[f, k + 1], 1), :]
                S2d[pl.ds(b * 1024 + f * 8 + rr, 1), :] = jnp.where(lane < W, even, odd)
        return c

    lax.fori_loop(0, ND // 4, one, 0)


def spread_chunk(b, R2d, Y):
    for h in range(2):
        k8 = b * 16 + 8 * h
        six, seven = (k8 + 6) * W, (k8 + 7) * W
        for m in range(3):
            parts = [
                R2d[pl.ds(b * 1024 + t0 * 64 + 2 * m + h, 8, stride=8), :] for t0 in range(16)
            ]
            turned = jnp.concatenate(parts, axis=0).T
            at = (k8 + 2 * m) * W
            Y[at : at + 96, :] = turned[0:96]
            if m == 0:
                Y[six : six + 32, :] = turned[96:128]
            elif m == 1:
                Y[seven : seven + 32, :] = turned[96:128]
            else:
                Y[six + 32 : six + 48, :] = turned[96:112]
                Y[seven + 32 : seven + 48, :] = turned[112:128]


def coarse_kernel(
    r_hbm,
    w_hbm,
    pat_hbm,
    ca_hbm,
    binv_hbm,
    off_hbm,
    opat_hbm,
    x_out,
    Y,
    r,
    w,
    pat,
    ca,
    binv,
    off,
    opat,
    A,
    S,
    R,
    S2,
    R2,
    G,
    rhs,
    X,
    E,
    H,
    D,
    coup,
    pc,
    pb,
    slot_v,
    odd,
    inv_v,
    slot,
    inv,
    load_sem,
    small_sem,
    s1,
    r1,
    s2,
    r2,
    hs,
    hr,
):
    small = [
        pltpu.make_async_copy(x, y, small_sem.at[n])
        for n, (x, y) in enumerate(
            [
                (pat_hbm, pat),
                (ca_hbm, ca),
                (binv_hbm, binv),
                (off_hbm, off),
                (opat_hbm, opat),
                (slot_v, slot),
                (inv_v, inv),
            ]
        )
    ]
    loads = []
    for b in range(CHUNKS):
        for p in range(FPA):
            n = pl.ds(p * AGG + b * 2048, 2048)
            loads.append((b, r_hbm.at[:, :, n], r.at[:, :, n], load_sem.at[0, b, p]))
            loads.append((b, w_hbm.at[:, :, n], w.at[:, :, n], load_sem.at[1, b, p]))
    loads = [(b, pltpu.make_async_copy(x, y, z)) for b, x, y, z in loads]
    small[0].start()
    for _, copy in loads:
        copy.start()
    for copy in small[1:5]:
        copy.start()
    start_barrier()

    S_rows, R_rows = S.reshape(CHUNKS * 1024, LANES), R.reshape(CHUNKS * 1024, LANES)
    S2_rows, R2_rows = S2.reshape(CHUNKS * 1024, LANES), R2.reshape(CHUNKS * 1024, LANES)
    small[0].wait()
    for b in range(CHUNKS):
        for at, copy in loads:
            if at == b:
                copy.wait()
        restrict_chunk(b, r, w, pat, A)
        pack_chunk(b, A, S_rows)
        if b == 0:
            end_barrier()
        send_chunk(S, R, b, s1, r1)
        keep_own(S, R, b)

    for copy in small[1:5]:
        copy.wait()
    E[...] = jnp.zeros(E.shape, F32)
    pc[...] = jnp.zeros(pc.shape, F32)
    pb[...] = jnp.zeros(pb.shape, F32)
    inv_v[...] = jnp.zeros(inv_v.shape, jnp.int32)
    index_tables(ca, slot_v, odd, inv_v)
    small[5].start()
    small[6].start()
    couplings(off, opat, binv, coup, pc, pb)
    small[5].wait()
    small[6].wait()

    for b in range(CHUNKS):
        wait_chunk(R, b, r1)
        unfold_chunk(b, R_rows)
    gather_rows(slot, R_rows, G)
    cells_to_planes(G, odd, rhs, binv, X)

    halos = [halo_copies(s, X, E, H, hs, hr) for s in range(3)]
    start_copies(halos[0][:2])
    pack_edges(0, X, E)
    start_copies(halos[0][2:])
    for s in range(3):
        if s < 2:

            def new_at(row, v, s=s):
                return X.at[s + 1, pl.ds(pl.multiple_of(row * W + W + v * 8, 8), 8)]
        else:

            def new_at(row, v):
                return x_out.at[pl.ds(pl.multiple_of(row * W + v * 8, 8), 8)]

        def inner(two, c, s=s, new_at=new_at):
            for u in range(2):
                sweep_row(s, 1 + two * 2 + u, rhs, binv, coup, X, new_at)
            return c

        lax.fori_loop(0, (NI - 2) // 2, inner, 0)
        finish_copies(halos[s][:2])
        lax.fori_loop(
            0,
            2,
            lambda n, c, s=s, new_at=new_at: (
                sweep_row(s, n * (NI - 1), rhs, binv, coup, X, new_at),
                c,
            )[1],
            0,
        )
        finish_copies(halos[s][2:])
        correct_edges(s, H, pc, pb, D)
        add_edges(0, D, new_at)
        add_edges(2, D, new_at)
        if s < 2:
            start_copies(halos[s + 1][:2])
        add_edges(1, D, new_at)
        if s < 2:
            pack_edges(s + 1, X, E)
            start_copies(halos[s + 1][2:])

    planes_to_cells(x_out, G)
    for b in range(CHUNKS):
        collect_chunk(b, inv, G, S2_rows)
        fold_chunk(b, S2_rows)
        send_chunk(S2, R2, b, s2, r2)
        keep_own(S2, R2, b)
    for b in range(CHUNKS):
        wait_chunk(R2, b, r2)
        spread_chunk(b, R2_rows, Y)

    for b in range(CHUNKS):
        wait_chunk(R, b, s1)
        wait_chunk(R, b, s2)
    for copies in halos:
        for sends, _, copy, _ in copies:
            pl.when(sends)(copy.wait_send)


def prolong_kernel(y, x, w, pat, out, planes):
    step = pl.program_id(0)

    def line(n, c):
        row = step * 6 + n
        for v in range(6):
            at = (v % 2 * 24 + v // 2) * NI + row
            planes[pl.ds(at, 8, stride=3 * NI), :] = x[pl.ds(row * W + v * 8, 8), :]
        return c

    lax.fori_loop(0, NI // FPA, line, 0)

    def one(k, c):
        n = pl.multiple_of(k * LANES, LANES)
        base = pl.multiple_of(k * W, 8)
        there = bcast_row(pat, pl.ds(k, 1), slice(None)).astype(F32)
        src = [
            [y[pl.ds(base + i * 16 + qg * 8, 8), :] * there for qg in range(2)] for i in range(3)
        ]
        for j in range(3):
            acc = None
            for i in range(3):
                wij = jnp.broadcast_to(w[i, j : j + 1, pl.ds(n, LANES)], (8, LANES))
                terms = [wij * src[i][qg] for qg in range(2)]
                acc = terms if acc is None else [x + z for x, z in zip(acc, terms)]
            for qg in range(2):
                out[j, qg * 8 : qg * 8 + 8, pl.ds(n, LANES)] = acc[qg]
        return c

    lax.fori_loop(0, NK, one, 0)


def body(residual, restriction, pattern, cell_aggregate, block_inverse, off_blocks, op_pattern):
    turned = residual.transpose(1, 0, 2)
    pat = pattern.reshape(384, LANES)
    vmem = pl.BlockSpec(memory_space=pltpu.VMEM)
    hbm = pl.BlockSpec(memory_space=pltpu.HBM)
    msg = pltpu.VMEM((CHUNKS, ND, 8, LANES), F32)
    plane = pltpu.VMEM((NI * W, LANES), F32)
    edge = pltpu.VMEM((2, 3, 3, 8, LANES), F32)
    x, y = pl.pallas_call(
        coarse_kernel,
        out_shape=(
            jax.ShapeDtypeStruct((NI * W, LANES), F32),
            jax.ShapeDtypeStruct((NK * W, LANES), F32),
        ),
        in_specs=[hbm] * 7,
        out_specs=(vmem, vmem),
        scratch_shapes=[
            pltpu.VMEM((3, NQ, FPA * AGG), F32),
            pltpu.VMEM((3, 3, FPA * AGG), F32),
            pltpu.VMEM((384, LANES), jnp.int32),
            pltpu.VMEM((NI, LANES), jnp.int32),
            pltpu.VMEM((9, NI, LANES), F32),
            pltpu.VMEM((36, NI, LANES), F32),
            pltpu.VMEM((4, NI, LANES), jnp.int32),
            plane,
            msg,
            msg,
            msg,
            msg,
            pltpu.VMEM((AGG, LANES), F32),
            plane,
            pltpu.VMEM((3, (NI + 2) * W, LANES), F32),
            edge,
            edge,
            pltpu.VMEM((2, 3, 8, LANES), F32),
            pltpu.VMEM((36, NI, LANES), F32),
            pltpu.VMEM((2, 9, 8, LANES), F32),
            pltpu.VMEM((2, 9, 8, LANES), F32),
            pltpu.VMEM((NI, LANES), jnp.int32),
            pltpu.VMEM((NI, LANES), jnp.int32),
            pltpu.VMEM((ND, LANES), jnp.int32),
            pltpu.SMEM((NI, LANES), jnp.int32),
            pltpu.SMEM((ND, LANES), jnp.int32),
            pltpu.SemaphoreType.DMA((2, CHUNKS, FPA)),
            pltpu.SemaphoreType.DMA((7,)),
            pltpu.SemaphoreType.DMA((CHUNKS,)),
            pltpu.SemaphoreType.DMA((CHUNKS,)),
            pltpu.SemaphoreType.DMA((CHUNKS,)),
            pltpu.SemaphoreType.DMA((CHUNKS,)),
            pltpu.SemaphoreType.DMA((3, 4)),
            pltpu.SemaphoreType.DMA((3, 4)),
        ],
        compiler_params=pltpu.CompilerParams(
            collective_id=0, has_side_effects=True, vmem_limit_bytes=46 * 1024 * 1024
        ),
    )(
        *[
            pltpu.with_memory_space_constraint(x, pltpu.HBM)
            for x in (
                turned,
                restriction,
                pat,
                cell_aggregate,
                block_inverse.reshape(9, NI, LANES),
                off_blocks.reshape(36, NI, LANES),
                op_pattern,
            )
        ]
    )
    fine, planes = pl.pallas_call(
        prolong_kernel,
        grid=(FPA,),
        out_shape=(
            jax.ShapeDtypeStruct((3, NQ, FPA * AGG), F32),
            jax.ShapeDtypeStruct((NQ * 3 * NI, LANES), F32),
        ),
        in_specs=[
            vmem,
            vmem,
            pl.BlockSpec((3, 3, AGG), lambda p: (0, 0, p)),
            pl.BlockSpec((NK, LANES), lambda p: (p, 0)),
        ],
        out_specs=(
            pl.BlockSpec((3, NQ, AGG), lambda p: (0, 0, p)),
            pl.BlockSpec((NQ * 3 * NI, LANES), lambda p: (0, 0)),
        ),
        compiler_params=pltpu.CompilerParams(vmem_limit_bytes=16 * 1024 * 1024),
    )(y, x, restriction, pat)
    return planes.reshape(NQ, 3, NI, LANES), fine.transpose(1, 0, 2)


def solution(mesh):
    in_specs = (
        P(None, None, ("row", "col")),
        P(None, None, ("row", "col")),
        P(("row", "col")),
        P("row", "col"),
        P(None, None, "row", "col"),
        P(None, None, None, "row", "col"),
        P(None, "row", "col"),
    )
    out_specs = (P(None, None, "row", "col"), P(None, None, ("row", "col")))
    return jax.shard_map(body, mesh=mesh, in_specs=in_specs, out_specs=out_specs, check_vma=False)
```

```python
import functools

import jax
import jax.numpy as jnp
from jax import lax
from jax.experimental import pallas as pl
from jax.experimental.pallas import tpu as pltpu
from jax.sharding import PartitionSpec as P

MESH = pl.DeviceIdType.MESH
ND = 128
NQ = 16
NI = 48
NK = 48
W = 48
AGG = 6144
FPA = 8
CHUNKS = 3
LANES = 128
F32 = jnp.float32


def me_index():
    return lax.axis_index("row") * 8 + lax.axis_index("col")


def lane_ids():
    return lax.broadcasted_iota(jnp.int32, (8, LANES), 1)


def bcast_row(ref, *idx):
    return jnp.broadcast_to(ref[idx], (8, LANES))


def each_peer(visit):
    row, col = lax.axis_index("row"), lax.axis_index("col")
    cols = [lax.rem(col + d, 8) for d in range(8)]
    for other in cols[1:]:
        visit(row, other)

    def one(d, c):
        there = lax.rem(row + d, 16)
        for other in cols:
            visit(there, other)
        return c

    lax.fori_loop(1, 16, one, 0)


def start_barrier():
    bar = pltpu.get_barrier_semaphore()
    each_peer(
        lambda row, col: pl.semaphore_signal(
            bar, inc=1, device_id=(row, col), device_id_type=MESH
        )
    )


def end_barrier():
    pl.semaphore_wait(pltpu.get_barrier_semaphore(), ND - 1)


def send_chunk(S, R, b, ssem, rsem):
    dst = R.at[b, me_index(), pl.ds(0, 6)]

    def visit(row, col):
        pltpu.make_async_remote_copy(
            S.at[b, row * 8 + col, pl.ds(0, 6)],
            dst,
            ssem.at[b],
            rsem.at[b],
            device_id=(row, col),
            device_id_type=MESH,
        ).start()

    each_peer(visit)


def wait_chunk(R, b, sem):
    block = R.at[b, pl.ds(0, ND - 1), pl.ds(0, 6)]
    pltpu.make_async_copy(block, block, sem.at[b]).wait()


def keep_own(S, R, b):
    me = me_index()
    R[b, me] = S[b, me]


def restrict_chunk(b, r, w, pat, A):
    def one(kk, c):
        k = b * 16 + kk
        acc = [[None] * 2 for _ in range(3)]
        for p in range(FPA):
            n = pl.multiple_of(p * AGG + k * LANES, LANES)
            there = bcast_row(pat, pl.ds(p * 48 + k, 1), slice(None)).astype(F32)
            here = [
                [r[j, qg * 8 : qg * 8 + 8, pl.ds(n, LANES)] * there for qg in range(2)]
                for j in range(3)
            ]
            for i in range(3):
                for j in range(3):
                    wij = jnp.broadcast_to(w[i, j : j + 1, pl.ds(n, LANES)], (8, LANES))
                    for qg in range(2):
                        term = wij * here[j][qg]
                        acc[i][qg] = term if acc[i][qg] is None else acc[i][qg] + term
        for i in range(3):
            for qg in range(2):
                at = pl.multiple_of(k * W + i * 16 + qg * 8, 8)
                A[pl.ds(at, 8), :] = acc[i][qg]
        return c

    lax.fori_loop(0, 16, one, 0)


def pack_chunk(b, A, S2d):
    for h in range(2):
        k8 = b * 16 + 8 * h
        six, seven = (k8 + 6) * W, (k8 + 7) * W
        for m in range(3):
            at = (k8 + 2 * m) * W
            head = A[at : at + 96, :]
            if m == 0:
                tail = [A[six : six + 32, :]]
            elif m == 1:
                tail = [A[seven : seven + 32, :]]
            else:
                tail = [A[six + 32 : six + 48, :], A[seven + 32 : seven + 48, :]]
            turned = jnp.concatenate([head] + tail, axis=0).T
            for t0 in range(16):
                rows = pl.ds(b * 1024 + t0 * 64 + 2 * m + h, 8, stride=8)
                S2d[rows, :] = turned[t0 * 8 : t0 * 8 + 8, :]


def unfold_chunk(b, R2d):
    lane = lane_ids()

    def one(fb, c):
        for base, h in [(b * 1024 + (fb * 4 + u) * 64, h) for u in range(4) for h in range(2)]:
            x0 = R2d[pl.ds(base + h, 8, stride=8), :]
            x1 = R2d[pl.ds(base + 2 + h, 8, stride=8), :]
            x2 = R2d[pl.ds(base + 4 + h, 8, stride=8), :]
            six = jnp.where(lane < 32, pltpu.roll(x0, 32, 1), pltpu.roll(x2, 64, 1))
            seven = jnp.where(lane < 80, pltpu.roll(x1, 80, 1), pltpu.roll(x2, 96, 1))
            R2d[pl.ds(base + 6 + h, 8, stride=8), :] = jnp.where(lane < 48, six, seven)
        return c

    lax.fori_loop(0, 4, one, 0)


def index_tables(ca, slot_v, odd, inv_v):
    def one(blk, acc):
        rows = pl.ds(pl.multiple_of(blk * 8, 8), 8)
        pair = lax.shift_right_logical(ca[rows, :], 7)
        owner = lax.shift_right_logical(lax.shift_right_logical(pair, 4) * 171, 9)
        local = pair - owner * NK
        bit = [lax.shift_right_logical(local, n) & 1 for n in range(4)]
        chunk = lax.shift_right_logical(local, 4)
        at = chunk * 1024 + owner * 8 + (bit[2] * 2 + bit[1]) * 2 + bit[3]
        slot_v[rows, :] = jnp.clip(at, 0, CHUNKS * 1024 - 1)
        odd[rows, :] = bit[0]
        for u in range(8):
            who = jnp.broadcast_to(owner[u : u + 1], (ND, LANES))
            by_owner = (who == lax.broadcasted_iota(jnp.int32, (ND, LANES), 0)).astype(F32)
            which = jnp.broadcast_to(local[u : u + 1], (NK, LANES))
            here = which == lax.broadcasted_iota(jnp.int32, (NK, LANES), 0)
            column = lax.broadcasted_iota(jnp.int32, (NK, LANES), 1).astype(F32)
            line = (blk * 8 + u).astype(F32)
            cells = jnp.concatenate(
                [jnp.where(here, column, 0.0), jnp.where(here, line, 0.0)], axis=0
            )
            acc = acc + lax.dot_general(
                by_owner.astype(jnp.bfloat16),
                cells.astype(jnp.bfloat16),
                (((1,), (1,)), ((), ())),
                preferred_element_type=F32,
            )
        return acc

    acc = lax.fori_loop(0, NI // 8, one, jnp.zeros((ND, 2 * NK), F32))
    cell = (acc[:, NK:] * LANES + acc[:, :NK]).astype(jnp.int32)
    inv_v[:, 0:NK] = jnp.clip(cell, 0, AGG - 1)


def gather_rows(slot, R2d, G):
    def some(row, c):
        base = pl.multiple_of(row * LANES, LANES)
        for u in range(LANES):
            G[pl.ds(base + u, 1), :] = R2d[pl.ds(slot[row, u], 1), :]
        return c

    lax.fori_loop(0, NI, some, 0)


def solve_block(binv, row, total):
    out = []
    for i in range(3):
        acc = None
        for j in range(3):
            coef = bcast_row(binv, i * 3 + j, pl.ds(row, 1), slice(None))
            terms = [coef * total[j][qg] for qg in range(2)]
            acc = terms if acc is None else [x + y for x, y in zip(acc, terms)]
        out.append(acc)
    return out


def cells_to_planes(G, odd, rhs, binv, X):
    def one(blk, c):
        for u in range(8):
            row = blk * 8 + u
            base = pl.multiple_of(row * W, 8)
            turned = G[pl.ds(pl.multiple_of(row * LANES, LANES), LANES), :].T
            is_odd = bcast_row(odd, pl.ds(row, 1), slice(None)) == 1
            total = [[None] * 2 for _ in range(3)]
            for v in range(6):
                here = jnp.where(
                    is_odd, turned[W + v * 8 : W + v * 8 + 8, :], turned[v * 8 : v * 8 + 8, :]
                )
                rhs[pl.ds(base + v * 8, 8), :] = here
                total[v // 2][v % 2] = here
            new = solve_block(binv, row, total)
            for v in range(6):
                X[0, pl.ds(base + W + v * 8, 8), :] = new[v // 2][v % 2]
        return c

    lax.fori_loop(0, NI // 8, one, 0)


def couplings(off, opat, binv, coup, pc, pb):
    def couple(blk, c):
        at = pl.ds(pl.multiple_of(blk * 8, 8), 8)
        for d in range(4):
            there = opat[d, at, :].astype(F32)
            for e in range(9):
                coup[d * 9 + e, at, :] = off[d * 9 + e, at, :] * there
        return c

    lax.fori_loop(0, NI // 8, couple, 0)

    def pack(e, c):
        for blk in range(3):
            for src, plane, keep in (
                (coup, 18 + e, (0,)),
                (coup, 27 + e, (1,)),
                (binv, e, (0, 1)),
            ):
                parts = [
                    bcast_row(src, plane, slice(blk * 16 + n, blk * 16 + n + 1), slice(None))
                    for n in range(16)
                ]
                turned = jnp.concatenate(parts, axis=0).T
                for side in keep:
                    line = turned[0:1] if side == 0 else turned[LANES - 1 : LANES]
                    dst = pb if src is binv else pc
                    for qg in range(2):
                        dst[side, e, qg * 3 + blk : qg * 3 + blk + 1, :] = line
        return c

    lax.fori_loop(0, 9, pack, 0)

    def mask(e, c):
        lane = lax.broadcasted_iota(jnp.int32, (NI, LANES), 1)
        coup[18 + e] = jnp.where(lane == 0, 0.0, coup[18 + e])
        coup[27 + e] = jnp.where(lane == LANES - 1, 0.0, coup[27 + e])
        return c

    lax.fori_loop(0, 9, mask, 0)


def pack_edges(s, X, E):
    for blk in range(3):
        for v in range(6):
            parts = [
                X[s, (blk * 16 + n + 1) * W + v * 8 : (blk * 16 + n + 1) * W + v * 8 + 8, :]
                for n in range(16)
            ]
            turned = jnp.concatenate(parts, axis=0).T
            at = v % 2 * 3 + blk
            E[0, s, v // 2, at : at + 1, :] = turned[0:1]
            E[1, s, v // 2, at : at + 1, :] = turned[LANES - 1 : LANES]


def halo_copies(s, X, E, H, hs, hr):
    row, col = lax.axis_index("row"), lax.axis_index("col")
    own_first = X.at[s, pl.ds(W, W)]
    own_last = X.at[s, pl.ds(NI * W, W)]
    above = X.at[s, pl.ds(0, W)]
    below = X.at[s, pl.ds((NI + 1) * W, W)]
    table = [
        (row > 0, row < 15, own_first, below, (row - 1, col)),
        (row < 15, row > 0, own_last, above, (row + 1, col)),
        (col > 0, col < 7, E.at[0, s], H.at[1, s], (row, col - 1)),
        (col < 7, col > 0, E.at[1, s], H.at[0, s], (row, col + 1)),
    ]
    return [
        (
            sends,
            receives,
            pltpu.make_async_remote_copy(
                src, dst, hs.at[s, n], hr.at[s, n], device_id=dev, device_id_type=MESH
            ),
            dst,
        )
        for n, (sends, receives, src, dst, dev) in enumerate(table)
    ]


def start_copies(copies):
    for sends, _, copy, _ in copies:
        pl.when(sends)(copy.start)


def finish_copies(copies):
    for _, receives, copy, dst in copies:
        pl.when(receives)(copy.wait_recv)

        def clear(dst=dst):
            dst[...] = jnp.zeros(dst.shape, F32)

        pl.when(jnp.logical_not(receives))(clear)


def sweep_row(s, row, rhs, binv, coup, X, new_at):
    base = pl.multiple_of(row * W, 8)

    def at(v):
        return pl.ds(base + v * 8, 8)

    own = [X[s, at(v + 6), :] for v in range(6)]
    left = [pltpu.roll(x, 1, 1) for x in own]
    right = [pltpu.roll(x, LANES - 1, 1) for x in own]
    total = [[rhs[at(j * 2 + qg), :] for qg in range(2)] for j in range(3)]
    for d in range(4):
        for k in range(3):
            near = []
            for qg in range(2):
                v = k * 2 + qg
                if d == 0:
                    near.append(X[s, at(v), :])
                elif d == 1:
                    near.append(X[s, at(v + 12), :])
                else:
                    near.append((left if d == 2 else right)[v])
            for j in range(3):
                coef = bcast_row(coup, d * 9 + j * 3 + k, pl.ds(row, 1), slice(None))
                for qg in range(2):
                    total[j][qg] = total[j][qg] - coef * near[qg]
    new = solve_block(binv, row, total)
    for v in range(6):
        new_at(row, v)[...] = new[v // 2][v % 2]


def correct_edges(s, H, pc, pb, D):
    for side in range(2):
        push = []
        for j in range(3):
            acc = None
            for k in range(3):
                term = pc[side, j * 3 + k] * H[side, s, k]
                acc = term if acc is None else acc + term
            push.append(acc)
        for i in range(3):
            acc = None
            for j in range(3):
                term = pb[side, i * 3 + j] * push[j]
                acc = term if acc is None else acc + term
            D[side, i] = -acc


def add_edges(blk, D, new_at):
    sub = lax.broadcasted_iota(jnp.int32, (8, LANES), 0)
    zero = jnp.zeros((LANES - 16, LANES), F32)
    for v in range(6):
        at = v % 2 * 3 + blk
        first = jnp.where(sub == 0, bcast_row(D, 0, v // 2, slice(at, at + 1), slice(None)), 0.0)
        last = jnp.where(sub == 7, bcast_row(D, 1, v // 2, slice(at, at + 1), slice(None)), 0.0)
        turned = jnp.concatenate([first, zero, last], axis=0).T
        for n in range(16):
            ref = new_at(blk * 16 + n, v)
            ref[...] = ref[...] + turned[n * 8 : n * 8 + 8]


def planes_to_cells(last, G):
    def one(blk, c):
        for u in range(8):
            row = blk * 8 + u
            x = last[pl.ds(pl.multiple_of(row * W, 8), W), :]
            turned = jnp.concatenate([x, x], axis=0).T
            G[pl.ds(pl.multiple_of(row * LANES, LANES), LANES), 0 : 2 * W] = turned
        return c

    lax.fori_loop(0, NI // 8, one, 0)


def return_all(inv, G, S2, S2_rows, R2, ssem, rsem):
    row, col = lax.axis_index("row"), lax.axis_index("col")
    cols = [lax.rem(col + d, 8) for d in range(8)]
    me = me_index()
    low = lax.broadcasted_iota(jnp.int32, (1, LANES), 1) < W
    lane = lane_ids()

    def collect(b, there):
        for u in range(8):
            f = there * 8 + u
            for rr in range(8):
                k = b * 16 + rr % 2 * 8 + rr // 2 * 2
                even = G[pl.ds(inv[f, k], 1), :]
                odd = G[pl.ds(inv[f, k + 1], 1), :]
                S2_rows[pl.ds(b * 1024 + f * 8 + rr, 1), :] = jnp.where(low, even, odd)

    def fold_start(b, there):
        base = b * 1024 + there * 64
        done = []
        for h in range(2):
            d = S2_rows[pl.ds(base + 6 + h, 8, stride=8), :]
            for m, moved in enumerate(
                (
                    pltpu.roll(d, 96, 1),
                    pltpu.roll(d, 48, 1),
                    jnp.where(lane < 112, pltpu.roll(d, 64, 1), pltpu.roll(d, 32, 1)),
                )
            ):
                rows = pl.ds(base + 2 * m + h, 8, stride=8)
                done.append((rows, jnp.where(lane >= 96, moved, S2_rows[rows, :])))
        return done

    def fold_end(done):
        for rows, x in done:
            S2_rows[rows, :] = x

    def send(b, there):
        def one(c):
            pltpu.make_async_remote_copy(
                S2.at[b, there * 8 + c, pl.ds(0, 6)],
                R2.at[b, me, pl.ds(0, 6)],
                ssem.at[b],
                rsem.at[b],
                device_id=(there, c),
                device_id_type=MESH,
            ).start()

        for c in cols[1:]:
            one(c)
        pl.when(there != row)(lambda: one(cols[0]))

    def peer(d):
        return lax.rem(row + d, 16)

    for b in range(CHUNKS):
        collect(b, peer(0))
        done = fold_start(b, peer(0))
        if b > 0:
            send(b - 1, peer(15))
        collect(b, peer(1))
        fold_end(done)

        def step(d, c, b=b):
            done = fold_start(b, peer(d - 1))
            collect(b, peer(d))
            fold_end(done)
            send(b, peer(d - 2))
            return c

        lax.fori_loop(2, 16, step, 0)
        fold_end(fold_start(b, peer(15)))
        send(b, peer(14))
        R2[b, me] = S2[b, me]
    send(CHUNKS - 1, peer(15))


def spread_chunk(b, R2d, Y):
    for h in range(2):
        k8 = b * 16 + 8 * h
        six, seven = (k8 + 6) * W, (k8 + 7) * W
        for m in range(3):
            parts = [
                R2d[pl.ds(b * 1024 + t0 * 64 + 2 * m + h, 8, stride=8), :] for t0 in range(16)
            ]
            turned = jnp.concatenate(parts, axis=0).T
            at = (k8 + 2 * m) * W
            Y[at : at + 96, :] = turned[0:96]
            if m == 0:
                Y[six : six + 32, :] = turned[96:128]
            elif m == 1:
                Y[seven : seven + 32, :] = turned[96:128]
            else:
                Y[six + 32 : six + 48, :] = turned[96:112]
                Y[seven + 32 : seven + 48, :] = turned[112:128]


def coarse_kernel(
    r_hbm,
    w_hbm,
    pat_hbm,
    ca_hbm,
    binv_hbm,
    off_hbm,
    opat_hbm,
    x_out,
    Y,
    r,
    w,
    pat,
    ca,
    binv,
    off,
    opat,
    A,
    S,
    R,
    S2,
    R2,
    G,
    rhs,
    X,
    E,
    H,
    D,
    coup,
    pc,
    pb,
    slot_v,
    odd,
    inv_v,
    slot,
    inv,
    load_sem,
    small_sem,
    s1,
    r1,
    s2,
    r2,
    hs,
    hr,
):
    small = [
        pltpu.make_async_copy(x, y, small_sem.at[n])
        for n, (x, y) in enumerate(
            [
                (pat_hbm, pat),
                (ca_hbm, ca),
                (binv_hbm, binv),
                (off_hbm, off),
                (opat_hbm, opat),
                (slot_v, slot),
                (inv_v, inv),
            ]
        )
    ]
    loads = []
    for b in range(CHUNKS):
        for p in range(FPA):
            n = pl.ds(p * AGG + b * 2048, 2048)
            loads.append((b, r_hbm.at[:, :, n], r.at[:, :, n], load_sem.at[0, b, p]))
            loads.append((b, w_hbm.at[:, :, n], w.at[:, :, n], load_sem.at[1, b, p]))
    loads = [(b, pltpu.make_async_copy(x, y, z)) for b, x, y, z in loads]
    def load(b):
        for at, copy in loads:
            if at == b:
                copy.start()

    small[0].start()
    load(0)
    start_barrier()
    load(1)

    S_rows, R_rows = S.reshape(CHUNKS * 1024, LANES), R.reshape(CHUNKS * 1024, LANES)
    S2_rows, R2_rows = S2.reshape(CHUNKS * 1024, LANES), R2.reshape(CHUNKS * 1024, LANES)
    small[0].wait()
    for b in range(CHUNKS):
        for at, copy in loads:
            if at == b:
                copy.wait()
        if b == 0:
            load(2)
            for copy in small[1:5]:
                copy.start()
        restrict_chunk(b, r, w, pat, A)
        pack_chunk(b, A, S_rows)
        if b == 0:
            end_barrier()
        send_chunk(S, R, b, s1, r1)
        keep_own(S, R, b)

    for copy in small[1:5]:
        copy.wait()
    E[...] = jnp.zeros(E.shape, F32)
    pc[...] = jnp.zeros(pc.shape, F32)
    pb[...] = jnp.zeros(pb.shape, F32)
    inv_v[...] = jnp.zeros(inv_v.shape, jnp.int32)
    index_tables(ca, slot_v, odd, inv_v)
    small[5].start()
    small[6].start()
    couplings(off, opat, binv, coup, pc, pb)
    small[5].wait()
    small[6].wait()

    for b in range(CHUNKS):
        wait_chunk(R, b, r1)
        unfold_chunk(b, R_rows)
    gather_rows(slot, R_rows, G)
    cells_to_planes(G, odd, rhs, binv, X)

    halos = [halo_copies(s, X, E, H, hs, hr) for s in range(3)]
    start_copies(halos[0][:2])
    pack_edges(0, X, E)
    start_copies(halos[0][2:])
    for s in range(3):
        if s < 2:

            def new_at(row, v, s=s):
                return X.at[s + 1, pl.ds(pl.multiple_of(row * W + W + v * 8, 8), 8)]
        else:

            def new_at(row, v):
                return x_out.at[pl.ds(pl.multiple_of(row * W + v * 8, 8), 8)]

        def inner(two, c, s=s, new_at=new_at):
            for u in range(2):
                sweep_row(s, 1 + two * 2 + u, rhs, binv, coup, X, new_at)
            return c

        lax.fori_loop(0, (NI - 2) // 2, inner, 0)
        finish_copies(halos[s][:2])
        lax.fori_loop(
            0,
            2,
            lambda n, c, s=s, new_at=new_at: (
                sweep_row(s, n * (NI - 1), rhs, binv, coup, X, new_at),
                c,
            )[1],
            0,
        )
        finish_copies(halos[s][2:])
        correct_edges(s, H, pc, pb, D)
        add_edges(0, D, new_at)
        add_edges(2, D, new_at)
        if s < 2:
            start_copies(halos[s + 1][:2])
        add_edges(1, D, new_at)
        if s < 2:
            pack_edges(s + 1, X, E)
            start_copies(halos[s + 1][2:])

    planes_to_cells(x_out, G)
    return_all(inv, G, S2, S2_rows, R2, s2, r2)
    for b in range(CHUNKS):
        wait_chunk(R2, b, r2)
        spread_chunk(b, R2_rows, Y)

    for b in range(CHUNKS):
        wait_chunk(R, b, s1)
        wait_chunk(R, b, s2)
    for copies in halos:
        for sends, _, copy, _ in copies:
            pl.when(sends)(copy.wait_send)


def prolong_kernel(y, x, w, pat, out, planes_out, fine, planes, sem, psem):
    def line(row, c):
        for v in range(6):
            at = (v % 2 * 24 + v // 2) * NI + row
            planes[pl.ds(at, 8, stride=3 * NI), :] = x[pl.ds(row * W + v * 8, 8), :]
        return c

    lax.fori_loop(0, NI, line, 0)
    plane_copy = pltpu.make_async_copy(planes, planes_out, psem)
    plane_copy.start()

    def copies(p):
        n = pl.ds(pl.multiple_of(p * AGG, AGG), AGG)
        return [
            pltpu.make_async_copy(fine.at[j, :, n], out.at[j, :, n], sem.at[p, j])
            for j in range(3)
        ]

    def block(p, c):
        def some(blk, c):
            for u in range(4):
                k = blk * 4 + u
                at = pl.ds(pl.multiple_of(p * AGG + k * LANES, LANES), LANES)
                base = pl.multiple_of(k * W, 8)
                there = bcast_row(pat, pl.ds(p * NK + k, 1), slice(None)).astype(F32)
                src = [
                    [y[pl.ds(base + i * 16 + qg * 8, 8), :] * there for qg in range(2)]
                    for i in range(3)
                ]
                for j in range(3):
                    acc = None
                    for i in range(3):
                        wij = jnp.broadcast_to(w[i, j : j + 1, at], (8, LANES))
                        terms = [wij * src[i][qg] for qg in range(2)]
                        acc = terms if acc is None else [a + z for a, z in zip(acc, terms)]
                    for qg in range(2):
                        fine[j, qg * 8 : qg * 8 + 8, at] = acc[qg]
            return c

        lax.fori_loop(0, NK // 4, some, 0)
        for copy in copies(p):
            copy.start()
        return c

    lax.fori_loop(0, FPA, block, 0)
    plane_copy.wait()

    def finish(p, c):
        for copy in copies(p):
            copy.wait()
        return c

    lax.fori_loop(0, FPA, finish, 0)


def body(residual, restriction, pattern, cell_aggregate, block_inverse, off_blocks, op_pattern):
    turned = residual.transpose(1, 0, 2)
    pat = pattern.reshape(384, LANES)
    vmem = pl.BlockSpec(memory_space=pltpu.VMEM)
    hbm = pl.BlockSpec(memory_space=pltpu.HBM)
    msg = pltpu.VMEM((CHUNKS, ND, 8, LANES), F32)
    plane = pltpu.VMEM((NI * W, LANES), F32)
    edge = pltpu.VMEM((2, 3, 3, 8, LANES), F32)
    x, y = pl.pallas_call(
        coarse_kernel,
        out_shape=(
            jax.ShapeDtypeStruct((NI * W, LANES), F32),
            jax.ShapeDtypeStruct((NK * W, LANES), F32),
        ),
        in_specs=[hbm] * 7,
        out_specs=(vmem, vmem),
        scratch_shapes=[
            pltpu.VMEM((3, NQ, FPA * AGG), F32),
            pltpu.VMEM((3, 3, FPA * AGG), F32),
            pltpu.VMEM((384, LANES), jnp.int32),
            pltpu.VMEM((NI, LANES), jnp.int32),
            pltpu.VMEM((9, NI, LANES), F32),
            pltpu.VMEM((36, NI, LANES), F32),
            pltpu.VMEM((4, NI, LANES), jnp.int32),
            plane,
            msg,
            msg,
            msg,
            msg,
            pltpu.VMEM((AGG, LANES), F32),
            plane,
            pltpu.VMEM((3, (NI + 2) * W, LANES), F32),
            edge,
            edge,
            pltpu.VMEM((2, 3, 8, LANES), F32),
            pltpu.VMEM((36, NI, LANES), F32),
            pltpu.VMEM((2, 9, 8, LANES), F32),
            pltpu.VMEM((2, 9, 8, LANES), F32),
            pltpu.VMEM((NI, LANES), jnp.int32),
            pltpu.VMEM((NI, LANES), jnp.int32),
            pltpu.VMEM((ND, LANES), jnp.int32),
            pltpu.SMEM((NI, LANES), jnp.int32),
            pltpu.SMEM((ND, LANES), jnp.int32),
            pltpu.SemaphoreType.DMA((2, CHUNKS, FPA)),
            pltpu.SemaphoreType.DMA((7,)),
            pltpu.SemaphoreType.DMA((CHUNKS,)),
            pltpu.SemaphoreType.DMA((CHUNKS,)),
            pltpu.SemaphoreType.DMA((CHUNKS,)),
            pltpu.SemaphoreType.DMA((CHUNKS,)),
            pltpu.SemaphoreType.DMA((3, 4)),
            pltpu.SemaphoreType.DMA((3, 4)),
        ],
        compiler_params=pltpu.CompilerParams(
            collective_id=0, has_side_effects=True, vmem_limit_bytes=46 * 1024 * 1024
        ),
    )(
        *[
            pltpu.with_memory_space_constraint(x, pltpu.HBM)
            for x in (
                turned,
                restriction,
                pat,
                cell_aggregate,
                block_inverse.reshape(9, NI, LANES),
                off_blocks.reshape(36, NI, LANES),
                op_pattern,
            )
        ]
    )
    fine, planes = pl.pallas_call(
        prolong_kernel,
        out_shape=(
            jax.ShapeDtypeStruct((3, NQ, FPA * AGG), F32),
            jax.ShapeDtypeStruct((NQ * 3 * NI, LANES), F32),
        ),
        in_specs=[vmem] * 4,
        out_specs=(hbm, hbm),
        scratch_shapes=[
            pltpu.VMEM((3, NQ, FPA * AGG), F32),
            pltpu.VMEM((NQ * 3 * NI, LANES), F32),
            pltpu.SemaphoreType.DMA((FPA, 3)),
            pltpu.SemaphoreType.DMA,
        ],
        compiler_params=pltpu.CompilerParams(vmem_limit_bytes=24 * 1024 * 1024),
    )(y, x, restriction, pat)
    return planes.reshape(NQ, 3, NI, LANES), fine.transpose(1, 0, 2)


def solution(mesh):
    in_specs = (
        P(None, None, ("row", "col")),
        P(None, None, ("row", "col")),
        P(("row", "col")),
        P("row", "col"),
        P(None, None, "row", "col"),
        P(None, None, None, "row", "col"),
        P(None, "row", "col"),
    )
    out_specs = (P(None, None, "row", "col"), P(None, None, ("row", "col")))
    return jax.shard_map(body, mesh=mesh, in_specs=in_specs, out_specs=out_specs, check_vma=False)
```

```python
import functools

import jax
import jax.numpy as jnp
from jax import lax
from jax.experimental import pallas as pl
from jax.experimental.pallas import tpu as pltpu
from jax.sharding import PartitionSpec as P

MESH = pl.DeviceIdType.MESH
ND = 128
NQ = 16
NI = 48
NK = 48
W = 48
AGG = 6144
FPA = 8
CHUNKS = 3
LANES = 128
F32 = jnp.float32


def me_index():
    return lax.axis_index("row") * 8 + lax.axis_index("col")


def lane_ids():
    return lax.broadcasted_iota(jnp.int32, (8, LANES), 1)


def bcast_row(ref, *idx):
    return jnp.broadcast_to(ref[idx], (8, LANES))


def peer_row(row, far, near):
    z = lax.rem(row // 4 + far, 4)
    return z * 4 + lax.rem(lax.rem(row, 4) + near, 4)


def each_peer(visit):
    row, col = lax.axis_index("row"), lax.axis_index("col")
    cols = [lax.rem(col + d, 8) for d in (2, 6, 1, 3, 5, 7, 4, 0)]
    for far in (2, 1, 3, 0):

        def one(n, c, far=far):
            there = peer_row(row, far, 3 - n)
            for other in cols:
                visit(there, other)
            return c

        lax.fori_loop(0, 4 if far else 3, one, 0)
    for other in cols[:-1]:
        visit(row, other)


def start_barrier():
    bar = pltpu.get_barrier_semaphore()
    each_peer(
        lambda row, col: pl.semaphore_signal(
            bar, inc=1, device_id=(row, col), device_id_type=MESH
        )
    )


def end_barrier():
    pl.semaphore_wait(pltpu.get_barrier_semaphore(), ND - 1)


def send_chunk(S, R, b, ssem, rsem):
    dst = R.at[b, me_index(), pl.ds(0, 6)]

    def visit(row, col):
        pltpu.make_async_remote_copy(
            S.at[b, row * 8 + col, pl.ds(0, 6)],
            dst,
            ssem.at[b],
            rsem.at[b],
            device_id=(row, col),
            device_id_type=MESH,
        ).start()

    each_peer(visit)


def wait_chunk(R, b, sem):
    block = R.at[b, pl.ds(0, ND - 1), pl.ds(0, 6)]
    pltpu.make_async_copy(block, block, sem.at[b]).wait()


def keep_own(S, R, b):
    me = me_index()
    R[b, me] = S[b, me]


def restrict_chunk(b, r, w, pat, A):
    def one(kk, c):
        k = b * 16 + kk
        acc = [[None] * 2 for _ in range(3)]
        for p in range(FPA):
            n = pl.multiple_of(p * AGG + k * LANES, LANES)
            there = bcast_row(pat, pl.ds(p * 48 + k, 1), slice(None)).astype(F32)
            here = [
                [r[j, qg * 8 : qg * 8 + 8, pl.ds(n, LANES)] * there for qg in range(2)]
                for j in range(3)
            ]
            for i in range(3):
                for j in range(3):
                    wij = jnp.broadcast_to(w[i, j : j + 1, pl.ds(n, LANES)], (8, LANES))
                    for qg in range(2):
                        term = wij * here[j][qg]
                        acc[i][qg] = term if acc[i][qg] is None else acc[i][qg] + term
        for i in range(3):
            for qg in range(2):
                at = pl.multiple_of(k * W + i * 16 + qg * 8, 8)
                A[pl.ds(at, 8), :] = acc[i][qg]
        return c

    lax.fori_loop(0, 16, one, 0)


def pack_chunk(b, A, S2d):
    for h in range(2):
        k8 = b * 16 + 8 * h
        six, seven = (k8 + 6) * W, (k8 + 7) * W
        for m in range(3):
            at = (k8 + 2 * m) * W
            head = A[at : at + 96, :]
            if m == 0:
                tail = [A[six : six + 32, :]]
            elif m == 1:
                tail = [A[seven : seven + 32, :]]
            else:
                tail = [A[six + 32 : six + 48, :], A[seven + 32 : seven + 48, :]]
            turned = jnp.concatenate([head] + tail, axis=0).T
            for t0 in range(16):
                rows = pl.ds(b * 1024 + t0 * 64 + 2 * m + h, 8, stride=8)
                S2d[rows, :] = turned[t0 * 8 : t0 * 8 + 8, :]


def unfold_chunk(b, R2d):
    lane = lane_ids()

    def one(fb, c):
        for base, h in [(b * 1024 + (fb * 8 + u) * 64, h) for u in range(8) for h in range(2)]:
            x0 = R2d[pl.ds(base + h, 8, stride=8), :]
            x1 = R2d[pl.ds(base + 2 + h, 8, stride=8), :]
            x2 = R2d[pl.ds(base + 4 + h, 8, stride=8), :]
            six = jnp.where(lane < 32, pltpu.roll(x0, 32, 1), pltpu.roll(x2, 64, 1))
            seven = jnp.where(lane < 80, pltpu.roll(x1, 80, 1), pltpu.roll(x2, 96, 1))
            R2d[pl.ds(base + 6 + h, 8, stride=8), :] = jnp.where(lane < 48, six, seven)
        return c

    lax.fori_loop(0, 2, one, 0)


def index_tables(ca, slot_v, odd, inv_v):
    def one(blk, acc):
        rows = pl.ds(pl.multiple_of(blk * 8, 8), 8)
        pair = lax.shift_right_logical(ca[rows, :], 7)
        owner = lax.shift_right_logical(lax.shift_right_logical(pair, 4) * 171, 9)
        local = pair - owner * NK
        bit = [lax.shift_right_logical(local, n) & 1 for n in range(4)]
        chunk = lax.shift_right_logical(local, 4)
        at = chunk * 1024 + owner * 8 + (bit[2] * 2 + bit[1]) * 2 + bit[3]
        slot_v[rows, :] = jnp.clip(at, 0, CHUNKS * 1024 - 1)
        odd[rows, :] = bit[0]
        for u in range(8):
            who = jnp.broadcast_to(owner[u : u + 1], (ND, LANES))
            by_owner = (who == lax.broadcasted_iota(jnp.int32, (ND, LANES), 0)).astype(F32)
            which = jnp.broadcast_to(local[u : u + 1], (NK, LANES))
            here = which == lax.broadcasted_iota(jnp.int32, (NK, LANES), 0)
            column = lax.broadcasted_iota(jnp.int32, (NK, LANES), 1).astype(F32)
            line = (blk * 8 + u).astype(F32)
            cells = jnp.concatenate(
                [jnp.where(here, column, 0.0), jnp.where(here, line, 0.0)], axis=0
            )
            acc = acc + lax.dot_general(
                by_owner.astype(jnp.bfloat16),
                cells.astype(jnp.bfloat16),
                (((1,), (1,)), ((), ())),
                preferred_element_type=F32,
            )
        return acc

    acc = lax.fori_loop(0, NI // 8, one, jnp.zeros((ND, 2 * NK), F32))
    cell = (acc[:, NK:] * LANES + acc[:, :NK]).astype(jnp.int32)
    inv_v[:, 0:NK] = jnp.clip(cell, 0, AGG - 1)


def solve_block(binv, row, total):
    out = []
    for i in range(3):
        acc = None
        for j in range(3):
            coef = bcast_row(binv, i * 3 + j, pl.ds(row, 1), slice(None))
            terms = [coef * total[j][qg] for qg in range(2)]
            acc = terms if acc is None else [x + y for x, y in zip(acc, terms)]
        out.append(acc)
    return out


def slot_copy(blk, n, slot_v, slot, sem):
    rows = pl.ds(pl.multiple_of(blk * 8, 8), 8)
    return pltpu.make_async_copy(slot_v.at[rows], slot.at[n], sem.at[n])


def gather_cells(slot_v, slot, sem, R2d, G, odd, rhs, binv, X):
    def finish(row):
        base = pl.multiple_of(row * W, 8)
        turned = G[pl.ds(pl.multiple_of(row * LANES, LANES), LANES), :].T
        is_odd = bcast_row(odd, pl.ds(row, 1), slice(None)) == 1
        total = [[None] * 2 for _ in range(3)]
        for v in range(6):
            here = jnp.where(
                is_odd, turned[W + v * 8 : W + v * 8 + 8, :], turned[v * 8 : v * 8 + 8, :]
            )
            rhs[pl.ds(base + v * 8, 8), :] = here
            total[v // 2][v % 2] = here
        new = solve_block(binv, row, total)
        for v in range(6):
            X[0, pl.ds(base + W + v * 8, 8), :] = new[v // 2][v % 2]

    def some(two, c):
        for n in range(2):
            blk = two * 2 + n
            slot_copy(blk, n, slot_v, slot, sem).wait()
            for u in range(8):
                row = blk * 8 + u
                base = pl.multiple_of(row * LANES, LANES)
                for k in range(LANES):
                    G[pl.ds(base + k, 1), :] = R2d[pl.ds(slot[n, u, k], 1), :]
                finish(row)
            pl.when(two < 2)(slot_copy(blk + 2, n, slot_v, slot, sem).start)
        return c

    lax.fori_loop(0, 3, some, 0)


def couplings(off, opat, binv, coup, pc, pb):
    def couple(blk, c):
        at = pl.ds(pl.multiple_of(blk * 8, 8), 8)
        for d in range(4):
            there = opat[d, at, :].astype(F32)
            for e in range(9):
                coup[d * 9 + e, at, :] = off[d * 9 + e, at, :] * there
        return c

    lax.fori_loop(0, NI // 8, couple, 0)

    def pack(e, c):
        for blk in range(3):
            for src, plane, keep in (
                (coup, 18 + e, (0,)),
                (coup, 27 + e, (1,)),
                (binv, e, (0, 1)),
            ):
                parts = [
                    bcast_row(src, plane, slice(blk * 16 + n, blk * 16 + n + 1), slice(None))
                    for n in range(16)
                ]
                turned = jnp.concatenate(parts, axis=0).T
                for side in keep:
                    line = turned[0:1] if side == 0 else turned[LANES - 1 : LANES]
                    dst = pb if src is binv else pc
                    for qg in range(2):
                        dst[side, e, qg * 3 + blk : qg * 3 + blk + 1, :] = line
        return c

    lax.fori_loop(0, 9, pack, 0)

    def mask(e, c):
        lane = lax.broadcasted_iota(jnp.int32, (NI, LANES), 1)
        coup[18 + e] = jnp.where(lane == 0, 0.0, coup[18 + e])
        coup[27 + e] = jnp.where(lane == LANES - 1, 0.0, coup[27 + e])
        return c

    lax.fori_loop(0, 9, mask, 0)


def pack_edges(s, X, E):
    for blk in range(3):
        for v in range(6):
            parts = [
                X[s, (blk * 16 + n + 1) * W + v * 8 : (blk * 16 + n + 1) * W + v * 8 + 8, :]
                for n in range(16)
            ]
            turned = jnp.concatenate(parts, axis=0).T
            at = v % 2 * 3 + blk
            E[0, s, v // 2, at : at + 1, :] = turned[0:1]
            E[1, s, v // 2, at : at + 1, :] = turned[LANES - 1 : LANES]


def halo_copies(s, X, E, H, hs, hr):
    row, col = lax.axis_index("row"), lax.axis_index("col")
    own_first = X.at[s, pl.ds(W, W)]
    own_last = X.at[s, pl.ds(NI * W, W)]
    above = X.at[s, pl.ds(0, W)]
    below = X.at[s, pl.ds((NI + 1) * W, W)]
    table = [
        (row > 0, row < 15, own_first, below, (row - 1, col)),
        (row < 15, row > 0, own_last, above, (row + 1, col)),
        (col > 0, col < 7, E.at[0, s], H.at[1, s], (row, col - 1)),
        (col < 7, col > 0, E.at[1, s], H.at[0, s], (row, col + 1)),
    ]
    return [
        (
            sends,
            receives,
            pltpu.make_async_remote_copy(
                src, dst, hs.at[s, n], hr.at[s, n], device_id=dev, device_id_type=MESH
            ),
            dst,
        )
        for n, (sends, receives, src, dst, dev) in enumerate(table)
    ]


def start_copies(copies):
    for sends, _, copy, _ in copies:
        pl.when(sends)(copy.start)


def finish_copies(copies):
    for _, receives, copy, dst in copies:
        pl.when(receives)(copy.wait_recv)

        def clear(dst=dst):
            dst[...] = jnp.zeros(dst.shape, F32)

        pl.when(jnp.logical_not(receives))(clear)


def sweep_row(s, row, rhs, binv, coup, X, new_at):
    base = pl.multiple_of(row * W, 8)

    def at(v):
        return pl.ds(base + v * 8, 8)

    own = [X[s, at(v + 6), :] for v in range(6)]
    left = [pltpu.roll(x, 1, 1) for x in own]
    right = [pltpu.roll(x, LANES - 1, 1) for x in own]
    total = [[rhs[at(j * 2 + qg), :] for qg in range(2)] for j in range(3)]
    for d in range(4):
        for k in range(3):
            near = []
            for qg in range(2):
                v = k * 2 + qg
                if d == 0:
                    near.append(X[s, at(v), :])
                elif d == 1:
                    near.append(X[s, at(v + 12), :])
                else:
                    near.append((left if d == 2 else right)[v])
            for j in range(3):
                coef = bcast_row(coup, d * 9 + j * 3 + k, pl.ds(row, 1), slice(None))
                for qg in range(2):
                    total[j][qg] = total[j][qg] - coef * near[qg]
    new = solve_block(binv, row, total)
    for v in range(6):
        new_at(row, v)[...] = new[v // 2][v % 2]


def correct_edges(s, H, pc, pb, D):
    for side in range(2):
        push = []
        for j in range(3):
            acc = None
            for k in range(3):
                term = pc[side, j * 3 + k] * H[side, s, k]
                acc = term if acc is None else acc + term
            push.append(acc)
        for i in range(3):
            acc = None
            for j in range(3):
                term = pb[side, i * 3 + j] * push[j]
                acc = term if acc is None else acc + term
            D[side, i] = -acc


def add_edges(blk, D, new_at):
    sub = lax.broadcasted_iota(jnp.int32, (8, LANES), 0)
    zero = jnp.zeros((LANES - 16, LANES), F32)
    for v in range(6):
        at = v % 2 * 3 + blk
        first = jnp.where(sub == 0, bcast_row(D, 0, v // 2, slice(at, at + 1), slice(None)), 0.0)
        last = jnp.where(sub == 7, bcast_row(D, 1, v // 2, slice(at, at + 1), slice(None)), 0.0)
        turned = jnp.concatenate([first, zero, last], axis=0).T
        for n in range(16):
            ref = new_at(blk * 16 + n, v)
            ref[...] = ref[...] + turned[n * 8 : n * 8 + 8]


def planes_to_cells(last, G):
    def one(blk, c):
        for u in range(16):
            row = blk * 16 + u
            x = last[pl.ds(pl.multiple_of(row * W, 8), W), :]
            turned = jnp.concatenate([x, x], axis=0).T
            G[pl.ds(pl.multiple_of(row * LANES, LANES), LANES), 0 : 2 * W] = turned
        return c

    lax.fori_loop(0, NI // 16, one, 0)


def return_all(inv, G, S2, S2_rows, R2, ssem, rsem):
    row, col = lax.axis_index("row"), lax.axis_index("col")
    cols = [lax.rem(col + d, 8) for d in range(8)]
    me = me_index()
    low = lax.broadcasted_iota(jnp.int32, (1, LANES), 1) < W
    lane = lane_ids()

    def collect(b, there):
        for u in range(8):
            f = there * 8 + u
            for rr in range(8):
                k = b * 16 + rr % 2 * 8 + rr // 2 * 2
                even = G[pl.ds(inv[f, k], 1), :]
                odd = G[pl.ds(inv[f, k + 1], 1), :]
                S2_rows[pl.ds(b * 1024 + f * 8 + rr, 1), :] = jnp.where(low, even, odd)

    def fold_start(b, there):
        base = b * 1024 + there * 64
        done = []
        for h in range(2):
            d = S2_rows[pl.ds(base + 6 + h, 8, stride=8), :]
            for m, moved in enumerate(
                (
                    pltpu.roll(d, 96, 1),
                    pltpu.roll(d, 48, 1),
                    jnp.where(lane < 112, pltpu.roll(d, 64, 1), pltpu.roll(d, 32, 1)),
                )
            ):
                rows = pl.ds(base + 2 * m + h, 8, stride=8)
                done.append((rows, jnp.where(lane >= 96, moved, S2_rows[rows, :])))
        return done

    def fold_end(done):
        for rows, x in done:
            S2_rows[rows, :] = x

    def send(b, there):
        def one(c):
            pltpu.make_async_remote_copy(
                S2.at[b, there * 8 + c, pl.ds(0, 6)],
                R2.at[b, me, pl.ds(0, 6)],
                ssem.at[b],
                rsem.at[b],
                device_id=(there, c),
                device_id_type=MESH,
            ).start()

        for c in cols[1:]:
            one(c)
        pl.when(there != row)(lambda: one(cols[0]))

    def peer(d):
        group = d // 4
        far = jnp.where(group == 0, 2, jnp.where(group == 1, 1, jnp.where(group == 2, 3, 0)))
        return peer_row(row, far, 3 - lax.rem(d, 4))

    for b in range(CHUNKS):
        collect(b, peer(0))
        done = fold_start(b, peer(0))
        if b > 0:
            send(b - 1, peer(15))
        collect(b, peer(1))
        fold_end(done)

        def step(d, c, b=b):
            done = fold_start(b, peer(d - 1))
            collect(b, peer(d))
            fold_end(done)
            send(b, peer(d - 2))
            return c

        lax.fori_loop(2, 16, step, 0)
        fold_end(fold_start(b, peer(15)))
        send(b, peer(14))
        R2[b, me] = S2[b, me]
    send(CHUNKS - 1, peer(15))


def spread_chunk(b, R2d, Y):
    for h in range(2):
        k8 = b * 16 + 8 * h
        six, seven = (k8 + 6) * W, (k8 + 7) * W
        for m in range(3):
            parts = [
                R2d[pl.ds(b * 1024 + t0 * 64 + 2 * m + h, 8, stride=8), :] for t0 in range(16)
            ]
            turned = jnp.concatenate(parts, axis=0).T
            at = (k8 + 2 * m) * W
            Y[at : at + 96, :] = turned[0:96]
            if m == 0:
                Y[six : six + 32, :] = turned[96:128]
            elif m == 1:
                Y[seven : seven + 32, :] = turned[96:128]
            else:
                Y[six + 32 : six + 48, :] = turned[96:112]
                Y[seven + 32 : seven + 48, :] = turned[112:128]


def coarse_kernel(
    r_hbm,
    w_hbm,
    pat_hbm,
    ca_hbm,
    binv_hbm,
    off_hbm,
    opat_hbm,
    x_out,
    Y,
    r,
    w,
    pat,
    ca,
    binv,
    off,
    opat,
    A,
    S,
    R,
    S2,
    R2,
    G,
    rhs,
    X,
    E,
    H,
    D,
    coup,
    pc,
    pb,
    slot_v,
    odd,
    inv_v,
    slot,
    inv,
    load_sem,
    small_sem,
    slot_sem,
    s1,
    r1,
    s2,
    r2,
    hs,
    hr,
):
    small = [
        pltpu.make_async_copy(x, y, small_sem.at[n])
        for n, (x, y) in enumerate(
            [
                (pat_hbm, pat),
                (ca_hbm, ca),
                (binv_hbm, binv),
                (off_hbm, off),
                (opat_hbm, opat),
                (inv_v, inv),
            ]
        )
    ]
    loads = []
    for b in range(CHUNKS):
        for p in range(FPA):
            n = pl.ds(p * AGG + b * 2048, 2048)
            loads.append((b, r_hbm.at[:, :, n], r.at[:, :, n], load_sem.at[0, b, p]))
            loads.append((b, w_hbm.at[:, :, n], w.at[:, :, n], load_sem.at[1, b, p]))
    loads = [(b, pltpu.make_async_copy(x, y, z)) for b, x, y, z in loads]
    def load(b):
        for at, copy in loads:
            if at == b:
                copy.start()

    small[0].start()
    load(0)
    start_barrier()
    load(1)

    S_rows, R_rows = S.reshape(CHUNKS * 1024, LANES), R.reshape(CHUNKS * 1024, LANES)
    S2_rows, R2_rows = S2.reshape(CHUNKS * 1024, LANES), R2.reshape(CHUNKS * 1024, LANES)
    small[0].wait()
    for b in range(CHUNKS):
        for at, copy in loads:
            if at == b:
                copy.wait()
        if b == 0:
            load(2)
            for copy in small[1:5]:
                copy.start()
        restrict_chunk(b, r, w, pat, A)
        pack_chunk(b, A, S_rows)
        if b == 0:
            end_barrier()
        send_chunk(S, R, b, s1, r1)
        keep_own(S, R, b)

    for copy in small[1:5]:
        copy.wait()
    E[...] = jnp.zeros(E.shape, F32)
    pc[...] = jnp.zeros(pc.shape, F32)
    pb[...] = jnp.zeros(pb.shape, F32)
    inv_v[...] = jnp.zeros(inv_v.shape, jnp.int32)
    index_tables(ca, slot_v, odd, inv_v)
    small[5].start()
    for n in range(2):
        slot_copy(n, n, slot_v, slot, slot_sem).start()
    couplings(off, opat, binv, coup, pc, pb)
    small[5].wait()

    for b in range(CHUNKS):
        wait_chunk(R, b, r1)
        unfold_chunk(b, R_rows)
    gather_cells(slot_v, slot, slot_sem, R_rows, G, odd, rhs, binv, X)

    halos = [halo_copies(s, X, E, H, hs, hr) for s in range(3)]
    start_copies(halos[0][:2])
    pack_edges(0, X, E)
    start_copies(halos[0][2:])
    for s in range(3):
        if s < 2:

            def new_at(row, v, s=s):
                return X.at[s + 1, pl.ds(pl.multiple_of(row * W + W + v * 8, 8), 8)]
        else:

            def new_at(row, v):
                return x_out.at[pl.ds(pl.multiple_of(row * W + v * 8, 8), 8)]

        def inner(two, c, s=s, new_at=new_at):
            for u in range(2):
                sweep_row(s, 1 + two * 2 + u, rhs, binv, coup, X, new_at)
            return c

        lax.fori_loop(0, (NI - 2) // 2, inner, 0)
        finish_copies(halos[s][:2])
        lax.fori_loop(
            0,
            2,
            lambda n, c, s=s, new_at=new_at: (
                sweep_row(s, n * (NI - 1), rhs, binv, coup, X, new_at),
                c,
            )[1],
            0,
        )
        if s < 2:
            pack_edges(s + 1, X, E)
        finish_copies(halos[s][2:])
        correct_edges(s, H, pc, pb, D)
        if s < 2:
            for side in range(2):
                E[side, s + 1] = E[side, s + 1] + D[side]
            start_copies(halos[s + 1][2:])
        add_edges(0, D, new_at)
        add_edges(2, D, new_at)
        if s < 2:
            start_copies(halos[s + 1][:2])
        add_edges(1, D, new_at)

    planes_to_cells(x_out, G)
    return_all(inv, G, S2, S2_rows, R2, s2, r2)
    for b in range(CHUNKS):
        wait_chunk(R2, b, r2)
        spread_chunk(b, R2_rows, Y)

    for b in range(CHUNKS):
        wait_chunk(R, b, s1)
        wait_chunk(R, b, s2)
    for copies in halos:
        for sends, _, copy, _ in copies:
            pl.when(sends)(copy.wait_send)


def prolong_kernel(y, x, w, pat, out, planes_out, fine, planes, sem, psem):
    def line(row, c):
        for v in range(6):
            at = (v % 2 * 24 + v // 2) * NI + row
            planes[pl.ds(at, 8, stride=3 * NI), :] = x[pl.ds(row * W + v * 8, 8), :]
        return c

    lax.fori_loop(0, NI, line, 0)
    plane_copy = pltpu.make_async_copy(planes, planes_out, psem)
    plane_copy.start()

    def copies(p):
        n = pl.ds(pl.multiple_of(p * AGG, AGG), AGG)
        return [
            pltpu.make_async_copy(fine.at[j, :, n], out.at[j, :, n], sem.at[p, j])
            for j in range(3)
        ]

    def block(p, c):
        def some(blk, c):
            for u in range(4):
                k = blk * 4 + u
                at = pl.ds(pl.multiple_of(p * AGG + k * LANES, LANES), LANES)
                base = pl.multiple_of(k * W, 8)
                there = bcast_row(pat, pl.ds(p * NK + k, 1), slice(None)).astype(F32)
                src = [
                    [y[pl.ds(base + i * 16 + qg * 8, 8), :] * there for qg in range(2)]
                    for i in range(3)
                ]
                for j in range(3):
                    acc = None
                    for i in range(3):
                        wij = jnp.broadcast_to(w[i, j : j + 1, at], (8, LANES))
                        terms = [wij * src[i][qg] for qg in range(2)]
                        acc = terms if acc is None else [a + z for a, z in zip(acc, terms)]
                    for qg in range(2):
                        fine[j, qg * 8 : qg * 8 + 8, at] = acc[qg]
            return c

        lax.fori_loop(0, NK // 4, some, 0)
        for copy in copies(p):
            copy.start()
        return c

    lax.fori_loop(0, FPA, block, 0)
    plane_copy.wait()

    def finish(p, c):
        for copy in copies(p):
            copy.wait()
        return c

    lax.fori_loop(0, FPA, finish, 0)


def body(residual, restriction, pattern, cell_aggregate, block_inverse, off_blocks, op_pattern):
    turned = residual.transpose(1, 0, 2)
    pat = pattern.reshape(384, LANES)
    vmem = pl.BlockSpec(memory_space=pltpu.VMEM)
    hbm = pl.BlockSpec(memory_space=pltpu.HBM)
    msg = pltpu.VMEM((CHUNKS, ND, 8, LANES), F32)
    plane = pltpu.VMEM((NI * W, LANES), F32)
    edge = pltpu.VMEM((2, 3, 3, 8, LANES), F32)
    x, y = pl.pallas_call(
        coarse_kernel,
        out_shape=(
            jax.ShapeDtypeStruct((NI * W, LANES), F32),
            jax.ShapeDtypeStruct((NK * W, LANES), F32),
        ),
        in_specs=[hbm] * 7,
        out_specs=(vmem, vmem),
        scratch_shapes=[
            pltpu.VMEM((3, NQ, FPA * AGG), F32),
            pltpu.VMEM((3, 3, FPA * AGG), F32),
            pltpu.VMEM((384, LANES), jnp.int32),
            pltpu.VMEM((NI, LANES), jnp.int32),
            pltpu.VMEM((9, NI, LANES), F32),
            pltpu.VMEM((36, NI, LANES), F32),
            pltpu.VMEM((4, NI, LANES), jnp.int32),
            plane,
            msg,
            msg,
            msg,
            msg,
            pltpu.VMEM((AGG, LANES), F32),
            plane,
            pltpu.VMEM((3, (NI + 2) * W, LANES), F32),
            edge,
            edge,
            pltpu.VMEM((2, 3, 8, LANES), F32),
            pltpu.VMEM((36, NI, LANES), F32),
            pltpu.VMEM((2, 9, 8, LANES), F32),
            pltpu.VMEM((2, 9, 8, LANES), F32),
            pltpu.VMEM((NI, LANES), jnp.int32),
            pltpu.VMEM((NI, LANES), jnp.int32),
            pltpu.VMEM((ND, LANES), jnp.int32),
            pltpu.SMEM((2, 8, LANES), jnp.int32),
            pltpu.SMEM((ND, LANES), jnp.int32),
            pltpu.SemaphoreType.DMA((2, CHUNKS, FPA)),
            pltpu.SemaphoreType.DMA((6,)),
            pltpu.SemaphoreType.DMA((2,)),
            pltpu.SemaphoreType.DMA((CHUNKS,)),
            pltpu.SemaphoreType.DMA((CHUNKS,)),
            pltpu.SemaphoreType.DMA((CHUNKS,)),
            pltpu.SemaphoreType.DMA((CHUNKS,)),
            pltpu.SemaphoreType.DMA((3, 4)),
            pltpu.SemaphoreType.DMA((3, 4)),
        ],
        compiler_params=pltpu.CompilerParams(
            collective_id=0, has_side_effects=True, vmem_limit_bytes=46 * 1024 * 1024
        ),
    )(
        *[
            pltpu.with_memory_space_constraint(x, pltpu.HBM)
            for x in (
                turned,
                restriction,
                pat,
                cell_aggregate,
                block_inverse.reshape(9, NI, LANES),
                off_blocks.reshape(36, NI, LANES),
                op_pattern,
            )
        ]
    )
    fine, planes = pl.pallas_call(
        prolong_kernel,
        out_shape=(
            jax.ShapeDtypeStruct((3, NQ, FPA * AGG), F32),
            jax.ShapeDtypeStruct((NQ * 3 * NI, LANES), F32),
        ),
        in_specs=[vmem] * 4,
        out_specs=(hbm, hbm),
        scratch_shapes=[
            pltpu.VMEM((3, NQ, FPA * AGG), F32),
            pltpu.VMEM((NQ * 3 * NI, LANES), F32),
            pltpu.SemaphoreType.DMA((FPA, 3)),
            pltpu.SemaphoreType.DMA,
        ],
        compiler_params=pltpu.CompilerParams(vmem_limit_bytes=24 * 1024 * 1024),
    )(y, x, restriction, pat)
    return planes.reshape(NQ, 3, NI, LANES), fine.transpose(1, 0, 2)


def solution(mesh):
    in_specs = (
        P(None, None, ("row", "col")),
        P(None, None, ("row", "col")),
        P(("row", "col")),
        P("row", "col"),
        P(None, None, "row", "col"),
        P(None, None, None, "row", "col"),
        P(None, "row", "col"),
    )
    out_specs = (P(None, None, "row", "col"), P(None, None, ("row", "col")))
    return jax.shard_map(body, mesh=mesh, in_specs=in_specs, out_specs=out_specs, check_vma=False)
```

```python
import functools

import jax
import jax.numpy as jnp
from jax import lax
from jax.experimental import pallas as pl
from jax.experimental.pallas import tpu as pltpu
from jax.sharding import PartitionSpec as P

MESH = pl.DeviceIdType.MESH
ND = 128
NQ = 16
NI = 48
NK = 48
W = 48
AGG = 6144
FPA = 8
CHUNKS = 3
LANES = 128
F32 = jnp.float32


def me_index():
    return lax.axis_index("row") * 8 + lax.axis_index("col")


def lane_ids():
    return lax.broadcasted_iota(jnp.int32, (8, LANES), 1)


def bcast_row(ref, *idx):
    return jnp.broadcast_to(ref[idx], (8, LANES))


def peer_row(row, far, near):
    z = lax.rem(row // 4 + far, 4)
    return z * 4 + lax.rem(lax.rem(row, 4) + near, 4)


def each_peer(visit):
    row, col = lax.axis_index("row"), lax.axis_index("col")
    cols = [lax.rem(col + d, 8) for d in (2, 6, 1, 3, 5, 7, 4, 0)]
    for far in (2, 1, 3, 0):

        def one(n, c, far=far):
            there = peer_row(row, far, 3 - n)
            for other in cols:
                visit(there, other)
            return c

        lax.fori_loop(0, 4 if far else 3, one, 0)
    for other in cols[:-1]:
        visit(row, other)


def start_barrier():
    bar = pltpu.get_barrier_semaphore()
    each_peer(
        lambda row, col: pl.semaphore_signal(
            bar, inc=1, device_id=(row, col), device_id_type=MESH
        )
    )


def end_barrier():
    pl.semaphore_wait(pltpu.get_barrier_semaphore(), ND - 1)


def send_chunk(S, R, b, ssem, rsem):
    dst = R.at[b, me_index(), pl.ds(0, 6)]

    def visit(row, col):
        pltpu.make_async_remote_copy(
            S.at[b, row * 8 + col, pl.ds(0, 6)],
            dst,
            ssem.at[b],
            rsem.at[b],
            device_id=(row, col),
            device_id_type=MESH,
        ).start()

    each_peer(visit)


def wait_chunk(R, b, sem):
    block = R.at[b, pl.ds(0, ND - 1), pl.ds(0, 6)]
    pltpu.make_async_copy(block, block, sem.at[b]).wait()


def keep_own(S, R, b):
    me = me_index()
    R[b, me] = S[b, me]


def restrict_chunk(b, r, w, pat, A):
    def one(kk, c):
        k = b * 16 + kk
        acc = [[None] * 2 for _ in range(3)]
        for p in range(FPA):
            n = pl.multiple_of(p * AGG + k * LANES, LANES)
            there = bcast_row(pat, pl.ds(p * 48 + k, 1), slice(None)).astype(F32)
            here = [
                [r[j, qg * 8 : qg * 8 + 8, pl.ds(n, LANES)] * there for qg in range(2)]
                for j in range(3)
            ]
            for i in range(3):
                for j in range(3):
                    wij = jnp.broadcast_to(w[i, j : j + 1, pl.ds(n, LANES)], (8, LANES))
                    for qg in range(2):
                        term = wij * here[j][qg]
                        acc[i][qg] = term if acc[i][qg] is None else acc[i][qg] + term
        for i in range(3):
            for qg in range(2):
                at = pl.multiple_of(k * W + i * 16 + qg * 8, 8)
                A[pl.ds(at, 8), :] = acc[i][qg]
        return c

    lax.fori_loop(0, 16, one, 0)


def pack_chunk(b, A, S2d):
    for h in range(2):
        k8 = b * 16 + 8 * h
        six, seven = (k8 + 6) * W, (k8 + 7) * W
        for m in range(3):
            at = (k8 + 2 * m) * W
            head = A[at : at + 96, :]
            if m == 0:
                tail = [A[six : six + 32, :]]
            elif m == 1:
                tail = [A[seven : seven + 32, :]]
            else:
                tail = [A[six + 32 : six + 48, :], A[seven + 32 : seven + 48, :]]
            turned = jnp.concatenate([head] + tail, axis=0).T
            for t0 in range(16):
                rows = pl.ds(b * 1024 + t0 * 64 + 2 * m + h, 8, stride=8)
                S2d[rows, :] = turned[t0 * 8 : t0 * 8 + 8, :]


def unfold_chunk(b, R2d):
    lane = lane_ids()

    def one(fb, c):
        for base, h in [(b * 1024 + (fb * 8 + u) * 64, h) for u in range(8) for h in range(2)]:
            x0 = R2d[pl.ds(base + h, 8, stride=8), :]
            x1 = R2d[pl.ds(base + 2 + h, 8, stride=8), :]
            x2 = R2d[pl.ds(base + 4 + h, 8, stride=8), :]
            six = jnp.where(lane < 32, pltpu.roll(x0, 32, 1), pltpu.roll(x2, 64, 1))
            seven = jnp.where(lane < 80, pltpu.roll(x1, 80, 1), pltpu.roll(x2, 96, 1))
            R2d[pl.ds(base + 6 + h, 8, stride=8), :] = jnp.where(lane < 48, six, seven)
        return c

    lax.fori_loop(0, 2, one, 0)


def index_tables(ca, slot_v, odd, inv_v):
    def one(blk, acc):
        rows = pl.ds(pl.multiple_of(blk * 8, 8), 8)
        pair = lax.shift_right_logical(ca[rows, :], 7)
        owner = lax.shift_right_logical(lax.shift_right_logical(pair, 4) * 171, 9)
        local = pair - owner * NK
        bit = [lax.shift_right_logical(local, n) & 1 for n in range(4)]
        chunk = lax.shift_right_logical(local, 4)
        at = chunk * 1024 + owner * 8 + (bit[2] * 2 + bit[1]) * 2 + bit[3]
        slot_v[rows, :] = jnp.clip(at, 0, CHUNKS * 1024 - 1)
        odd[rows, :] = bit[0]
        for u in range(8):
            who = jnp.broadcast_to(owner[u : u + 1], (ND, LANES))
            by_owner = (who == lax.broadcasted_iota(jnp.int32, (ND, LANES), 0)).astype(F32)
            which = jnp.broadcast_to(local[u : u + 1], (NK, LANES))
            here = which == lax.broadcasted_iota(jnp.int32, (NK, LANES), 0)
            column = lax.broadcasted_iota(jnp.int32, (NK, LANES), 1).astype(F32)
            line = (blk * 8 + u).astype(F32)
            cells = jnp.concatenate(
                [jnp.where(here, column, 0.0), jnp.where(here, line, 0.0)], axis=0
            )
            acc = acc + lax.dot_general(
                by_owner.astype(jnp.bfloat16),
                cells.astype(jnp.bfloat16),
                (((1,), (1,)), ((), ())),
                preferred_element_type=F32,
            )
        return acc

    acc = lax.fori_loop(0, NI // 8, one, jnp.zeros((ND, 2 * NK), F32))
    cell = (acc[:, NK:] * LANES + acc[:, :NK]).astype(jnp.int32)
    inv_v[:, 0:NK] = jnp.clip(cell, 0, AGG - 1)


def solve_block(binv, row, total):
    out = []
    for i in range(3):
        acc = None
        for j in range(3):
            coef = bcast_row(binv, i * 3 + j, pl.ds(row, 1), slice(None))
            terms = [coef * total[j][qg] for qg in range(2)]
            acc = terms if acc is None else [x + y for x, y in zip(acc, terms)]
        out.append(acc)
    return out


def slot_copy(blk, n, slot_v, slot, sem):
    rows = pl.ds(pl.multiple_of(blk * 8, 8), 8)
    return pltpu.make_async_copy(slot_v.at[rows], slot.at[n], sem.at[n])


def gather_rows(slot_v, slot, sem, R2d, G):
    def some(two, c):
        for n in range(2):
            blk = two * 2 + n
            slot_copy(blk, n, slot_v, slot, sem).wait()
            base = pl.multiple_of(blk * 8 * LANES, LANES)
            for u in range(8):
                for k in range(LANES):
                    G[pl.ds(base + u * LANES + k, 1), :] = R2d[pl.ds(slot[n, u, k], 1), :]
            pl.when(two < 2)(slot_copy(blk + 2, n, slot_v, slot, sem).start)
        return c

    lax.fori_loop(0, 3, some, 0)


def cells_to_planes(G, odd, rhs, binv, X):
    def one(blk, c):
        for u in range(8):
            row = blk * 8 + u
            base = pl.multiple_of(row * W, 8)
            turned = G[pl.ds(pl.multiple_of(row * LANES, LANES), LANES), :].T
            is_odd = bcast_row(odd, pl.ds(row, 1), slice(None)) == 1
            total = [[None] * 2 for _ in range(3)]
            for v in range(6):
                here = jnp.where(
                    is_odd, turned[W + v * 8 : W + v * 8 + 8, :], turned[v * 8 : v * 8 + 8, :]
                )
                rhs[pl.ds(base + v * 8, 8), :] = here
                total[v // 2][v % 2] = here
            new = solve_block(binv, row, total)
            for v in range(6):
                X[0, pl.ds(base + W + v * 8, 8), :] = new[v // 2][v % 2]
        return c

    lax.fori_loop(0, NI // 8, one, 0)


def couplings(off, opat, binv, coup, pc, pb):
    def couple(blk, c):
        at = pl.ds(pl.multiple_of(blk * 8, 8), 8)
        for d in range(4):
            there = opat[d, at, :].astype(F32)
            for e in range(9):
                coup[d * 9 + e, at, :] = off[d * 9 + e, at, :] * there
        return c

    lax.fori_loop(0, NI // 8, couple, 0)

    def pack(e, c):
        for blk in range(3):
            for src, plane, keep in (
                (coup, 18 + e, (0,)),
                (coup, 27 + e, (1,)),
                (binv, e, (0, 1)),
            ):
                parts = [
                    bcast_row(src, plane, slice(blk * 16 + n, blk * 16 + n + 1), slice(None))
                    for n in range(16)
                ]
                turned = jnp.concatenate(parts, axis=0).T
                for side in keep:
                    line = turned[0:1] if side == 0 else turned[LANES - 1 : LANES]
                    dst = pb if src is binv else pc
                    for qg in range(2):
                        dst[side, e, qg * 3 + blk : qg * 3 + blk + 1, :] = line
        return c

    lax.fori_loop(0, 9, pack, 0)

    def mask(e, c):
        lane = lax.broadcasted_iota(jnp.int32, (NI, LANES), 1)
        coup[18 + e] = jnp.where(lane == 0, 0.0, coup[18 + e])
        coup[27 + e] = jnp.where(lane == LANES - 1, 0.0, coup[27 + e])
        return c

    lax.fori_loop(0, 9, mask, 0)


def pack_edges(s, X, E):
    for blk in range(3):
        for v in range(6):
            parts = [
                X[s, (blk * 16 + n + 1) * W + v * 8 : (blk * 16 + n + 1) * W + v * 8 + 8, :]
                for n in range(16)
            ]
            turned = jnp.concatenate(parts, axis=0).T
            at = v % 2 * 3 + blk
            E[0, s, v // 2, at : at + 1, :] = turned[0:1]
            E[1, s, v // 2, at : at + 1, :] = turned[LANES - 1 : LANES]


def halo_copies(s, X, U, E, H, hs, hr):
    row, col = lax.axis_index("row"), lax.axis_index("col")
    own_first = X.at[s, pl.ds(W, W)] if s == 0 else U.at[s - 1, 0]
    own_last = X.at[s, pl.ds(NI * W, W)] if s == 0 else U.at[s - 1, 1]
    above = X.at[s, pl.ds(0, W)]
    below = X.at[s, pl.ds((NI + 1) * W, W)]
    table = [
        (row > 0, row < 15, own_first, below, (row - 1, col)),
        (row < 15, row > 0, own_last, above, (row + 1, col)),
        (col > 0, col < 7, E.at[0, s], H.at[1, s], (row, col - 1)),
        (col < 7, col > 0, E.at[1, s], H.at[0, s], (row, col + 1)),
    ]
    return [
        (
            sends,
            receives,
            pltpu.make_async_remote_copy(
                src, dst, hs.at[s, n], hr.at[s, n], device_id=dev, device_id_type=MESH
            ),
            dst,
        )
        for n, (sends, receives, src, dst, dev) in enumerate(table)
    ]


def start_copies(copies):
    for sends, _, copy, _ in copies:
        pl.when(sends)(copy.start)


def finish_copies(copies):
    for _, receives, copy, dst in copies:
        pl.when(receives)(copy.wait_recv)

        def clear(dst=dst):
            dst[...] = jnp.zeros(dst.shape, F32)

        pl.when(jnp.logical_not(receives))(clear)


def row_total(s, row, rhs, coup, X, skip=None):
    base = pl.multiple_of(row * W, 8)

    def at(v):
        return pl.ds(base + v * 8, 8)

    own = [X[s, at(v + 6), :] for v in range(6)]
    left = [pltpu.roll(x, 1, 1) for x in own]
    right = [pltpu.roll(x, LANES - 1, 1) for x in own]
    total = [[rhs[at(j * 2 + qg), :] for qg in range(2)] for j in range(3)]
    for d in range(4):
        if d == skip:
            continue
        if d < 2:
            near = [X[s, at(v + 12 * d), :] for v in range(6)]
        else:
            near = left if d == 2 else right
        total = less_direction(d, row, coup, near, total)
    return total


def less_direction(d, row, coup, near, total):
    total = [list(t) for t in total]
    for k in range(3):
        for j in range(3):
            coef = bcast_row(coup, d * 9 + j * 3 + k, pl.ds(row, 1), slice(None))
            for qg in range(2):
                total[j][qg] = total[j][qg] - coef * near[k * 2 + qg]
    return total


def edge_lanes(blk, n, D):
    lane = lane_ids()
    here = lane == lax.broadcasted_iota(jnp.int32, (8, LANES), 0) + 8 * n
    out = []
    for v in range(6):
        at = v % 2 * 3 + blk
        ends = []
        for side in range(2):
            line = bcast_row(D, side, v // 2, slice(at, at + 1), slice(None))
            ends.append(jnp.sum(jnp.where(here, line, 0.0), axis=1, keepdims=True))
        out.append(jnp.where(lane == 0, ends[0], jnp.where(lane == LANES - 1, ends[1], 0.0)))
    return out


def correct_edges(s, H, pc, pb, D):
    for side in range(2):
        push = []
        for j in range(3):
            acc = None
            for k in range(3):
                term = pc[side, j * 3 + k] * H[side, s, k]
                acc = term if acc is None else acc + term
            push.append(acc)
        for i in range(3):
            acc = None
            for j in range(3):
                term = pb[side, i * 3 + j] * push[j]
                acc = term if acc is None else acc + term
            D[side, i] = -acc


def add_edges(blk, D, new_at):
    sub = lax.broadcasted_iota(jnp.int32, (8, LANES), 0)
    zero = jnp.zeros((LANES - 16, LANES), F32)
    for v in range(6):
        at = v % 2 * 3 + blk
        first = jnp.where(sub == 0, bcast_row(D, 0, v // 2, slice(at, at + 1), slice(None)), 0.0)
        last = jnp.where(sub == 7, bcast_row(D, 1, v // 2, slice(at, at + 1), slice(None)), 0.0)
        turned = jnp.concatenate([first, zero, last], axis=0).T
        for n in range(16):
            ref = new_at(blk * 16 + n, v)
            ref[...] = ref[...] + turned[n * 8 : n * 8 + 8]


def planes_to_cells(last, G):
    def one(blk, c):
        for u in range(16):
            row = blk * 16 + u
            x = last[pl.ds(pl.multiple_of(row * W, 8), W), :]
            turned = jnp.concatenate([x, x], axis=0).T
            G[pl.ds(pl.multiple_of(row * LANES, LANES), LANES), 0 : 2 * W] = turned
        return c

    lax.fori_loop(0, NI // 16, one, 0)


def return_all(inv, G, S2, S2_rows, R2, ssem, rsem):
    row, col = lax.axis_index("row"), lax.axis_index("col")
    cols = [lax.rem(col + d, 8) for d in range(8)]
    me = me_index()
    low = lax.broadcasted_iota(jnp.int32, (1, LANES), 1) < W
    lane = lane_ids()

    def collect(b, there):
        for u in range(8):
            f = there * 8 + u
            for rr in range(8):
                k = b * 16 + rr % 2 * 8 + rr // 2 * 2
                even = G[pl.ds(inv[f, k], 1), :]
                odd = G[pl.ds(inv[f, k + 1], 1), :]
                S2_rows[pl.ds(b * 1024 + f * 8 + rr, 1), :] = jnp.where(low, even, odd)

    def fold_start(b, there):
        base = b * 1024 + there * 64
        done = []
        for h in range(2):
            d = S2_rows[pl.ds(base + 6 + h, 8, stride=8), :]
            for m, moved in enumerate(
                (
                    pltpu.roll(d, 96, 1),
                    pltpu.roll(d, 48, 1),
                    jnp.where(lane < 112, pltpu.roll(d, 64, 1), pltpu.roll(d, 32, 1)),
                )
            ):
                rows = pl.ds(base + 2 * m + h, 8, stride=8)
                done.append((rows, jnp.where(lane >= 96, moved, S2_rows[rows, :])))
        return done

    def fold_end(done):
        for rows, x in done:
            S2_rows[rows, :] = x

    def send(b, there):
        def one(c):
            pltpu.make_async_remote_copy(
                S2.at[b, there * 8 + c, pl.ds(0, 6)],
                R2.at[b, me, pl.ds(0, 6)],
                ssem.at[b],
                rsem.at[b],
                device_id=(there, c),
                device_id_type=MESH,
            ).start()

        for c in cols[1:]:
            one(c)
        pl.when(there != row)(lambda: one(cols[0]))

    def peer(d):
        group = d // 4
        far = jnp.where(group == 0, 2, jnp.where(group == 1, 1, jnp.where(group == 2, 3, 0)))
        return peer_row(row, far, 3 - lax.rem(d, 4))

    for b in range(CHUNKS):
        collect(b, peer(0))
        done = fold_start(b, peer(0))
        if b > 0:
            send(b - 1, peer(15))
        collect(b, peer(1))
        fold_end(done)

        def step(d, c, b=b):
            done = fold_start(b, peer(d - 1))
            collect(b, peer(d))
            fold_end(done)
            send(b, peer(d - 2))
            return c

        lax.fori_loop(2, 16, step, 0)
        fold_end(fold_start(b, peer(15)))
        send(b, peer(14))
        R2[b, me] = S2[b, me]
    send(CHUNKS - 1, peer(15))


def spread_chunk(b, R2d, Y):
    for h in range(2):
        k8 = b * 16 + 8 * h
        six, seven = (k8 + 6) * W, (k8 + 7) * W
        for m in range(3):
            parts = [
                R2d[pl.ds(b * 1024 + t0 * 64 + 2 * m + h, 8, stride=8), :] for t0 in range(16)
            ]
            turned = jnp.concatenate(parts, axis=0).T
            at = (k8 + 2 * m) * W
            Y[at : at + 96, :] = turned[0:96]
            if m == 0:
                Y[six : six + 32, :] = turned[96:128]
            elif m == 1:
                Y[seven : seven + 32, :] = turned[96:128]
            else:
                Y[six + 32 : six + 48, :] = turned[96:112]
                Y[seven + 32 : seven + 48, :] = turned[112:128]


def coarse_kernel(
    r_hbm,
    w_hbm,
    pat_hbm,
    ca_hbm,
    binv_hbm,
    off_hbm,
    opat_hbm,
    x_out,
    Y,
    w,
    pat,
    r,
    ca,
    binv,
    off,
    opat,
    A,
    S,
    R,
    S2,
    R2,
    G,
    rhs,
    X,
    U,
    E,
    H,
    D,
    coup,
    pc,
    pb,
    slot_v,
    odd,
    inv_v,
    slot,
    inv,
    load_sem,
    small_sem,
    slot_sem,
    inv_sem,
    s1,
    r1,
    s2,
    r2,
    hs,
    hr,
):
    small = [
        pltpu.make_async_copy(x, y, small_sem.at[n])
        for n, (x, y) in enumerate(
            [
                (pat_hbm, pat),
                (ca_hbm, ca),
                (binv_hbm, binv),
                (off_hbm, off),
                (opat_hbm, opat),
            ]
        )
    ]
    loads = []
    for b in range(CHUNKS):
        for p in range(FPA):
            n = pl.ds(p * AGG + b * 2048, 2048)
            loads.append((b, r_hbm.at[:, :, n], r.at[:, :, n], load_sem.at[0, b, p]))
            loads.append((b, w_hbm.at[:, :, n], w.at[:, :, n], load_sem.at[1, b, p]))
    loads = [(b, pltpu.make_async_copy(x, y, z)) for b, x, y, z in loads]
    def load(b):
        for at, copy in loads:
            if at == b:
                copy.start()

    small[0].start()
    load(0)
    start_barrier()
    load(1)

    S_rows, R_rows = S.reshape(CHUNKS * 1024, LANES), R.reshape(CHUNKS * 1024, LANES)
    S2_rows, R2_rows = S2.reshape(CHUNKS * 1024, LANES), R2.reshape(CHUNKS * 1024, LANES)
    small[0].wait()
    for b in range(CHUNKS):
        for at, copy in loads:
            if at == b:
                copy.wait()
        if b == 0:
            load(2)
            for copy in small[1:5]:
                copy.start()
        restrict_chunk(b, r, w, pat, A)
        pack_chunk(b, A, S_rows)
        if b == 0:
            end_barrier()
        send_chunk(S, R, b, s1, r1)
        keep_own(S, R, b)

    for copy in small[1:5]:
        copy.wait()
    E[...] = jnp.zeros(E.shape, F32)
    pc[...] = jnp.zeros(pc.shape, F32)
    pb[...] = jnp.zeros(pb.shape, F32)
    inv_v[...] = jnp.zeros(inv_v.shape, jnp.int32)
    index_tables(ca, slot_v, odd, inv_v)
    inv_copy = pltpu.make_async_copy(inv_v, inv, inv_sem)
    inv_copy.start()
    for n in range(2):
        slot_copy(n, n, slot_v, slot, slot_sem).start()
    couplings(off, opat, binv, coup, pc, pb)
    inv_copy.wait()

    for b in range(CHUNKS):
        wait_chunk(R, b, r1)
        unfold_chunk(b, R_rows)
    gather_rows(slot_v, slot, slot_sem, R_rows, G)
    cells_to_planes(G, odd, rhs, binv, X)

    halos = [halo_copies(s, X, U, E, H, hs, hr) for s in range(3)]
    start_copies(halos[0][:2])
    pack_edges(0, X, E)
    start_copies(halos[0][2:])
    ends = ((0, 0, 0), (NI - 1, 2, 15))
    for s in range(3):
        if s < 2:

            def new_at(row, v, s=s):
                return X.at[s + 1, pl.ds(pl.multiple_of(row * W + W + v * 8, 8), 8)]
        else:

            def new_at(row, v):
                return x_out.at[pl.ds(pl.multiple_of(row * W + v * 8, 8), 8)]

        def inner(two, c, s=s, new_at=new_at):
            for u in range(2):
                row = 1 + two * 2 + u
                new = solve_block(binv, row, row_total(s, row, rhs, coup, X))
                for v in range(6):
                    new_at(row, v)[...] = new[v // 2][v % 2]
            return c

        lax.fori_loop(0, (NI - 2) // 2, inner, 0)
        totals = [row_total(s, row, rhs, coup, X, skip=d) for d, (row, _, _) in enumerate(ends)]
        finish_copies(halos[s][:2])
        new = []
        for d, (row, _, _) in enumerate(ends):
            near = [X[s, pl.ds((row + 2 * d) * W + v * 8, 8), :] for v in range(6)]
            new.append(solve_block(binv, row, less_direction(d, row, coup, near, totals[d])))
            for v in range(6):
                new_at(row, v)[...] = new[d][v // 2][v % 2]
        finish_copies(halos[s][2:])
        correct_edges(s, H, pc, pb, D)
        if s < 2:
            for d, (_, blk, n) in enumerate(ends):
                more = edge_lanes(blk, n, D)
                for v in range(6):
                    U[s, d, v * 8 : v * 8 + 8, :] = new[d][v // 2][v % 2] + more[v]
            start_copies(halos[s + 1][:2])
            pack_edges(s + 1, X, E)
            for side in range(2):
                E[side, s + 1] = E[side, s + 1] + D[side]
            start_copies(halos[s + 1][2:])
        for blk in range(3):
            add_edges(blk, D, new_at)

    planes_to_cells(x_out, G)
    return_all(inv, G, S2, S2_rows, R2, s2, r2)
    for b in range(CHUNKS):
        wait_chunk(R2, b, r2)
        spread_chunk(b, R2_rows, Y)

    for b in range(CHUNKS):
        wait_chunk(R, b, s1)
        wait_chunk(R, b, s2)
    for copies in halos:
        for sends, _, copy, _ in copies:
            pl.when(sends)(copy.wait_send)


def prolong_kernel(y, x, w, pat, out, planes_out, fine, planes, sem, psem):
    def line(row, c):
        for v in range(6):
            at = (v % 2 * 24 + v // 2) * NI + row
            planes[pl.ds(at, 8, stride=3 * NI), :] = x[pl.ds(row * W + v * 8, 8), :]
        return c

    lax.fori_loop(0, NI, line, 0)
    plane_copy = pltpu.make_async_copy(planes, planes_out, psem)
    plane_copy.start()

    def copies(p):
        n = pl.ds(pl.multiple_of(p * AGG, AGG), AGG)
        return [
            pltpu.make_async_copy(fine.at[j, :, n], out.at[j, :, n], sem.at[p, j])
            for j in range(3)
        ]

    def block(p, c):
        def some(blk, c):
            for u in range(4):
                k = blk * 4 + u
                at = pl.ds(pl.multiple_of(p * AGG + k * LANES, LANES), LANES)
                base = pl.multiple_of(k * W, 8)
                there = bcast_row(pat, pl.ds(p * NK + k, 1), slice(None)).astype(F32)
                src = [
                    [y[pl.ds(base + i * 16 + qg * 8, 8), :] * there for qg in range(2)]
                    for i in range(3)
                ]
                for j in range(3):
                    acc = None
                    for i in range(3):
                        wij = jnp.broadcast_to(w[i, j : j + 1, at], (8, LANES))
                        terms = [wij * src[i][qg] for qg in range(2)]
                        acc = terms if acc is None else [a + z for a, z in zip(acc, terms)]
                    for qg in range(2):
                        fine[j, qg * 8 : qg * 8 + 8, at] = acc[qg]
            return c

        lax.fori_loop(0, NK // 4, some, 0)
        for copy in copies(p):
            copy.start()
        return c

    lax.fori_loop(0, FPA, block, 0)
    plane_copy.wait()

    def finish(p, c):
        for copy in copies(p):
            copy.wait()
        return c

    lax.fori_loop(0, FPA, finish, 0)


def body(residual, restriction, pattern, cell_aggregate, block_inverse, off_blocks, op_pattern):
    turned = residual.transpose(1, 0, 2)
    pat = pattern.reshape(384, LANES)
    vmem = pl.BlockSpec(memory_space=pltpu.VMEM)
    hbm = pl.BlockSpec(memory_space=pltpu.HBM)
    msg = pltpu.VMEM((CHUNKS, ND, 8, LANES), F32)
    plane = pltpu.VMEM((NI * W, LANES), F32)
    edge = pltpu.VMEM((2, 3, 3, 8, LANES), F32)
    x, y, held, held_pat = pl.pallas_call(
        coarse_kernel,
        out_shape=(
            jax.ShapeDtypeStruct((NI * W, LANES), F32),
            jax.ShapeDtypeStruct((NK * W, LANES), F32),
            jax.ShapeDtypeStruct((3, 3, FPA * AGG), F32),
            jax.ShapeDtypeStruct((384, LANES), jnp.int32),
        ),
        in_specs=[hbm] * 7,
        out_specs=(vmem,) * 4,
        scratch_shapes=[
            pltpu.VMEM((3, NQ, FPA * AGG), F32),
            pltpu.VMEM((NI, LANES), jnp.int32),
            pltpu.VMEM((9, NI, LANES), F32),
            pltpu.VMEM((36, NI, LANES), F32),
            pltpu.VMEM((4, NI, LANES), jnp.int32),
            plane,
            msg,
            msg,
            msg,
            msg,
            pltpu.VMEM((AGG, LANES), F32),
            plane,
            pltpu.VMEM((3, (NI + 2) * W, LANES), F32),
            pltpu.VMEM((2, 2, W, LANES), F32),
            edge,
            edge,
            pltpu.VMEM((2, 3, 8, LANES), F32),
            pltpu.VMEM((36, NI, LANES), F32),
            pltpu.VMEM((2, 9, 8, LANES), F32),
            pltpu.VMEM((2, 9, 8, LANES), F32),
            pltpu.VMEM((NI, LANES), jnp.int32),
            pltpu.VMEM((NI, LANES), jnp.int32),
            pltpu.VMEM((ND, LANES), jnp.int32),
            pltpu.SMEM((2, 8, LANES), jnp.int32),
            pltpu.SMEM((ND, LANES), jnp.int32),
            pltpu.SemaphoreType.DMA((2, CHUNKS, FPA)),
            pltpu.SemaphoreType.DMA((5,)),
            pltpu.SemaphoreType.DMA((2,)),
            pltpu.SemaphoreType.DMA,
            pltpu.SemaphoreType.DMA((CHUNKS,)),
            pltpu.SemaphoreType.DMA((CHUNKS,)),
            pltpu.SemaphoreType.DMA((CHUNKS,)),
            pltpu.SemaphoreType.DMA((CHUNKS,)),
            pltpu.SemaphoreType.DMA((3, 4)),
            pltpu.SemaphoreType.DMA((3, 4)),
        ],
        compiler_params=pltpu.CompilerParams(
            collective_id=0, has_side_effects=True, vmem_limit_bytes=46 * 1024 * 1024
        ),
    )(
        *[
            pltpu.with_memory_space_constraint(x, pltpu.HBM)
            for x in (
                turned,
                restriction,
                pat,
                cell_aggregate,
                block_inverse.reshape(9, NI, LANES),
                off_blocks.reshape(36, NI, LANES),
                op_pattern,
            )
        ]
    )
    fine, planes = pl.pallas_call(
        prolong_kernel,
        out_shape=(
            jax.ShapeDtypeStruct((3, NQ, FPA * AGG), F32),
            jax.ShapeDtypeStruct((NQ * 3 * NI, LANES), F32),
        ),
        in_specs=[vmem] * 4,
        out_specs=(hbm, hbm),
        scratch_shapes=[
            pltpu.VMEM((3, NQ, FPA * AGG), F32),
            pltpu.VMEM((NQ * 3 * NI, LANES), F32),
            pltpu.SemaphoreType.DMA((FPA, 3)),
            pltpu.SemaphoreType.DMA,
        ],
        compiler_params=pltpu.CompilerParams(vmem_limit_bytes=24 * 1024 * 1024),
    )(y, x, held, held_pat)
    return planes.reshape(NQ, 3, NI, LANES), fine.transpose(1, 0, 2)


def solution(mesh):
    in_specs = (
        P(None, None, ("row", "col")),
        P(None, None, ("row", "col")),
        P(("row", "col")),
        P("row", "col"),
        P(None, None, "row", "col"),
        P(None, None, None, "row", "col"),
        P(None, "row", "col"),
    )
    out_specs = (P(None, None, "row", "col"), P(None, None, ("row", "col")))
    return jax.shard_map(body, mesh=mesh, in_specs=in_specs, out_specs=out_specs, check_vma=False)
```

```python
import functools

import jax
import jax.numpy as jnp
from jax import lax
from jax.experimental import pallas as pl
from jax.experimental.pallas import tpu as pltpu
from jax.sharding import PartitionSpec as P

MESH = pl.DeviceIdType.MESH
ND = 128
NQ = 16
NI = 48
NK = 48
W = 48
AGG = 6144
FPA = 8
CHUNKS = 3
LANES = 128
F32 = jnp.float32


def me_index():
    return lax.axis_index("row") * 8 + lax.axis_index("col")


def lane_ids():
    return lax.broadcasted_iota(jnp.int32, (8, LANES), 1)


def bcast_row(ref, *idx):
    return jnp.broadcast_to(ref[idx], (8, LANES))


def peer_row(row, far, near):
    z = lax.rem(row // 4 + far, 4)
    return z * 4 + lax.rem(lax.rem(row, 4) + near, 4)


def each_peer(visit):
    row, col = lax.axis_index("row"), lax.axis_index("col")
    cols = [lax.rem(col + d, 8) for d in (2, 6, 1, 3, 5, 7, 4, 0)]
    for far in (2, 1, 3, 0):

        def one(n, c, far=far):
            there = peer_row(row, far, 3 - n)
            for other in cols:
                visit(there, other)
            return c

        lax.fori_loop(0, 4 if far else 3, one, 0)
    for other in cols[:-1]:
        visit(row, other)


def start_barrier():
    bar = pltpu.get_barrier_semaphore()
    each_peer(
        lambda row, col: pl.semaphore_signal(
            bar, inc=1, device_id=(row, col), device_id_type=MESH
        )
    )


def end_barrier():
    pl.semaphore_wait(pltpu.get_barrier_semaphore(), ND - 1)


def send_chunk(S, R, b, ssem, rsem):
    dst = R.at[b, me_index(), pl.ds(0, 6)]

    def visit(row, col):
        pltpu.make_async_remote_copy(
            S.at[b, row * 8 + col, pl.ds(0, 6)],
            dst,
            ssem.at[b],
            rsem.at[b],
            device_id=(row, col),
            device_id_type=MESH,
        ).start()

    each_peer(visit)


def wait_chunk(R, b, sem):
    block = R.at[b, pl.ds(0, ND - 1), pl.ds(0, 6)]
    pltpu.make_async_copy(block, block, sem.at[b]).wait()


def keep_own(S, R, b):
    me = me_index()
    R[b, me] = S[b, me]


def restrict_chunk(b, r, w, pat, A):
    def one(kk, c):
        k = b * 16 + kk
        acc = [[None] * 2 for _ in range(3)]
        for p in range(FPA):
            n = pl.multiple_of(p * AGG + k * LANES, LANES)
            there = bcast_row(pat, pl.ds(p * 48 + k, 1), slice(None)).astype(F32)
            here = [
                [r[j, qg * 8 : qg * 8 + 8, pl.ds(n, LANES)] * there for qg in range(2)]
                for j in range(3)
            ]
            for i in range(3):
                for j in range(3):
                    wij = jnp.broadcast_to(w[i, j : j + 1, pl.ds(n, LANES)], (8, LANES))
                    for qg in range(2):
                        term = wij * here[j][qg]
                        acc[i][qg] = term if acc[i][qg] is None else acc[i][qg] + term
        for i in range(3):
            for qg in range(2):
                at = pl.multiple_of(k * W + i * 16 + qg * 8, 8)
                A[pl.ds(at, 8), :] = acc[i][qg]
        return c

    lax.fori_loop(0, 16, one, 0)


def pack_chunk(b, A, S2d):
    for h in range(2):
        k8 = b * 16 + 8 * h
        six, seven = (k8 + 6) * W, (k8 + 7) * W
        for m in range(3):
            at = (k8 + 2 * m) * W
            head = A[at : at + 96, :]
            if m == 0:
                tail = [A[six : six + 32, :]]
            elif m == 1:
                tail = [A[seven : seven + 32, :]]
            else:
                tail = [A[six + 32 : six + 48, :], A[seven + 32 : seven + 48, :]]
            turned = jnp.concatenate([head] + tail, axis=0).T
            for t0 in range(16):
                rows = pl.ds(b * 1024 + t0 * 64 + 2 * m + h, 8, stride=8)
                S2d[rows, :] = turned[t0 * 8 : t0 * 8 + 8, :]


def unfold_chunk(b, R2d):
    lane = lane_ids()

    def one(fb, c):
        for base, h in [(b * 1024 + (fb * 8 + u) * 64, h) for u in range(8) for h in range(2)]:
            x0 = R2d[pl.ds(base + h, 8, stride=8), :]
            x1 = R2d[pl.ds(base + 2 + h, 8, stride=8), :]
            x2 = R2d[pl.ds(base + 4 + h, 8, stride=8), :]
            six = jnp.where(lane < 32, pltpu.roll(x0, 32, 1), pltpu.roll(x2, 64, 1))
            seven = jnp.where(lane < 80, pltpu.roll(x1, 80, 1), pltpu.roll(x2, 96, 1))
            R2d[pl.ds(base + 6 + h, 8, stride=8), :] = jnp.where(lane < 48, six, seven)
        return c

    lax.fori_loop(0, 2, one, 0)


def index_tables(ca, slot_v, odd, inv_v):
    def one(blk, acc):
        rows = pl.ds(pl.multiple_of(blk * 8, 8), 8)
        pair = lax.shift_right_logical(ca[rows, :], 7)
        owner = lax.shift_right_logical(lax.shift_right_logical(pair, 4) * 171, 9)
        local = pair - owner * NK
        bit = [lax.shift_right_logical(local, n) & 1 for n in range(4)]
        chunk = lax.shift_right_logical(local, 4)
        at = chunk * 1024 + owner * 8 + (bit[2] * 2 + bit[1]) * 2 + bit[3]
        slot_v[rows, :] = jnp.clip(at, 0, CHUNKS * 1024 - 1)
        odd[rows, :] = bit[0]
        for u in range(8):
            who = jnp.broadcast_to(owner[u : u + 1], (ND, LANES))
            by_owner = (who == lax.broadcasted_iota(jnp.int32, (ND, LANES), 0)).astype(F32)
            which = jnp.broadcast_to(local[u : u + 1], (NK, LANES))
            here = which == lax.broadcasted_iota(jnp.int32, (NK, LANES), 0)
            column = lax.broadcasted_iota(jnp.int32, (NK, LANES), 1).astype(F32)
            line = (blk * 8 + u).astype(F32)
            cells = jnp.concatenate(
                [jnp.where(here, column, 0.0), jnp.where(here, line, 0.0)], axis=0
            )
            acc = acc + lax.dot_general(
                by_owner.astype(jnp.bfloat16),
                cells.astype(jnp.bfloat16),
                (((1,), (1,)), ((), ())),
                preferred_element_type=F32,
            )
        return acc

    acc = lax.fori_loop(0, NI // 8, one, jnp.zeros((ND, 2 * NK), F32))
    cell = (acc[:, NK:] * LANES + acc[:, :NK]).astype(jnp.int32)
    inv_v[:, 0:NK] = jnp.clip(cell, 0, AGG - 1)


def solve_block(binv, row, total):
    out = []
    for i in range(3):
        acc = None
        for j in range(3):
            coef = bcast_row(binv, i * 3 + j, pl.ds(row, 1), slice(None))
            terms = [coef * total[j][qg] for qg in range(2)]
            acc = terms if acc is None else [x + y for x, y in zip(acc, terms)]
        out.append(acc)
    return out


def slot_copy(blk, n, slot_v, slot, sem):
    rows = pl.ds(pl.multiple_of(blk * 8, 8), 8)
    return pltpu.make_async_copy(slot_v.at[rows], slot.at[n], sem.at[n])


def gather_cells(slot_v, slot, sem, R2d, near, odd, rhs, binv, X):
    def fetch(blk, n):
        slot_copy(blk, n, slot_v, slot, sem).wait()
        for u in range(8):
            for k in range(LANES):
                near[n][pl.ds(u * LANES + k, 1), :] = R2d[pl.ds(slot[n, u, k], 1), :]

    def planes(blk, n):
        for u in range(8):
            row = blk * 8 + u
            base = pl.multiple_of(row * W, 8)
            turned = near[n][pl.ds(u * LANES, LANES), :].T
            is_odd = bcast_row(odd, pl.ds(row, 1), slice(None)) == 1
            total = [[None] * 2 for _ in range(3)]
            for v in range(6):
                here = jnp.where(
                    is_odd, turned[W + v * 8 : W + v * 8 + 8, :], turned[v * 8 : v * 8 + 8, :]
                )
                rhs[pl.ds(base + v * 8, 8), :] = here
                total[v // 2][v % 2] = here
            new = solve_block(binv, row, total)
            for v in range(6):
                X[0, pl.ds(base + W + v * 8, 8), :] = new[v // 2][v % 2]

    fetch(0, 0)
    slot_copy(2, 0, slot_v, slot, sem).start()

    def some(two, c):
        blk = two * 2 + 1
        fetch(blk, 1)
        planes(blk - 1, 0)
        slot_copy(jnp.minimum(blk + 2, 5), 1, slot_v, slot, sem).start()
        fetch(blk + 1, 0)
        planes(blk, 1)
        slot_copy(jnp.minimum(blk + 3, 5), 0, slot_v, slot, sem).start()
        return c

    lax.fori_loop(0, 2, some, 0)
    fetch(5, 1)
    planes(4, 0)
    slot_copy(5, 0, slot_v, slot, sem).wait()
    planes(5, 1)


def couplings(off, opat, binv, coup, pc, pb):
    def couple(blk, c):
        at = pl.ds(pl.multiple_of(blk * 8, 8), 8)
        for d in range(4):
            there = opat[d, at, :].astype(F32)
            for e in range(9):
                coup[d * 9 + e, at, :] = off[d * 9 + e, at, :] * there
        return c

    lax.fori_loop(0, NI // 8, couple, 0)

    def pack(e, c):
        for blk in range(3):
            for src, plane, keep in (
                (coup, 18 + e, (0,)),
                (coup, 27 + e, (1,)),
                (binv, e, (0, 1)),
            ):
                parts = [
                    bcast_row(src, plane, slice(blk * 16 + n, blk * 16 + n + 1), slice(None))
                    for n in range(16)
                ]
                turned = jnp.concatenate(parts, axis=0).T
                for side in keep:
                    line = turned[0:1] if side == 0 else turned[LANES - 1 : LANES]
                    dst = pb if src is binv else pc
                    for qg in range(2):
                        dst[side, e, qg * 3 + blk : qg * 3 + blk + 1, :] = line
        return c

    lax.fori_loop(0, 9, pack, 0)

    def mask(e, c):
        lane = lax.broadcasted_iota(jnp.int32, (NI, LANES), 1)
        coup[18 + e] = jnp.where(lane == 0, 0.0, coup[18 + e])
        coup[27 + e] = jnp.where(lane == LANES - 1, 0.0, coup[27 + e])
        return c

    lax.fori_loop(0, 9, mask, 0)


def pack_edges(s, X, E, ends=True):
    zero = jnp.zeros((8, LANES), F32)
    for blk in range(3):
        for v in range(6):
            rows = [blk * 16 + n for n in range(16)]
            parts = [
                X[s, (row + 1) * W + v * 8 : (row + 1) * W + v * 8 + 8, :]
                if ends or 0 < row < NI - 1
                else zero
                for row in rows
            ]
            turned = jnp.concatenate(parts, axis=0).T
            at = v % 2 * 3 + blk
            E[0, s, v // 2, at : at + 1, :] = turned[0:1]
            E[1, s, v // 2, at : at + 1, :] = turned[LANES - 1 : LANES]


def patch_edges(s, blk, n, new, E):
    here = lane_ids() == lax.broadcasted_iota(jnp.int32, (8, LANES), 0) + 8 * n
    for v in range(6):
        at = v % 2 * 3 + blk
        x = new[v // 2][v % 2]
        for side, column in enumerate((x[:, 0:1], x[:, LANES - 1 : LANES])):
            line = jnp.sum(jnp.where(here, column, 0.0), axis=0, keepdims=True)
            E[side, s, v // 2, at : at + 1, :] = E[side, s, v // 2, at : at + 1, :] + line


def halo_copies(s, X, U, E, H, hs, hr):
    row, col = lax.axis_index("row"), lax.axis_index("col")
    own_first = X.at[s, pl.ds(W, W)] if s == 0 else U.at[s - 1, 0]
    own_last = X.at[s, pl.ds(NI * W, W)] if s == 0 else U.at[s - 1, 1]
    above = X.at[s, pl.ds(0, W)]
    below = X.at[s, pl.ds((NI + 1) * W, W)]
    table = [
        (row > 0, row < 15, own_first, below, (row - 1, col)),
        (row < 15, row > 0, own_last, above, (row + 1, col)),
        (col > 0, col < 7, E.at[0, s], H.at[1, s], (row, col - 1)),
        (col < 7, col > 0, E.at[1, s], H.at[0, s], (row, col + 1)),
    ]
    return [
        (
            sends,
            receives,
            pltpu.make_async_remote_copy(
                src, dst, hs.at[s, n], hr.at[s, n], device_id=dev, device_id_type=MESH
            ),
            dst,
        )
        for n, (sends, receives, src, dst, dev) in enumerate(table)
    ]


def start_copies(copies):
    for sends, _, copy, _ in copies:
        pl.when(sends)(copy.start)


def finish_copies(copies):
    for _, receives, copy, dst in copies:
        pl.when(receives)(copy.wait_recv)

        def clear(dst=dst):
            dst[...] = jnp.zeros(dst.shape, F32)

        pl.when(jnp.logical_not(receives))(clear)


def row_total(s, row, rhs, coup, X, skip=None):
    base = pl.multiple_of(row * W, 8)

    def at(v):
        return pl.ds(base + v * 8, 8)

    own = [X[s, at(v + 6), :] for v in range(6)]
    left = [pltpu.roll(x, 1, 1) for x in own]
    right = [pltpu.roll(x, LANES - 1, 1) for x in own]
    total = [[rhs[at(j * 2 + qg), :] for qg in range(2)] for j in range(3)]
    for d in range(4):
        if d == skip:
            continue
        if d < 2:
            near = [X[s, at(v + 12 * d), :] for v in range(6)]
        else:
            near = left if d == 2 else right
        total = less_direction(d, row, coup, near, total)
    return total


def less_direction(d, row, coup, near, total):
    total = [list(t) for t in total]
    for k in range(3):
        for j in range(3):
            coef = bcast_row(coup, d * 9 + j * 3 + k, pl.ds(row, 1), slice(None))
            for qg in range(2):
                total[j][qg] = total[j][qg] - coef * near[k * 2 + qg]
    return total


def edge_lanes(blk, n, D):
    lane = lane_ids()
    here = lane == lax.broadcasted_iota(jnp.int32, (8, LANES), 0) + 8 * n
    out = []
    for v in range(6):
        at = v % 2 * 3 + blk
        ends = []
        for side in range(2):
            line = bcast_row(D, side, v // 2, slice(at, at + 1), slice(None))
            ends.append(jnp.sum(jnp.where(here, line, 0.0), axis=1, keepdims=True))
        out.append(jnp.where(lane == 0, ends[0], jnp.where(lane == LANES - 1, ends[1], 0.0)))
    return out


def correct_edges(s, H, pc, pb, D):
    for side in range(2):
        push = []
        for j in range(3):
            acc = None
            for k in range(3):
                term = pc[side, j * 3 + k] * H[side, s, k]
                acc = term if acc is None else acc + term
            push.append(acc)
        for i in range(3):
            acc = None
            for j in range(3):
                term = pb[side, i * 3 + j] * push[j]
                acc = term if acc is None else acc + term
            D[side, i] = -acc


def add_edges(blk, D, new_at):
    sub = lax.broadcasted_iota(jnp.int32, (8, LANES), 0)
    zero = jnp.zeros((LANES - 16, LANES), F32)
    for v in range(6):
        at = v % 2 * 3 + blk
        first = jnp.where(sub == 0, bcast_row(D, 0, v // 2, slice(at, at + 1), slice(None)), 0.0)
        last = jnp.where(sub == 7, bcast_row(D, 1, v // 2, slice(at, at + 1), slice(None)), 0.0)
        turned = jnp.concatenate([first, zero, last], axis=0).T
        for n in range(16):
            ref = new_at(blk * 16 + n, v)
            ref[...] = ref[...] + turned[n * 8 : n * 8 + 8]


def planes_to_cells(row, last, G):
    x = last[pl.ds(pl.multiple_of(row * W, 8), W), :]
    turned = jnp.concatenate([x, x], axis=0).T
    G[pl.ds(pl.multiple_of(row * LANES, LANES), LANES), 0 : 2 * W] = turned


def correct_cells(D, G):
    lane = lane_ids()
    sub = lax.broadcasted_iota(jnp.int32, (8, LANES), 0)
    group = lax.shift_right_logical(lane, 3)
    for side, column in ((0, 0), (1, LANES - 1)):
        for blk in range(3):
            for half in range(2):
                source = (lane & 7) + (sub + half * 8) * 8
                acc = jnp.zeros((8, LANES), F32)
                for v in range(6):
                    at = v % 2 * 3 + blk
                    line = bcast_row(D, side, v // 2, slice(at, at + 1), slice(None))
                    moved = jnp.take_along_axis(line, source, axis=1)
                    acc = jnp.where((group == v) | (group == v + 6), moved, acc)
                rows = pl.ds((blk * 16 + half * 8) * LANES + column, 8, stride=LANES)
                G[rows, :] = G[rows, :] + acc


def return_all(inv, G, S2, S2_rows, R2, ssem, rsem):
    row, col = lax.axis_index("row"), lax.axis_index("col")
    cols = [lax.rem(col + d, 8) for d in range(8)]
    me = me_index()
    low = lax.broadcasted_iota(jnp.int32, (1, LANES), 1) < W
    lane = lane_ids()

    def collect(b, there):
        for u in range(8):
            f = there * 8 + u
            for rr in range(8):
                k = b * 16 + rr % 2 * 8 + rr // 2 * 2
                even = G[pl.ds(inv[f, k], 1), :]
                odd = G[pl.ds(inv[f, k + 1], 1), :]
                S2_rows[pl.ds(b * 1024 + f * 8 + rr, 1), :] = jnp.where(low, even, odd)

    def fold_start(b, there):
        base = b * 1024 + there * 64
        done = []
        for h in range(2):
            d = S2_rows[pl.ds(base + 6 + h, 8, stride=8), :]
            for m, moved in enumerate(
                (
                    pltpu.roll(d, 96, 1),
                    pltpu.roll(d, 48, 1),
                    jnp.where(lane < 112, pltpu.roll(d, 64, 1), pltpu.roll(d, 32, 1)),
                )
            ):
                rows = pl.ds(base + 2 * m + h, 8, stride=8)
                done.append((rows, jnp.where(lane >= 96, moved, S2_rows[rows, :])))
        return done

    def fold_end(done):
        for rows, x in done:
            S2_rows[rows, :] = x

    def send(b, there):
        def one(c):
            pltpu.make_async_remote_copy(
                S2.at[b, there * 8 + c, pl.ds(0, 6)],
                R2.at[b, me, pl.ds(0, 6)],
                ssem.at[b],
                rsem.at[b],
                device_id=(there, c),
                device_id_type=MESH,
            ).start()

        for c in cols[1:]:
            one(c)
        pl.when(there != row)(lambda: one(cols[0]))

    def peer(d):
        group = d // 4
        far = jnp.where(group == 0, 2, jnp.where(group == 1, 1, jnp.where(group == 2, 3, 0)))
        return peer_row(row, far, 3 - lax.rem(d, 4))

    for b in range(CHUNKS):
        collect(b, peer(0))
        done = fold_start(b, peer(0))
        if b > 0:
            send(b - 1, peer(15))
        collect(b, peer(1))
        fold_end(done)

        def step(d, c, b=b):
            done = fold_start(b, peer(d - 1))
            collect(b, peer(d))
            fold_end(done)
            send(b, peer(d - 2))
            return c

        lax.fori_loop(2, 16, step, 0)
        fold_end(fold_start(b, peer(15)))
        send(b, peer(14))
        R2[b, me] = S2[b, me]
    send(CHUNKS - 1, peer(15))


def spread_chunk(b, R2d, Y):
    for h in range(2):
        k8 = b * 16 + 8 * h
        six, seven = (k8 + 6) * W, (k8 + 7) * W
        for m in range(3):
            parts = [
                R2d[pl.ds(b * 1024 + t0 * 64 + 2 * m + h, 8, stride=8), :] for t0 in range(16)
            ]
            turned = jnp.concatenate(parts, axis=0).T
            at = (k8 + 2 * m) * W
            Y[at : at + 96, :] = turned[0:96]
            if m == 0:
                Y[six : six + 32, :] = turned[96:128]
            elif m == 1:
                Y[seven : seven + 32, :] = turned[96:128]
            else:
                Y[six + 32 : six + 48, :] = turned[96:112]
                Y[seven + 32 : seven + 48, :] = turned[112:128]


def coarse_kernel(
    r_hbm,
    w_hbm,
    pat_hbm,
    ca_hbm,
    binv_hbm,
    off_hbm,
    opat_hbm,
    x_out,
    Y,
    w,
    pat,
    r,
    ca,
    binv,
    off,
    opat,
    A,
    S,
    R,
    S2,
    R2,
    G,
    G0,
    G1,
    rhs,
    X,
    U,
    E,
    H,
    D,
    coup,
    pc,
    pb,
    slot_v,
    odd,
    inv_v,
    slot,
    inv,
    load_sem,
    small_sem,
    slot_sem,
    inv_sem,
    s1,
    r1,
    s2,
    r2,
    hs,
    hr,
):
    small = [
        pltpu.make_async_copy(x, y, small_sem.at[n])
        for n, (x, y) in enumerate(
            [
                (pat_hbm, pat),
                (ca_hbm, ca),
                (binv_hbm, binv),
                (off_hbm, off),
                (opat_hbm, opat),
            ]
        )
    ]
    loads = []
    for b in range(CHUNKS):
        for p in range(FPA):
            n = pl.ds(p * AGG + b * 2048, 2048)
            loads.append((b, r_hbm.at[:, :, n], r.at[:, :, n], load_sem.at[0, b, p]))
            loads.append((b, w_hbm.at[:, :, n], w.at[:, :, n], load_sem.at[1, b, p]))
    loads = [(b, pltpu.make_async_copy(x, y, z)) for b, x, y, z in loads]
    def load(b):
        for at, copy in loads:
            if at == b:
                copy.start()

    small[0].start()
    load(0)
    start_barrier()
    load(1)

    S_rows, R_rows = S.reshape(CHUNKS * 1024, LANES), R.reshape(CHUNKS * 1024, LANES)
    S2_rows, R2_rows = S2.reshape(CHUNKS * 1024, LANES), R2.reshape(CHUNKS * 1024, LANES)
    small[0].wait()
    for b in range(CHUNKS):
        for at, copy in loads:
            if at == b:
                copy.wait()
        if b == 0:
            load(2)
            for copy in small[1:5]:
                copy.start()
        restrict_chunk(b, r, w, pat, A)
        pack_chunk(b, A, S_rows)
        if b == 0:
            end_barrier()
        send_chunk(S, R, b, s1, r1)
        keep_own(S, R, b)

    for copy in small[1:5]:
        copy.wait()
    E[...] = jnp.zeros(E.shape, F32)
    pc[...] = jnp.zeros(pc.shape, F32)
    pb[...] = jnp.zeros(pb.shape, F32)
    inv_v[...] = jnp.zeros(inv_v.shape, jnp.int32)
    index_tables(ca, slot_v, odd, inv_v)
    inv_copy = pltpu.make_async_copy(inv_v, inv, inv_sem)
    inv_copy.start()
    for n in range(2):
        slot_copy(n, n, slot_v, slot, slot_sem).start()
    couplings(off, opat, binv, coup, pc, pb)
    inv_copy.wait()

    for b in range(CHUNKS):
        wait_chunk(R, b, r1)
        unfold_chunk(b, R_rows)
    gather_cells(slot_v, slot, slot_sem, R_rows, (G0, G1), odd, rhs, binv, X)

    halos = [halo_copies(s, X, U, E, H, hs, hr) for s in range(3)]
    start_copies(halos[0][:2])
    pack_edges(0, X, E)
    start_copies(halos[0][2:])
    ends = ((0, 0, 0), (NI - 1, 2, 15))
    for s in range(3):
        if s < 2:

            def new_at(row, v, s=s):
                return X.at[s + 1, pl.ds(pl.multiple_of(row * W + W + v * 8, 8), 8)]
        else:

            def new_at(row, v):
                return x_out.at[pl.ds(pl.multiple_of(row * W + v * 8, 8), 8)]

        def inner(two, c, s=s, new_at=new_at):
            for u in range(2):
                row = 1 + two * 2 + u
                new = solve_block(binv, row, row_total(s, row, rhs, coup, X))
                for v in range(6):
                    new_at(row, v)[...] = new[v // 2][v % 2]
            return c

        lax.fori_loop(0, (NI - 2) // 2, inner, 0)
        totals = [row_total(s, row, rhs, coup, X, skip=d) for d, (row, _, _) in enumerate(ends)]
        if s < 2:
            pack_edges(s + 1, X, E, ends=False)
        else:

            def turn(part, c):
                for u in range(23):
                    planes_to_cells(1 + part * 23 + u, x_out, G)
                return c

            lax.fori_loop(0, 2, turn, 0)
        finish_copies(halos[s][:2])
        new = []
        for d, (row, _, _) in enumerate(ends):
            near = [X[s, pl.ds((row + 2 * d) * W + v * 8, 8), :] for v in range(6)]
            new.append(solve_block(binv, row, less_direction(d, row, coup, near, totals[d])))
            for v in range(6):
                new_at(row, v)[...] = new[d][v // 2][v % 2]
        if s < 2:
            for d, (_, blk, n) in enumerate(ends):
                patch_edges(s + 1, blk, n, new[d], E)
        else:
            for row in (0, NI - 1):
                planes_to_cells(row, x_out, G)
        finish_copies(halos[s][2:])
        correct_edges(s, H, pc, pb, D)
        if s < 2:
            for side in range(2):
                E[side, s + 1] = E[side, s + 1] + D[side]
            start_copies(halos[s + 1][2:])
            for d, (_, blk, n) in enumerate(ends):
                more = edge_lanes(blk, n, D)
                for v in range(6):
                    U[s, d, v * 8 : v * 8 + 8, :] = new[d][v // 2][v % 2] + more[v]
            start_copies(halos[s + 1][:2])
            for blk in range(3):
                add_edges(blk, D, new_at)
        else:
            correct_cells(D, G)

    return_all(inv, G, S2, S2_rows, R2, s2, r2)
    for blk in range(3):
        add_edges(blk, D, new_at)
    for b in range(CHUNKS):
        wait_chunk(R2, b, r2)
        spread_chunk(b, R2_rows, Y)

    for b in range(CHUNKS):
        wait_chunk(R, b, s1)
        wait_chunk(R, b, s2)
    for copies in halos:
        for sends, _, copy, _ in copies:
            pl.when(sends)(copy.wait_send)


def prolong_kernel(y, x, w, pat, out, planes_out, fine, planes, sem, psem):
    def line(row, c):
        for v in range(6):
            at = (v % 2 * 24 + v // 2) * NI + row
            planes[pl.ds(at, 8, stride=3 * NI), :] = x[pl.ds(row * W + v * 8, 8), :]
        return c

    lax.fori_loop(0, NI, line, 0)
    plane_copy = pltpu.make_async_copy(planes, planes_out, psem)
    plane_copy.start()

    def copies(p):
        n = pl.ds(pl.multiple_of(p * AGG, AGG), AGG)
        return [
            pltpu.make_async_copy(fine.at[j, :, n], out.at[j, :, n], sem.at[p, j])
            for j in range(3)
        ]

    def block(p, c):
        def some(blk, c):
            for u in range(4):
                k = blk * 4 + u
                at = pl.ds(pl.multiple_of(p * AGG + k * LANES, LANES), LANES)
                base = pl.multiple_of(k * W, 8)
                there = bcast_row(pat, pl.ds(p * NK + k, 1), slice(None)).astype(F32)
                src = [
                    [y[pl.ds(base + i * 16 + qg * 8, 8), :] * there for qg in range(2)]
                    for i in range(3)
                ]
                for j in range(3):
                    acc = None
                    for i in range(3):
                        wij = jnp.broadcast_to(w[i, j : j + 1, at], (8, LANES))
                        terms = [wij * src[i][qg] for qg in range(2)]
                        acc = terms if acc is None else [a + z for a, z in zip(acc, terms)]
                    for qg in range(2):
                        fine[j, qg * 8 : qg * 8 + 8, at] = acc[qg]
            return c

        lax.fori_loop(0, NK // 4, some, 0)
        for copy in copies(p):
            copy.start()
        return c

    lax.fori_loop(0, FPA, block, 0)
    plane_copy.wait()

    def finish(p, c):
        for copy in copies(p):
            copy.wait()
        return c

    lax.fori_loop(0, FPA, finish, 0)


def body(residual, restriction, pattern, cell_aggregate, block_inverse, off_blocks, op_pattern):
    turned = residual.transpose(1, 0, 2)
    pat = pattern.reshape(384, LANES)
    vmem = pl.BlockSpec(memory_space=pltpu.VMEM)
    hbm = pl.BlockSpec(memory_space=pltpu.HBM)
    msg = pltpu.VMEM((CHUNKS, ND, 8, LANES), F32)
    plane = pltpu.VMEM((NI * W, LANES), F32)
    edge = pltpu.VMEM((2, 3, 3, 8, LANES), F32)
    x, y, held, held_pat = pl.pallas_call(
        coarse_kernel,
        out_shape=(
            jax.ShapeDtypeStruct((NI * W, LANES), F32),
            jax.ShapeDtypeStruct((NK * W, LANES), F32),
            jax.ShapeDtypeStruct((3, 3, FPA * AGG), F32),
            jax.ShapeDtypeStruct((384, LANES), jnp.int32),
        ),
        in_specs=[hbm] * 7,
        out_specs=(vmem,) * 4,
        scratch_shapes=[
            pltpu.VMEM((3, NQ, FPA * AGG), F32),
            pltpu.VMEM((NI, LANES), jnp.int32),
            pltpu.VMEM((9, NI, LANES), F32),
            pltpu.VMEM((36, NI, LANES), F32),
            pltpu.VMEM((4, NI, LANES), jnp.int32),
            plane,
            msg,
            msg,
            msg,
            msg,
            pltpu.VMEM((AGG, LANES), F32),
            pltpu.VMEM((8 * LANES, LANES), F32),
            pltpu.VMEM((8 * LANES, LANES), F32),
            plane,
            pltpu.VMEM((3, (NI + 2) * W, LANES), F32),
            pltpu.VMEM((2, 2, W, LANES), F32),
            edge,
            edge,
            pltpu.VMEM((2, 3, 8, LANES), F32),
            pltpu.VMEM((36, NI, LANES), F32),
            pltpu.VMEM((2, 9, 8, LANES), F32),
            pltpu.VMEM((2, 9, 8, LANES), F32),
            pltpu.VMEM((NI, LANES), jnp.int32),
            pltpu.VMEM((NI, LANES), jnp.int32),
            pltpu.VMEM((ND, LANES), jnp.int32),
            pltpu.SMEM((2, 8, LANES), jnp.int32),
            pltpu.SMEM((ND, LANES), jnp.int32),
            pltpu.SemaphoreType.DMA((2, CHUNKS, FPA)),
            pltpu.SemaphoreType.DMA((5,)),
            pltpu.SemaphoreType.DMA((2,)),
            pltpu.SemaphoreType.DMA,
            pltpu.SemaphoreType.DMA((CHUNKS,)),
            pltpu.SemaphoreType.DMA((CHUNKS,)),
            pltpu.SemaphoreType.DMA((CHUNKS,)),
            pltpu.SemaphoreType.DMA((CHUNKS,)),
            pltpu.SemaphoreType.DMA((3, 4)),
            pltpu.SemaphoreType.DMA((3, 4)),
        ],
        compiler_params=pltpu.CompilerParams(
            collective_id=0, has_side_effects=True, vmem_limit_bytes=46 * 1024 * 1024
        ),
    )(
        *[
            pltpu.with_memory_space_constraint(x, pltpu.HBM)
            for x in (
                turned,
                restriction,
                pat,
                cell_aggregate,
                block_inverse.reshape(9, NI, LANES),
                off_blocks.reshape(36, NI, LANES),
                op_pattern,
            )
        ]
    )
    fine, planes = pl.pallas_call(
        prolong_kernel,
        out_shape=(
            jax.ShapeDtypeStruct((3, NQ, FPA * AGG), F32),
            jax.ShapeDtypeStruct((NQ * 3 * NI, LANES), F32),
        ),
        in_specs=[vmem] * 4,
        out_specs=(hbm, hbm),
        scratch_shapes=[
            pltpu.VMEM((3, NQ, FPA * AGG), F32),
            pltpu.VMEM((NQ * 3 * NI, LANES), F32),
            pltpu.SemaphoreType.DMA((FPA, 3)),
            pltpu.SemaphoreType.DMA,
        ],
        compiler_params=pltpu.CompilerParams(vmem_limit_bytes=24 * 1024 * 1024),
    )(y, x, held, held_pat)
    return planes.reshape(NQ, 3, NI, LANES), fine.transpose(1, 0, 2)


def solution(mesh):
    in_specs = (
        P(None, None, ("row", "col")),
        P(None, None, ("row", "col")),
        P(("row", "col")),
        P("row", "col"),
        P(None, None, "row", "col"),
        P(None, None, None, "row", "col"),
        P(None, "row", "col"),
    )
    out_specs = (P(None, None, "row", "col"), P(None, None, ("row", "col")))
    return jax.shard_map(body, mesh=mesh, in_specs=in_specs, out_specs=out_specs, check_vma=False)
```

```python
import functools

import jax
import jax.numpy as jnp
from jax import lax
from jax.experimental import pallas as pl
from jax.experimental.pallas import tpu as pltpu
from jax.sharding import PartitionSpec as P

MESH = pl.DeviceIdType.MESH
ND = 128
NQ = 16
NI = 48
NK = 48
W = 48
AGG = 6144
FPA = 8
CHUNKS = 3
LANES = 128
F32 = jnp.float32


def me_index():
    return lax.axis_index("row") * 8 + lax.axis_index("col")


def lane_ids():
    return lax.broadcasted_iota(jnp.int32, (8, LANES), 1)


def bcast_row(ref, *idx):
    return jnp.broadcast_to(ref[idx], (8, LANES))


def peer_row(row, far, near):
    z = lax.rem(row // 4 + far, 4)
    return z * 4 + lax.rem(lax.rem(row, 4) + near, 4)


def each_peer(visit):
    row, col = lax.axis_index("row"), lax.axis_index("col")
    cols = [lax.rem(col + d, 8) for d in (2, 6, 1, 3, 5, 7, 4, 0)]
    for far in (2, 1, 3, 0):

        def one(n, c, far=far):
            there = peer_row(row, far, 3 - n)
            for other in cols:
                visit(there, other)
            return c

        lax.fori_loop(0, 4 if far else 3, one, 0)
    for other in cols[:-1]:
        visit(row, other)


def start_barrier():
    bar = pltpu.get_barrier_semaphore()
    each_peer(
        lambda row, col: pl.semaphore_signal(
            bar, inc=1, device_id=(row, col), device_id_type=MESH
        )
    )


def end_barrier():
    pl.semaphore_wait(pltpu.get_barrier_semaphore(), ND - 1)


def send_chunk(S, R, b, ssem, rsem):
    dst = R.at[b, me_index(), pl.ds(0, 6)]

    def visit(row, col):
        pltpu.make_async_remote_copy(
            S.at[b, row * 8 + col, pl.ds(0, 6)],
            dst,
            ssem.at[b],
            rsem.at[b],
            device_id=(row, col),
            device_id_type=MESH,
        ).start()

    each_peer(visit)


def wait_chunk(R, b, sem):
    block = R.at[b, pl.ds(0, ND - 1), pl.ds(0, 6)]
    pltpu.make_async_copy(block, block, sem.at[b]).wait()


def keep_own(S, R, b):
    me = me_index()
    R[b, me] = S[b, me]


def restrict_chunk(b, r, w, pat, A):
    def one(kk, c):
        k = b * 16 + kk
        acc = [[None] * 2 for _ in range(3)]
        for p in range(FPA):
            n = pl.multiple_of(p * AGG + k * LANES, LANES)
            there = bcast_row(pat, pl.ds(p * 48 + k, 1), slice(None)).astype(F32)
            here = [
                [r[j, qg * 8 : qg * 8 + 8, pl.ds(n, LANES)] * there for qg in range(2)]
                for j in range(3)
            ]
            for i in range(3):
                for j in range(3):
                    wij = jnp.broadcast_to(w[i, j : j + 1, pl.ds(n, LANES)], (8, LANES))
                    for qg in range(2):
                        term = wij * here[j][qg]
                        acc[i][qg] = term if acc[i][qg] is None else acc[i][qg] + term
        for i in range(3):
            for qg in range(2):
                at = pl.multiple_of(k * W + i * 16 + qg * 8, 8)
                A[pl.ds(at, 8), :] = acc[i][qg]
        return c

    lax.fori_loop(0, 16, one, 0)


def pack_chunk(b, A, S2d):
    for h in range(2):
        k8 = b * 16 + 8 * h
        six, seven = (k8 + 6) * W, (k8 + 7) * W
        for m in range(3):
            at = (k8 + 2 * m) * W
            head = A[at : at + 96, :]
            if m == 0:
                tail = [A[six : six + 32, :]]
            elif m == 1:
                tail = [A[seven : seven + 32, :]]
            else:
                tail = [A[six + 32 : six + 48, :], A[seven + 32 : seven + 48, :]]
            turned = jnp.concatenate([head] + tail, axis=0).T
            for t0 in range(16):
                rows = pl.ds(b * 1024 + t0 * 64 + 2 * m + h, 8, stride=8)
                S2d[rows, :] = turned[t0 * 8 : t0 * 8 + 8, :]


def unfold_chunk(b, R2d):
    lane = lane_ids()

    def one(fb, c):
        for base, h in [(b * 1024 + (fb * 8 + u) * 64, h) for u in range(8) for h in range(2)]:
            x0 = R2d[pl.ds(base + h, 8, stride=8), :]
            x1 = R2d[pl.ds(base + 2 + h, 8, stride=8), :]
            x2 = R2d[pl.ds(base + 4 + h, 8, stride=8), :]
            six = jnp.where(lane < 32, pltpu.roll(x0, 32, 1), pltpu.roll(x2, 64, 1))
            seven = jnp.where(lane < 80, pltpu.roll(x1, 80, 1), pltpu.roll(x2, 96, 1))
            R2d[pl.ds(base + 6 + h, 8, stride=8), :] = jnp.where(lane < 48, six, seven)
        return c

    lax.fori_loop(0, 2, one, 0)


def index_tables(ca, slot_v, odd, inv_v):
    def one(blk, acc):
        rows = pl.ds(pl.multiple_of(blk * 8, 8), 8)
        pair = lax.shift_right_logical(ca[rows, :], 7)
        owner = lax.shift_right_logical(lax.shift_right_logical(pair, 4) * 171, 9)
        local = pair - owner * NK
        bit = [lax.shift_right_logical(local, n) & 1 for n in range(4)]
        chunk = lax.shift_right_logical(local, 4)
        at = chunk * 1024 + owner * 8 + (bit[2] * 2 + bit[1]) * 2 + bit[3]
        slot_v[rows, :] = jnp.clip(at, 0, CHUNKS * 1024 - 1)
        odd[rows, :] = bit[0]
        for u in range(8):
            who = jnp.broadcast_to(owner[u : u + 1], (ND, LANES))
            by_owner = (who == lax.broadcasted_iota(jnp.int32, (ND, LANES), 0)).astype(F32)
            which = jnp.broadcast_to(local[u : u + 1], (NK, LANES))
            here = which == lax.broadcasted_iota(jnp.int32, (NK, LANES), 0)
            column = lax.broadcasted_iota(jnp.int32, (NK, LANES), 1).astype(F32)
            line = (blk * 8 + u).astype(F32)
            cells = jnp.concatenate(
                [jnp.where(here, column, 0.0), jnp.where(here, line, 0.0)], axis=0
            )
            acc = acc + lax.dot_general(
                by_owner.astype(jnp.bfloat16),
                cells.astype(jnp.bfloat16),
                (((1,), (1,)), ((), ())),
                preferred_element_type=F32,
            )
        return acc

    acc = lax.fori_loop(0, NI // 8, one, jnp.zeros((ND, 2 * NK), F32))
    cell = (acc[:, NK:] * LANES + acc[:, :NK]).astype(jnp.int32)
    inv_v[:, 0:NK] = jnp.clip(cell, 0, AGG - 1)


def solve_block(binv, row, total):
    out = []
    for i in range(3):
        acc = None
        for j in range(3):
            coef = bcast_row(binv, i * 3 + j, pl.ds(row, 1), slice(None))
            terms = [coef * total[j][qg] for qg in range(2)]
            acc = terms if acc is None else [x + y for x, y in zip(acc, terms)]
        out.append(acc)
    return out


def early_edges(slot, R2d, T, edge_odd, pb, D, E):
    for side, column in ((0, 0), (1, LANES - 1)):
        for row in range(NI):
            T[side * 64 + row : side * 64 + row + 1, :] = R2d[pl.ds(slot[row, column], 1), :]
    turned = T[...].T
    is_odd = bcast_row(edge_odd, slice(0, 1), slice(None)) > 0.5
    lane = lane_ids()
    here = lax.broadcasted_iota(jnp.int32, (8, LANES), 0) == (lane & 7)
    D[...] = jnp.zeros(D.shape, F32)
    for v in range(6):
        at = v * 8
        cells = jnp.where(is_odd, turned[W + at : W + at + 8, :], turned[at : at + 8, :])
        for side in range(2):
            for blk in range(3):
                source = lax.shift_right_logical(lane, 3) + (side * 64 + blk * 16)
                moved = jnp.where(here, jnp.take_along_axis(cells, source, axis=1), 0.0)
                n = v % 2 * 3 + blk
                D[side, v // 2, n : n + 1, :] = jnp.sum(moved, axis=0, keepdims=True)
    for side in range(2):
        for i in range(3):
            acc = None
            for j in range(3):
                term = pb[side, i * 3 + j] * D[side, j]
                acc = term if acc is None else acc + term
            E[side, 0, i] = acc


def slot_copy(blk, n, slot_v, slot, sem):
    rows = pl.ds(pl.multiple_of(blk * 8, 8), 8)
    return pltpu.make_async_copy(slot_v.at[rows], slot.at[n], sem.at[n])


def nth_block(n):
    return jnp.where(n == 0, 0, jnp.where(n == 1, 5, n - 1))


def gather_cells(slot_v, slot, sem, R2d, near, odd, rhs, binv, X, ends_done):
    def fetch(step, n):
        slot_copy(nth_block(step), n, slot_v, slot, sem).wait()
        for u in range(8):
            for k in range(LANES):
                near[n][pl.ds(u * LANES + k, 1), :] = R2d[pl.ds(slot[n, u, k], 1), :]

    def planes(step, n):
        for u in range(8):
            row = nth_block(step) * 8 + u
            base = pl.multiple_of(row * W, 8)
            turned = near[n][pl.ds(u * LANES, LANES), :].T
            is_odd = bcast_row(odd, pl.ds(row, 1), slice(None)) == 1
            total = [[None] * 2 for _ in range(3)]
            for v in range(6):
                here = jnp.where(
                    is_odd, turned[W + v * 8 : W + v * 8 + 8, :], turned[v * 8 : v * 8 + 8, :]
                )
                rhs[pl.ds(base + v * 8, 8), :] = here
                total[v // 2][v % 2] = here
            new = solve_block(binv, row, total)
            for v in range(6):
                X[0, pl.ds(base + W + v * 8, 8), :] = new[v // 2][v % 2]

    fetch(0, 0)
    slot_copy(nth_block(2), 0, slot_v, slot, sem).start()

    def some(two, c):
        blk = two * 2 + 1
        fetch(blk, 1)
        planes(blk - 1, 0)
        slot_copy(nth_block(jnp.minimum(blk + 2, 5)), 1, slot_v, slot, sem).start()
        fetch(blk + 1, 0)
        planes(blk, 1)
        slot_copy(nth_block(jnp.minimum(blk + 3, 5)), 0, slot_v, slot, sem).start()
        pl.when(two == 0)(ends_done)
        return c

    lax.fori_loop(0, 2, some, 0)
    fetch(5, 1)
    planes(4, 0)
    slot_copy(nth_block(5), 0, slot_v, slot, sem).wait()
    planes(5, 1)


def couplings(off, opat, binv, coup, pc, pb):
    def couple(blk, c):
        at = pl.ds(pl.multiple_of(blk * 8, 8), 8)
        for d in range(4):
            there = opat[d, at, :].astype(F32)
            for e in range(9):
                coup[d * 9 + e, at, :] = off[d * 9 + e, at, :] * there
        return c

    lax.fori_loop(0, NI // 8, couple, 0)

    def pack(e, c):
        for blk in range(3):
            for src, plane, keep in (
                (coup, 18 + e, (0,)),
                (coup, 27 + e, (1,)),
                (binv, e, (0, 1)),
            ):
                parts = [
                    bcast_row(src, plane, slice(blk * 16 + n, blk * 16 + n + 1), slice(None))
                    for n in range(16)
                ]
                turned = jnp.concatenate(parts, axis=0).T
                for side in keep:
                    line = turned[0:1] if side == 0 else turned[LANES - 1 : LANES]
                    dst = pb if src is binv else pc
                    for qg in range(2):
                        dst[side, e, qg * 3 + blk : qg * 3 + blk + 1, :] = line
        return c

    lax.fori_loop(0, 9, pack, 0)

    def mask(e, c):
        lane = lax.broadcasted_iota(jnp.int32, (NI, LANES), 1)
        coup[18 + e] = jnp.where(lane == 0, 0.0, coup[18 + e])
        coup[27 + e] = jnp.where(lane == LANES - 1, 0.0, coup[27 + e])
        return c

    lax.fori_loop(0, 9, mask, 0)


def pack_edges(s, X, E, ends=True):
    zero = jnp.zeros((8, LANES), F32)
    for blk in range(3):
        for v in range(6):
            rows = [blk * 16 + n for n in range(16)]
            parts = [
                X[s, (row + 1) * W + v * 8 : (row + 1) * W + v * 8 + 8, :]
                if ends or 0 < row < NI - 1
                else zero
                for row in rows
            ]
            turned = jnp.concatenate(parts, axis=0).T
            at = v % 2 * 3 + blk
            E[0, s, v // 2, at : at + 1, :] = turned[0:1]
            E[1, s, v // 2, at : at + 1, :] = turned[LANES - 1 : LANES]


def patch_edges(s, blk, n, new, E):
    here = lane_ids() == lax.broadcasted_iota(jnp.int32, (8, LANES), 0) + 8 * n
    for v in range(6):
        at = v % 2 * 3 + blk
        x = new[v // 2][v % 2]
        for side, column in enumerate((x[:, 0:1], x[:, LANES - 1 : LANES])):
            line = jnp.sum(jnp.where(here, column, 0.0), axis=0, keepdims=True)
            E[side, s, v // 2, at : at + 1, :] = E[side, s, v // 2, at : at + 1, :] + line


def halo_copies(s, X, U, E, H, hs, hr):
    row, col = lax.axis_index("row"), lax.axis_index("col")
    own_first = X.at[s, pl.ds(W, W)] if s == 0 else U.at[s - 1, 0]
    own_last = X.at[s, pl.ds(NI * W, W)] if s == 0 else U.at[s - 1, 1]
    above = X.at[s, pl.ds(0, W)]
    below = X.at[s, pl.ds((NI + 1) * W, W)]
    table = [
        (row > 0, row < 15, own_first, below, (row - 1, col)),
        (row < 15, row > 0, own_last, above, (row + 1, col)),
        (col > 0, col < 7, E.at[0, s], H.at[1, s], (row, col - 1)),
        (col < 7, col > 0, E.at[1, s], H.at[0, s], (row, col + 1)),
    ]
    return [
        (
            sends,
            receives,
            pltpu.make_async_remote_copy(
                src, dst, hs.at[s, n], hr.at[s, n], device_id=dev, device_id_type=MESH
            ),
            dst,
        )
        for n, (sends, receives, src, dst, dev) in enumerate(table)
    ]


def start_copies(copies):
    for sends, _, copy, _ in copies:
        pl.when(sends)(copy.start)


def finish_copies(copies):
    for _, receives, copy, dst in copies:
        pl.when(receives)(copy.wait_recv)

        def clear(dst=dst):
            dst[...] = jnp.zeros(dst.shape, F32)

        pl.when(jnp.logical_not(receives))(clear)


def row_total(s, row, rhs, coup, X, skip=None):
    base = pl.multiple_of(row * W, 8)

    def at(v):
        return pl.ds(base + v * 8, 8)

    own = [X[s, at(v + 6), :] for v in range(6)]
    left = [pltpu.roll(x, 1, 1) for x in own]
    right = [pltpu.roll(x, LANES - 1, 1) for x in own]
    total = [[rhs[at(j * 2 + qg), :] for qg in range(2)] for j in range(3)]
    for d in range(4):
        if d == skip:
            continue
        if d < 2:
            near = [X[s, at(v + 12 * d), :] for v in range(6)]
        else:
            near = left if d == 2 else right
        total = less_direction(d, row, coup, near, total)
    return total


def less_direction(d, row, coup, near, total):
    total = [list(t) for t in total]
    for k in range(3):
        for j in range(3):
            coef = bcast_row(coup, d * 9 + j * 3 + k, pl.ds(row, 1), slice(None))
            for qg in range(2):
                total[j][qg] = total[j][qg] - coef * near[k * 2 + qg]
    return total


def edge_lanes(blk, n, D):
    lane = lane_ids()
    here = lane == lax.broadcasted_iota(jnp.int32, (8, LANES), 0) + 8 * n
    out = []
    for v in range(6):
        at = v % 2 * 3 + blk
        ends = []
        for side in range(2):
            line = bcast_row(D, side, v // 2, slice(at, at + 1), slice(None))
            ends.append(jnp.sum(jnp.where(here, line, 0.0), axis=1, keepdims=True))
        out.append(jnp.where(lane == 0, ends[0], jnp.where(lane == LANES - 1, ends[1], 0.0)))
    return out


def correct_edges(s, H, pc, pb, D):
    for side in range(2):
        push = []
        for j in range(3):
            acc = None
            for k in range(3):
                term = pc[side, j * 3 + k] * H[side, s, k]
                acc = term if acc is None else acc + term
            push.append(acc)
        for i in range(3):
            acc = None
            for j in range(3):
                term = pb[side, i * 3 + j] * push[j]
                acc = term if acc is None else acc + term
            D[side, i] = -acc


def add_edges(blk, D, new_at):
    sub = lax.broadcasted_iota(jnp.int32, (8, LANES), 0)
    zero = jnp.zeros((LANES - 16, LANES), F32)
    for v in range(6):
        at = v % 2 * 3 + blk
        first = jnp.where(sub == 0, bcast_row(D, 0, v // 2, slice(at, at + 1), slice(None)), 0.0)
        last = jnp.where(sub == 7, bcast_row(D, 1, v // 2, slice(at, at + 1), slice(None)), 0.0)
        turned = jnp.concatenate([first, zero, last], axis=0).T
        for n in range(16):
            ref = new_at(blk * 16 + n, v)
            ref[...] = ref[...] + turned[n * 8 : n * 8 + 8]


def planes_to_cells(row, last, G):
    x = last[pl.ds(pl.multiple_of(row * W, 8), W), :]
    turned = jnp.concatenate([x, x], axis=0).T
    G[pl.ds(pl.multiple_of(row * LANES, LANES), LANES), 0 : 2 * W] = turned


def correct_cells(D, G):
    lane = lane_ids()
    sub = lax.broadcasted_iota(jnp.int32, (8, LANES), 0)
    group = lax.shift_right_logical(lane, 3)
    for side, column in ((0, 0), (1, LANES - 1)):
        for blk in range(3):
            for half in range(2):
                source = (lane & 7) + (sub + half * 8) * 8
                acc = jnp.zeros((8, LANES), F32)
                for v in range(6):
                    at = v % 2 * 3 + blk
                    line = bcast_row(D, side, v // 2, slice(at, at + 1), slice(None))
                    moved = jnp.take_along_axis(line, source, axis=1)
                    acc = jnp.where((group == v) | (group == v + 6), moved, acc)
                rows = pl.ds((blk * 16 + half * 8) * LANES + column, 8, stride=LANES)
                G[rows, :] = G[rows, :] + acc


def return_all(inv, G, S2, S2_rows, R2, ssem, rsem):
    row, col = lax.axis_index("row"), lax.axis_index("col")
    cols = [lax.rem(col + d, 8) for d in range(8)]
    me = me_index()
    low = lax.broadcasted_iota(jnp.int32, (1, LANES), 1) < W
    lane = lane_ids()

    def collect(b, there):
        for u in range(8):
            f = there * 8 + u
            for rr in range(8):
                k = b * 16 + rr % 2 * 8 + rr // 2 * 2
                even = G[pl.ds(inv[f, k], 1), :]
                odd = G[pl.ds(inv[f, k + 1], 1), :]
                S2_rows[pl.ds(b * 1024 + f * 8 + rr, 1), :] = jnp.where(low, even, odd)

    def fold_start(b, there):
        base = b * 1024 + there * 64
        done = []
        for h in range(2):
            d = S2_rows[pl.ds(base + 6 + h, 8, stride=8), :]
            for m, moved in enumerate(
                (
                    pltpu.roll(d, 96, 1),
                    pltpu.roll(d, 48, 1),
                    jnp.where(lane < 112, pltpu.roll(d, 64, 1), pltpu.roll(d, 32, 1)),
                )
            ):
                rows = pl.ds(base + 2 * m + h, 8, stride=8)
                done.append((rows, jnp.where(lane >= 96, moved, S2_rows[rows, :])))
        return done

    def fold_end(done):
        for rows, x in done:
            S2_rows[rows, :] = x

    def send(b, there):
        def one(c):
            pltpu.make_async_remote_copy(
                S2.at[b, there * 8 + c, pl.ds(0, 6)],
                R2.at[b, me, pl.ds(0, 6)],
                ssem.at[b],
                rsem.at[b],
                device_id=(there, c),
                device_id_type=MESH,
            ).start()

        for c in cols[1:]:
            one(c)
        pl.when(there != row)(lambda: one(cols[0]))

    def peer(d):
        group = d // 4
        far = jnp.where(group == 0, 2, jnp.where(group == 1, 1, jnp.where(group == 2, 3, 0)))
        return peer_row(row, far, 3 - lax.rem(d, 4))

    for b in range(CHUNKS):
        collect(b, peer(0))
        done = fold_start(b, peer(0))
        if b > 0:
            send(b - 1, peer(15))
        collect(b, peer(1))
        fold_end(done)

        def step(d, c, b=b):
            done = fold_start(b, peer(d - 1))
            collect(b, peer(d))
            fold_end(done)
            send(b, peer(d - 2))
            return c

        lax.fori_loop(2, 16, step, 0)
        fold_end(fold_start(b, peer(15)))
        send(b, peer(14))
        R2[b, me] = S2[b, me]
    send(CHUNKS - 1, peer(15))


def spread_chunk(b, R2d, Y):
    for h in range(2):
        k8 = b * 16 + 8 * h
        six, seven = (k8 + 6) * W, (k8 + 7) * W
        for m in range(3):
            parts = [
                R2d[pl.ds(b * 1024 + t0 * 64 + 2 * m + h, 8, stride=8), :] for t0 in range(16)
            ]
            turned = jnp.concatenate(parts, axis=0).T
            at = (k8 + 2 * m) * W
            Y[at : at + 96, :] = turned[0:96]
            if m == 0:
                Y[six : six + 32, :] = turned[96:128]
            elif m == 1:
                Y[seven : seven + 32, :] = turned[96:128]
            else:
                Y[six + 32 : six + 48, :] = turned[96:112]
                Y[seven + 32 : seven + 48, :] = turned[112:128]


def coarse_kernel(
    r_hbm,
    w_hbm,
    pat_hbm,
    ca_hbm,
    binv_hbm,
    off_hbm,
    opat_hbm,
    x_out,
    Y,
    w,
    pat,
    r,
    ca,
    binv,
    off,
    opat,
    A,
    S,
    R,
    S2,
    R2,
    G,
    G0,
    G1,
    T,
    edge_odd,
    rhs,
    X,
    U,
    E,
    H,
    D,
    coup,
    pc,
    pb,
    slot_v,
    odd,
    inv_v,
    slot,
    ring,
    inv,
    load_sem,
    small_sem,
    slot_sem,
    ring_sem,
    inv_sem,
    s1,
    r1,
    s2,
    r2,
    hs,
    hr,
):
    small = [
        pltpu.make_async_copy(x, y, small_sem.at[n])
        for n, (x, y) in enumerate(
            [
                (pat_hbm, pat),
                (ca_hbm, ca),
                (binv_hbm, binv),
                (off_hbm, off),
                (opat_hbm, opat),
            ]
        )
    ]
    loads = []
    for b in range(CHUNKS):
        for p in range(FPA):
            n = pl.ds(p * AGG + b * 2048, 2048)
            loads.append((b, r_hbm.at[:, :, n], r.at[:, :, n], load_sem.at[0, b, p]))
            loads.append((b, w_hbm.at[:, :, n], w.at[:, :, n], load_sem.at[1, b, p]))
    loads = [(b, pltpu.make_async_copy(x, y, z)) for b, x, y, z in loads]
    def load(b):
        for at, copy in loads:
            if at == b:
                copy.start()

    small[0].start()
    load(0)
    start_barrier()
    load(1)

    S_rows, R_rows = S.reshape(CHUNKS * 1024, LANES), R.reshape(CHUNKS * 1024, LANES)
    S2_rows, R2_rows = S2.reshape(CHUNKS * 1024, LANES), R2.reshape(CHUNKS * 1024, LANES)
    small[0].wait()
    for b in range(CHUNKS):
        for at, copy in loads:
            if at == b:
                copy.wait()
        if b == 0:
            load(2)
            for copy in small[1:5]:
                copy.start()
        restrict_chunk(b, r, w, pat, A)
        pack_chunk(b, A, S_rows)
        if b == 0:
            end_barrier()
        send_chunk(S, R, b, s1, r1)
        keep_own(S, R, b)

    for copy in small[1:5]:
        copy.wait()
    E[...] = jnp.zeros(E.shape, F32)
    pc[...] = jnp.zeros(pc.shape, F32)
    pb[...] = jnp.zeros(pb.shape, F32)
    inv_v[...] = jnp.zeros(inv_v.shape, jnp.int32)
    index_tables(ca, slot_v, odd, inv_v)
    inv_copy = pltpu.make_async_copy(inv_v, inv, inv_sem)
    inv_copy.start()
    all_slots = pltpu.make_async_copy(slot_v, slot, slot_sem)
    all_slots.start()
    for n in range(2):
        slot_copy(nth_block(n), n, slot_v, ring, ring_sem).start()
    both = jnp.concatenate([odd[...].astype(F32), jnp.zeros((16, LANES), F32)], axis=0)
    turned = jnp.concatenate([both, both], axis=0).T
    low = lax.broadcasted_iota(jnp.int32, (1, LANES), 1) < 64
    edge_odd[0:1, :] = jnp.where(low, turned[0:1], turned[LANES - 1 : LANES])
    T[...] = jnp.zeros(T.shape, F32)
    couplings(off, opat, binv, coup, pc, pb)
    inv_copy.wait()
    all_slots.wait()

    for b in range(CHUNKS):
        wait_chunk(R, b, r1)
        unfold_chunk(b, R_rows)
    halos = [halo_copies(s, X, U, E, H, hs, hr) for s in range(3)]
    early_edges(slot, R_rows, T, edge_odd, pb, D, E)
    start_copies(halos[0][2:])
    gather_cells(
        slot_v,
        ring,
        ring_sem,
        R_rows,
        (G0, G1),
        odd,
        rhs,
        binv,
        X,
        lambda: start_copies(halos[0][:2]),
    )
    ends = ((0, 0, 0), (NI - 1, 2, 15))
    for s in range(3):
        if s < 2:

            def new_at(row, v, s=s):
                return X.at[s + 1, pl.ds(pl.multiple_of(row * W + W + v * 8, 8), 8)]
        else:

            def new_at(row, v):
                return x_out.at[pl.ds(pl.multiple_of(row * W + v * 8, 8), 8)]

        def inner(two, c, s=s, new_at=new_at):
            for u in range(2):
                row = 1 + two * 2 + u
                new = solve_block(binv, row, row_total(s, row, rhs, coup, X))
                for v in range(6):
                    new_at(row, v)[...] = new[v // 2][v % 2]
            return c

        lax.fori_loop(0, (NI - 2) // 2, inner, 0)
        totals = [row_total(s, row, rhs, coup, X, skip=d) for d, (row, _, _) in enumerate(ends)]
        if s < 2:
            pack_edges(s + 1, X, E, ends=False)
        else:

            def turn(part, c):
                for u in range(23):
                    planes_to_cells(1 + part * 23 + u, x_out, G)
                return c

            lax.fori_loop(0, 2, turn, 0)
        finish_copies(halos[s][:2])
        new = []
        for d, (row, _, _) in enumerate(ends):
            near = [X[s, pl.ds((row + 2 * d) * W + v * 8, 8), :] for v in range(6)]
            new.append(solve_block(binv, row, less_direction(d, row, coup, near, totals[d])))
            for v in range(6):
                new_at(row, v)[...] = new[d][v // 2][v % 2]
        if s < 2:
            for d, (_, blk, n) in enumerate(ends):
                patch_edges(s + 1, blk, n, new[d], E)
        else:
            for row in (0, NI - 1):
                planes_to_cells(row, x_out, G)
        finish_copies(halos[s][2:])
        correct_edges(s, H, pc, pb, D)
        if s < 2:
            for side in range(2):
                E[side, s + 1] = E[side, s + 1] + D[side]
            start_copies(halos[s + 1][2:])
            for d, (_, blk, n) in enumerate(ends):
                more = edge_lanes(blk, n, D)
                for v in range(6):
                    U[s, d, v * 8 : v * 8 + 8, :] = new[d][v // 2][v % 2] + more[v]
            start_copies(halos[s + 1][:2])
            for blk in range(3):
                add_edges(blk, D, new_at)
        else:
            correct_cells(D, G)

    return_all(inv, G, S2, S2_rows, R2, s2, r2)
    for blk in range(3):
        add_edges(blk, D, new_at)
    for b in range(CHUNKS):
        wait_chunk(R2, b, r2)
        spread_chunk(b, R2_rows, Y)

    for b in range(CHUNKS):
        wait_chunk(R, b, s1)
        wait_chunk(R, b, s2)
    for copies in halos:
        for sends, _, copy, _ in copies:
            pl.when(sends)(copy.wait_send)


def prolong_kernel(y, x, w, pat, out, planes_out, fine, planes, sem, psem):
    def line(row, c):
        for v in range(6):
            at = (v % 2 * 24 + v // 2) * NI + row
            planes[pl.ds(at, 8, stride=3 * NI), :] = x[pl.ds(row * W + v * 8, 8), :]
        return c

    lax.fori_loop(0, NI, line, 0)
    plane_copy = pltpu.make_async_copy(planes, planes_out, psem)
    plane_copy.start()

    def copies(p):
        n = pl.ds(pl.multiple_of(p * AGG, AGG), AGG)
        return [
            pltpu.make_async_copy(fine.at[j, :, n], out.at[j, :, n], sem.at[p, j])
            for j in range(3)
        ]

    def block(p, c):
        def some(blk, c):
            for u in range(4):
                k = blk * 4 + u
                at = pl.ds(pl.multiple_of(p * AGG + k * LANES, LANES), LANES)
                base = pl.multiple_of(k * W, 8)
                there = bcast_row(pat, pl.ds(p * NK + k, 1), slice(None)).astype(F32)
                src = [
                    [y[pl.ds(base + i * 16 + qg * 8, 8), :] * there for qg in range(2)]
                    for i in range(3)
                ]
                for j in range(3):
                    acc = None
                    for i in range(3):
                        wij = jnp.broadcast_to(w[i, j : j + 1, at], (8, LANES))
                        terms = [wij * src[i][qg] for qg in range(2)]
                        acc = terms if acc is None else [a + z for a, z in zip(acc, terms)]
                    for qg in range(2):
                        fine[j, qg * 8 : qg * 8 + 8, at] = acc[qg]
            return c

        lax.fori_loop(0, NK // 4, some, 0)
        for copy in copies(p):
            copy.start()
        return c

    lax.fori_loop(0, FPA, block, 0)
    plane_copy.wait()

    def finish(p, c):
        for copy in copies(p):
            copy.wait()
        return c

    lax.fori_loop(0, FPA, finish, 0)


def body(residual, restriction, pattern, cell_aggregate, block_inverse, off_blocks, op_pattern):
    turned = residual.transpose(1, 0, 2)
    pat = pattern.reshape(384, LANES)
    vmem = pl.BlockSpec(memory_space=pltpu.VMEM)
    hbm = pl.BlockSpec(memory_space=pltpu.HBM)
    msg = pltpu.VMEM((CHUNKS, ND, 8, LANES), F32)
    plane = pltpu.VMEM((NI * W, LANES), F32)
    edge = pltpu.VMEM((2, 3, 3, 8, LANES), F32)
    x, y, held, held_pat = pl.pallas_call(
        coarse_kernel,
        out_shape=(
            jax.ShapeDtypeStruct((NI * W, LANES), F32),
            jax.ShapeDtypeStruct((NK * W, LANES), F32),
            jax.ShapeDtypeStruct((3, 3, FPA * AGG), F32),
            jax.ShapeDtypeStruct((384, LANES), jnp.int32),
        ),
        in_specs=[hbm] * 7,
        out_specs=(vmem,) * 4,
        scratch_shapes=[
            pltpu.VMEM((3, NQ, FPA * AGG), F32),
            pltpu.VMEM((NI, LANES), jnp.int32),
            pltpu.VMEM((9, NI, LANES), F32),
            pltpu.VMEM((36, NI, LANES), F32),
            pltpu.VMEM((4, NI, LANES), jnp.int32),
            plane,
            msg,
            msg,
            msg,
            msg,
            pltpu.VMEM((AGG, LANES), F32),
            pltpu.VMEM((8 * LANES, LANES), F32),
            pltpu.VMEM((8 * LANES, LANES), F32),
            pltpu.VMEM((LANES, LANES), F32),
            pltpu.VMEM((8, LANES), F32),
            plane,
            pltpu.VMEM((3, (NI + 2) * W, LANES), F32),
            pltpu.VMEM((2, 2, W, LANES), F32),
            edge,
            edge,
            pltpu.VMEM((2, 3, 8, LANES), F32),
            pltpu.VMEM((36, NI, LANES), F32),
            pltpu.VMEM((2, 9, 8, LANES), F32),
            pltpu.VMEM((2, 9, 8, LANES), F32),
            pltpu.VMEM((NI, LANES), jnp.int32),
            pltpu.VMEM((NI, LANES), jnp.int32),
            pltpu.VMEM((ND, LANES), jnp.int32),
            pltpu.SMEM((NI, LANES), jnp.int32),
            pltpu.SMEM((2, 8, LANES), jnp.int32),
            pltpu.SMEM((ND, LANES), jnp.int32),
            pltpu.SemaphoreType.DMA((2, CHUNKS, FPA)),
            pltpu.SemaphoreType.DMA((5,)),
            pltpu.SemaphoreType.DMA,
            pltpu.SemaphoreType.DMA((2,)),
            pltpu.SemaphoreType.DMA,
            pltpu.SemaphoreType.DMA((CHUNKS,)),
            pltpu.SemaphoreType.DMA((CHUNKS,)),
            pltpu.SemaphoreType.DMA((CHUNKS,)),
            pltpu.SemaphoreType.DMA((CHUNKS,)),
            pltpu.SemaphoreType.DMA((3, 4)),
            pltpu.SemaphoreType.DMA((3, 4)),
        ],
        compiler_params=pltpu.CompilerParams(
            collective_id=0, has_side_effects=True, vmem_limit_bytes=46 * 1024 * 1024
        ),
    )(
        *[
            pltpu.with_memory_space_constraint(x, pltpu.HBM)
            for x in (
                turned,
                restriction,
                pat,
                cell_aggregate,
                block_inverse.reshape(9, NI, LANES),
                off_blocks.reshape(36, NI, LANES),
                op_pattern,
            )
        ]
    )
    fine, planes = pl.pallas_call(
        prolong_kernel,
        out_shape=(
            jax.ShapeDtypeStruct((3, NQ, FPA * AGG), F32),
            jax.ShapeDtypeStruct((NQ * 3 * NI, LANES), F32),
        ),
        in_specs=[vmem] * 4,
        out_specs=(hbm, hbm),
        scratch_shapes=[
            pltpu.VMEM((3, NQ, FPA * AGG), F32),
            pltpu.VMEM((NQ * 3 * NI, LANES), F32),
            pltpu.SemaphoreType.DMA((FPA, 3)),
            pltpu.SemaphoreType.DMA,
        ],
        compiler_params=pltpu.CompilerParams(vmem_limit_bytes=24 * 1024 * 1024),
    )(y, x, held, held_pat)
    return planes.reshape(NQ, 3, NI, LANES), fine.transpose(1, 0, 2)


def solution(mesh):
    in_specs = (
        P(None, None, ("row", "col")),
        P(None, None, ("row", "col")),
        P(("row", "col")),
        P("row", "col"),
        P(None, None, "row", "col"),
        P(None, None, None, "row", "col"),
        P(None, "row", "col"),
    )
    out_specs = (P(None, None, "row", "col"), P(None, None, ("row", "col")))
    return jax.shard_map(body, mesh=mesh, in_specs=in_specs, out_specs=out_specs, check_vma=False)
```
